8 devices in a mesh: g: 8 (over z, y, x, core).
Axes of the slice: x: 2, y: 2, z: 1, core: 2. Of those that a mesh axis runs over, the one named last changes fastest.
Arguments:
- node_feat: bfloat16 [4096, 1536], P(None, 'g')
- w_self1: bfloat16 [1536, 128], P('g')
- w_nbr1: bfloat16 [1536, 128], P('g')
- nbr_ids: int32 [4096, 10], P('g')
- nbr_mask: int32 [4096, 10], P('g')
- w_self2: bfloat16 [128, 128], replicated
- w_nbr2: bfloat16 [128, 128], replicated
- w_self3: bfloat16 [128, 7], replicated
- w_nbr3: bfloat16 [128, 7], replicated
Outputs:
- output: float32 [4096, 7], P('g')
All inputs are finite; a program needn't handle non-finite values.
Results may differ from the reference program's by a relative error of at most 0.00933618.
Values are sent between devices in bfloat16 or wider.
A program may use at most 1 GiB of HBM per device.

```python
import jax
import jax.numpy as jnp
from jax import lax

FEAT_DIM = 1536
HIDDEN = 128
CLASSES = 7
FAN_IN = 10
NUM_NODES = 4096
HOT_NODES = NUM_NODES // 16


def draw_graph(graph_key):
    key_ids, key_hot, key_pick, key_deg = jax.random.split(graph_key, 4)
    wide_ids = jax.random.randint(key_ids, (NUM_NODES, FAN_IN), 0, NUM_NODES)
    hot_ids = jax.random.randint(key_hot, (NUM_NODES, FAN_IN), 0, HOT_NODES)
    pick_hot = jax.random.randint(key_pick, (NUM_NODES, FAN_IN), 0, 4) == 0
    nbr_ids = jnp.where(pick_hot, hot_ids, wide_ids)
    nbr_ids = nbr_ids.at[0, 0].set(NUM_NODES - 1).at[NUM_NODES - 1, 0].set(0).astype(jnp.int32)
    degree = jax.random.randint(key_deg, (NUM_NODES,), 1, FAN_IN + 1)
    degree = degree.at[0].set(FAN_IN).at[1].set(1)
    nbr_mask = (jnp.arange(FAN_IN)[None, :] < degree[:, None]).astype(jnp.int32)
    return nbr_ids, nbr_mask


def dense_weight(weight_key, fan_rows, fan_cols):
    normal_draw = jax.random.normal(weight_key, (fan_rows, fan_cols), jnp.float32)
    return (normal_draw * fan_rows ** -0.5).astype(jnp.bfloat16)


def setup_inputs(seed: int = 0) -> dict:
    key_list = jax.random.split(jax.random.key(seed), 8)
    nbr_ids, nbr_mask = draw_graph(key_list[0])
    node_feat = jax.random.normal(key_list[1], (NUM_NODES, FEAT_DIM), jnp.float32).astype(jnp.bfloat16)
    return {
        "node_feat": node_feat,
        "w_self1": dense_weight(key_list[2], FEAT_DIM, HIDDEN),
        "w_nbr1": dense_weight(key_list[3], FEAT_DIM, HIDDEN),
        "nbr_ids": nbr_ids,
        "nbr_mask": nbr_mask,
        "w_self2": dense_weight(key_list[4], HIDDEN, HIDDEN),
        "w_nbr2": dense_weight(key_list[5], HIDDEN, HIDDEN),
        "w_self3": dense_weight(key_list[6], HIDDEN, CLASSES),
        "w_nbr3": dense_weight(key_list[7], HIDDEN, CLASSES),
    }


def nbr_mean(row_data, nbr_ids, nbr_mask):
    mask_f = nbr_mask.astype(jnp.float32)

    def add_slot(acc_sum, slot_cols):
        ids_col, mask_col = slot_cols
        return acc_sum + mask_col[:, None] * row_data[ids_col].astype(jnp.float32), None

    zero_acc = jnp.zeros((nbr_ids.shape[0], row_data.shape[1]), jnp.float32)
    slot_sum, _ = lax.scan(add_slot, zero_acc, (nbr_ids.T, mask_f.T))
    return slot_sum / jnp.sum(mask_f, axis=1, keepdims=True)


def reference(node_feat, w_self1, w_nbr1, nbr_ids, nbr_mask, w_self2, w_nbr2, w_self3, w_nbr3):
    self_part = jnp.dot(node_feat, w_self1, preferred_element_type=jnp.float32)
    nbr_proj = jnp.dot(node_feat, w_nbr1, preferred_element_type=jnp.float32)
    hidden1 = jax.nn.relu(self_part + nbr_mean(nbr_proj, nbr_ids, nbr_mask)).astype(jnp.bfloat16)
    mean_one = nbr_mean(hidden1, nbr_ids, nbr_mask).astype(jnp.bfloat16)
    pre_two = jnp.dot(hidden1, w_self2, preferred_element_type=jnp.float32) + jnp.dot(mean_one, w_nbr2, preferred_element_type=jnp.float32)
    hidden2 = jax.nn.relu(pre_two).astype(jnp.bfloat16)
    mean_two = nbr_mean(hidden2, nbr_ids, nbr_mask).astype(jnp.bfloat16)
    logits = jnp.dot(hidden2, w_self3, preferred_element_type=jnp.float32) + jnp.dot(mean_two, w_nbr3, preferred_element_type=jnp.float32)
    return logits
```

```python
import jax
import jax.numpy as jnp
from jax import lax
from jax.experimental import pallas as pl
from jax.experimental.pallas import tpu as pltpu
from jax.sharding import PartitionSpec as P

MESH = pl.DeviceIdType.MESH
N_DEV = 8
NODES = 4096
BLK = NODES // N_DEV
HALF = NODES // 2
FAN = 10
HID = 128
TILE = 256
LANES = 256
GROUPS = BLK // LANES
BF = jnp.bfloat16
F32 = jnp.float32


def spread_ids(ids_s32, idb, wb, inv, slot):
    for g in range(GROUPS):
        cols = slice(g * LANES, (g + 1) * LANES)
        words, weights = [], []
        degree = jnp.zeros((8, LANES), F32)
        for k in range(FAN):
            raw = jnp.broadcast_to(ids_s32[slot, k : k + 1, cols], (8, LANES))
            valid = raw >= 0
            degree += jnp.where(valid, 1.0, 0.0)
            upper = raw >= HALF
            word = jnp.where(upper, raw - HALF, raw)
            weight = jnp.where(valid, jnp.where(upper, 1.0, 0.0625), 0.0)
            for m in range(k):
                same = word == words[m]
                weights[m] = weights[m] + jnp.where(same, weight, 0.0)
                word = jnp.where(same, -1, word)
            words.append(word)
            weights.append(weight)
        inv[slot, :, cols] = 1.0 / degree
        for k in range(FAN):
            idb[slot, g, k] = words[k].astype(jnp.int16)
            wb[slot, g, k] = weights[k].astype(BF)


def build_tile(first_row, row_ids, idb, wb, slot, store_low, store_high):
    start = row_ids[...] + jnp.full((8, LANES), first_row, jnp.int32).astype(jnp.int16)
    for g in range(GROUPS):
        ids = [idb[slot, g, k] for k in range(FAN)]
        wts = [wb[slot, g, k] for k in range(FAN)]
        rows = start
        for r in range(TILE // 8):
            acc = jnp.zeros((8, LANES), BF)
            for k in range(FAN):
                acc = jnp.where(ids[k] == rows, wts[k], acc)
            high = jnp.floor(acc)
            store_high(r * 8, g * LANES, high)
            store_low(r * 8, g * LANES, (acc - high) * jnp.array(16.0, BF))
            rows = rows + jnp.array(8, jnp.int16)


def kernel(
    x_hbm, ws1, wn1, ids_in, mask_in, ws2, wn2, ws3t, wn3t, out_ref,
    x_v, w1t, w2st, w2nt, yown, yrecv, ysum, sown, ssend, srecv,
    ids_pkt, ids_rcv, ids_s32, row_ids, idb, wb, inv,
    lo0, hi0, lo1, hi1, a_own, acc, zacc, rs_send, rs_recv, h1, h2,
    x_sem, ids_ss, ids_rs, y_ss, y_rs, s_ss, s_rs, r_ss, r_rs, g1_ss, g1_rs, g2_ss, g2_rs,
):
    me = lax.axis_index("g")
    core = lax.rem(me, 2)
    cx = lax.rem(me // 2, 2)
    cy = me // 4
    partner = me + 1 - 2 * core
    peer_x = me + 2 - 4 * cx
    peer_y = me + 4 - 8 * cy
    peer_d = me + 6 - 4 * cx - 8 * cy
    peers = (peer_d, peer_y, peer_x)

    barrier = pltpu.get_barrier_semaphore()
    for peer in (peer_d, peer_y, peer_x, partner):
        pl.semaphore_signal(barrier, inc=1, device_id=(peer,), device_id_type=MESH)

    x_copies = []
    for b in range(N_DEV):
        cp = pltpu.make_async_copy(x_hbm.at[:, pl.ds(b * BLK, BLK)], x_v.at[b], x_sem.at[b])
        cp.start()
        x_copies.append(cp)

    def remote(src, dst, ss, rs, dev):
        return pltpu.make_async_remote_copy(
            src_ref=src, dst_ref=dst, send_sem=ss, recv_sem=rs, device_id=(dev,), device_id_type=MESH
        )

    masked = jnp.where(mask_in[...] > 0, ids_in[...], -1)
    ids_pkt[...] = jnp.full(ids_pkt.shape, -1, jnp.int16)
    ids_pkt[0:FAN, :] = masked.astype(jnp.int16)
    ids_s32[3, 0:FAN, :] = masked
    w1t[0:HID, :] = ws1[...].T
    w1t[HID:, :] = wn1[...].T
    w2st[...] = ws2[...].T
    w2nt[...] = wn2[...].T
    acc[...] = jnp.zeros_like(acc)

    pl.semaphore_wait(barrier, 4)
    sends = []
    id_copies = [remote(ids_pkt, ids_rcv.at[s], ids_ss.at[s], ids_rs.at[s], peers[s]) for s in range(3)]
    for cp in id_copies:
        cp.start()
    sends += id_copies

    for cp in x_copies:
        cp.wait()
    y_copies, s_copies = [], []
    for i in range(4):
        b = 2 * i + 1 - core
        part = jnp.dot(w1t[...], x_v[b], preferred_element_type=F32)
        yown[b] = part[HID:].astype(BF)
        ssend[i] = part[:HID].astype(BF)
        y_copies.append(remote(yown.at[b], yrecv.at[b], y_ss.at[2 * i], y_rs.at[2 * i + 1], partner))
        s_copies.append(remote(ssend.at[i], srecv.at[i], s_ss.at[i], s_rs.at[i], partner))
        b2 = 2 * i + core
        part2 = jnp.dot(w1t[...], x_v[b2], preferred_element_type=F32)
        yown[b2] = part2[HID:].astype(BF)
        sown[i] = part2[:HID]
        y_copies.append(remote(yown.at[b2], yrecv.at[b2], y_ss.at[2 * i + 1], y_rs.at[2 * i], partner))
        y_copies[-2].start()
        s_copies[-1].start()
        y_copies[-1].start()
    sends += y_copies + s_copies

    row_ids[...] = lax.broadcasted_iota(jnp.int32, (8, LANES), 0).astype(jnp.int16)
    spread_ids(ids_s32, idb, wb, inv, 3)

    def own_step(c, carry):
        for par in range(2):

            def put(half):
                def store(r, l, v):
                    a_own[half * 4 + c, par * TILE + r : par * TILE + r + 8, l : l + LANES] = v

                return store

            build_tile(c * 2 * TILE + par * TILE, row_ids, idb, wb, 3, put(0), put(1))
        return carry

    lax.fori_loop(0, 4, own_step, 0)

    for s in range(3):
        id_copies[s].wait_recv()
        ids_s32[s] = ids_rcv[s].astype(jnp.int32)
        spread_ids(ids_s32, idb, wb, inv, s)
    for cp in y_copies:
        cp.wait_recv()
    for cp in s_copies:
        cp.wait_recv()
    for b in range(N_DEV):
        ysum[b] = yown[b] + yrecv[b]

    bufs = ((lo0, hi0), (lo1, hi1))

    def put_into(ref):
        def store(r, l, v):
            ref[r : r + 8, l : l + LANES] = v

        return store

    def build_into(par, flat, slot):
        lo, hi = bufs[par]
        build_tile(lax.rem(flat, 8) * TILE, row_ids, idb, wb, slot, put_into(lo), put_into(hi))

    def dot_from(par, cc):
        lo, hi = bufs[par]
        cols = slice(par * TILE, (par + 1) * TILE)
        return jnp.dot(ysum[cc, :, cols], lo[...], preferred_element_type=F32) + jnp.dot(
            ysum[4 + cc, :, cols], hi[...], preferred_element_type=F32
        )

    def rs_copy(s):
        return remote(rs_send.at[s], rs_recv.at[s], r_ss.at[s], r_rs.at[s], peers[s])

    build_into(0, 0, 0)

    def rs_step(p, carry):
        s = p // 4
        cc = lax.rem(p, 4)
        acc[...] += dot_from(0, cc)
        build_into(1, 2 * p + 1, s)
        acc[...] += dot_from(1, cc)
        build_into(0, 2 * p + 2, lax.rem((2 * p + 2) // 8, 3))
        for t in range(3):

            @pl.when(p == 4 * t + 3)
            def _():
                chip = peers[t] // 2
                total = acc[...] * jnp.broadcast_to(inv[t, 0:1, :], (HID, BLK)) + sown[chip] + srecv[chip].astype(F32)
                rs_send[t] = total.astype(BF)
                acc[...] = jnp.zeros_like(acc)
                rs_copy(t).start()

        return carry

    lax.fori_loop(0, 12, rs_step, 0)
    rs_copies = [rs_copy(t) for t in range(3)]
    sends += rs_copies

    def own_dot(h, b):
        return jnp.dot(h[b], a_own[b], preferred_element_type=F32)

    inv_own = jnp.broadcast_to(inv[3, 0:1, :], (HID, BLK))
    zacc[...] = own_dot(ysum, 0)
    for b in range(1, N_DEV):
        zacc[...] += own_dot(ysum, b)
    chip_me = me // 2
    zacc[...] = zacc[...] * inv_own + sown[chip_me] + srecv[chip_me].astype(F32)
    for t in range(3):
        rs_copies[t].wait_recv()
        zacc[...] += rs_recv[t].astype(F32)
    h1[me] = jnp.maximum(zacc[...], 0.0).astype(BF)

    def gather_mean(h, ss, rs):
        first = [remote(h.at[me], h.at[me], ss.at[t], rs.at[t], peers[t]) for t in range(3)]
        to_partner = remote(h.at[me], h.at[me], ss.at[3], rs.at[3], partner)
        for cp in first:
            cp.start()
        to_partner.start()
        acc[...] = own_dot(h, me)
        to_partner.wait_recv()
        acc[...] += own_dot(h, partner)
        forwards = []
        for t in (1, 2, 0):
            first[t].wait_recv()
            fwd = remote(h.at[peers[t]], h.at[peers[t]], ss.at[4 + t], rs.at[4 + t], partner)
            fwd.start()
            forwards.append((t, fwd))
        for t in (1, 2, 0):
            acc[...] += own_dot(h, peers[t])
        for t, fwd in forwards:
            fwd.wait_recv()
            acc[...] += own_dot(h, peers[t] + 1 - 2 * core)
        return first + [to_partner] + [f for _, f in forwards]

    sends += gather_mean(h1, g1_ss, g1_rs)
    mean1 = (acc[...] * jnp.broadcast_to(inv[3, 0:1, :], (HID, BLK))).astype(BF)
    pre2 = jnp.dot(w2st[...], h1[me], preferred_element_type=F32) + jnp.dot(
        w2nt[...], mean1, preferred_element_type=F32
    )
    h2[me] = jnp.maximum(pre2, 0.0).astype(BF)
    sends += gather_mean(h2, g2_ss, g2_rs)
    mean2 = (acc[...] * jnp.broadcast_to(inv[3, 0:1, :], (HID, BLK))).astype(BF)
    out_ref[...] = jnp.dot(ws3t[...], h2[me], preferred_element_type=F32) + jnp.dot(
        wn3t[...], mean2, preferred_element_type=F32
    )
    for cp in sends:
        cp.wait_send()


def solution(mesh):
    def device_step(feat, ws1, wn1, ids, mask, ws2, wn2, ws3, wn3):
        vm = pl.BlockSpec(memory_space=pltpu.VMEM)
        dma = pltpu.SemaphoreType.DMA
        out_t = pl.pallas_call(
            kernel,
            out_shape=jax.ShapeDtypeStruct((7, BLK), F32),
            in_specs=[pl.BlockSpec(memory_space=pl.ANY)] + [vm] * 8,
            out_specs=vm,
            scratch_shapes=[
                pltpu.VMEM((N_DEV, 192, BLK), BF),
                pltpu.VMEM((2 * HID, 192), BF),
                pltpu.VMEM((HID, HID), BF),
                pltpu.VMEM((HID, HID), BF),
                pltpu.VMEM((N_DEV, HID, BLK), BF),
                pltpu.VMEM((N_DEV, HID, BLK), BF),
                pltpu.VMEM((N_DEV, HID, BLK), BF),
                pltpu.VMEM((4, HID, BLK), F32),
                pltpu.VMEM((4, HID, BLK), BF),
                pltpu.VMEM((4, HID, BLK), BF),
                pltpu.VMEM((16, BLK), jnp.int16),
                pltpu.VMEM((3, 16, BLK), jnp.int16),
                pltpu.VMEM((4, 16, BLK), jnp.int32),
                pltpu.VMEM((8, LANES), jnp.int16),
                pltpu.VMEM((4, GROUPS, FAN, 8, LANES), jnp.int16),
                pltpu.VMEM((4, GROUPS, FAN, 8, LANES), BF),
                pltpu.VMEM((4, 8, BLK), F32),
                pltpu.VMEM((TILE, BLK), BF),
                pltpu.VMEM((TILE, BLK), BF),
                pltpu.VMEM((TILE, BLK), BF),
                pltpu.VMEM((TILE, BLK), BF),
                pltpu.VMEM((N_DEV, BLK, BLK), BF),
                pltpu.VMEM((HID, BLK), F32),
                pltpu.VMEM((HID, BLK), F32),
                pltpu.VMEM((3, HID, BLK), BF),
                pltpu.VMEM((3, HID, BLK), BF),
                pltpu.VMEM((N_DEV, HID, BLK), BF),
                pltpu.VMEM((N_DEV, HID, BLK), BF),
                dma((N_DEV,)),
                dma((3,)), dma((3,)),
                dma((8,)), dma((8,)),
                dma((4,)), dma((4,)),
                dma((3,)), dma((3,)),
                dma((7,)), dma((7,)),
                dma((7,)), dma((7,)),
            ],
            compiler_params=pltpu.CompilerParams(
                collective_id=0, has_side_effects=True, vmem_limit_bytes=60 * 1024 * 1024
            ),
            name="graphsage",
        )(feat.T, ws1, wn1, ids.T, mask.T, ws2, wn2, ws3.T, wn3.T)
        return out_t.T

    col_split = P(None, "g")
    row_split = P("g", None)
    replicated = P()
    return jax.shard_map(
        device_step,
        mesh=mesh,
        in_specs=(col_split, row_split, row_split, row_split, row_split, replicated, replicated, replicated, replicated),
        out_specs=row_split,
        check_vma=False,
    )
```

```python
import jax
import jax.numpy as jnp
from jax import lax
from jax.experimental import pallas as pl
from jax.experimental.pallas import tpu as pltpu
from jax.sharding import PartitionSpec as P

MESH = pl.DeviceIdType.MESH
N_DEV = 8
NODES = 4096
BLK = NODES // N_DEV
HALF = NODES // 2
FAN = 10
HID = 128
TILE = 256
LANES = 256
GROUPS = BLK // LANES
BF = jnp.bfloat16
F32 = jnp.float32


def spread_ids(ids_s32, idb, wb, inv, slot):
    for g in range(GROUPS):
        cols = slice(g * LANES, (g + 1) * LANES)
        words, weights = [], []
        degree = jnp.zeros((8, LANES), F32)
        for k in range(FAN):
            raw = jnp.broadcast_to(ids_s32[slot, k : k + 1, cols], (8, LANES))
            valid = raw >= 0
            degree += jnp.where(valid, 1.0, 0.0)
            upper = raw >= HALF
            word = jnp.where(upper, raw - HALF, raw)
            weight = jnp.where(valid, jnp.where(upper, 1.0, 0.0625), 0.0)
            for m in range(k):
                same = word == words[m]
                weights[m] = weights[m] + jnp.where(same, weight, 0.0)
                word = jnp.where(same, -1, word)
            words.append(word)
            weights.append(weight)
        inv[slot, :, cols] = 1.0 / degree
        for k in range(FAN):
            idb[slot, g, k] = words[k].astype(jnp.int16)
            wb[slot, g, k] = weights[k].astype(BF)


def build_tile(tile, row_ids, idb, wb, slot, groups, store_low, store_high):
    for g in groups:
        ids = [idb[slot, g, k] for k in range(FAN)]
        wts = [wb[slot, g, k] for k in range(FAN)]
        for r in range(TILE // 8):
            rows = row_ids[tile, r]
            acc = jnp.zeros((8, LANES), BF)
            for k in range(FAN):
                acc = jnp.where(ids[k] == rows, wts[k], acc)
            high = jnp.floor(acc)
            store_high(r * 8, g * LANES, high)
            store_low(r * 8, g * LANES, acc - high)


def kernel(
    x_hbm, ws1_hbm, wn1_hbm, ids_hbm, mask_hbm, ws2_hbm, wn2_hbm, ws3_hbm, wn3_hbm, out_ref,
    x_v, ws1, wn1, ids_in, mask_in, ws2, wn2, ws3t, wn3t,
    w1t, w2st, w2nt, yown, yrecv, ysum, sown, ssend, srecv,
    ids_pkt, ids_rcv, ids_s32, row_ids, idb, wb, inv,
    lo0, hi0, lo1, hi1, lo2, hi2, lo3, hi3, a_own, acc, rs_send, rs_recv, h1, h2,
    in_sem, x_sem, ids_ss, ids_rs, y_ss, y_rs, s_ss, s_rs, r_ss, r_rs, g1_ss, g1_rs, g2_ss, g2_rs,
):
    me = lax.axis_index("g")
    core = lax.rem(me, 2)
    cx = lax.rem(me // 2, 2)
    cy = me // 4
    partner = me + 1 - 2 * core
    peer_x = me + 2 - 4 * cx
    peer_y = me + 4 - 8 * cy
    peer_d = me + 6 - 4 * cx - 8 * cy
    peers = (peer_d, peer_y, peer_x)

    barrier = pltpu.get_barrier_semaphore()
    for peer in (peer_d, peer_y, peer_x, partner):
        pl.semaphore_signal(barrier, inc=1, device_id=(peer,), device_id_type=MESH)

    def fetch(src, dst, i):
        cp = pltpu.make_async_copy(src, dst, in_sem.at[i])
        cp.start()
        return cp

    ids_cp = fetch(ids_hbm, ids_in, 0)
    mask_cp = fetch(mask_hbm, mask_in, 1)
    w1_cps = [fetch(ws1_hbm, ws1, 2), fetch(wn1_hbm, wn1, 3)]
    x_copies = []
    for b in range(N_DEV):
        cp = pltpu.make_async_copy(x_hbm.at[:, pl.ds(b * BLK, BLK)], x_v.at[b], x_sem.at[b])
        cp.start()
        x_copies.append(cp)
    late_cps = [fetch(ws2_hbm, ws2, 4), fetch(wn2_hbm, wn2, 5), fetch(ws3_hbm, ws3t, 6), fetch(wn3_hbm, wn3t, 7)]

    def remote(src, dst, ss, rs, dev):
        return pltpu.make_async_remote_copy(
            src_ref=src, dst_ref=dst, send_sem=ss, recv_sem=rs, device_id=(dev,), device_id_type=MESH
        )

    for tile in range(HALF // TILE):
        for r in range(TILE // 8):
            rows = lax.broadcasted_iota(jnp.int32, (8, LANES), 0) + (tile * TILE + r * 8)
            row_ids[tile, r] = rows.astype(jnp.int16)
    ids_pkt[...] = jnp.full(ids_pkt.shape, -1, jnp.int16)
    ids_cp.wait()
    mask_cp.wait()
    masked = jnp.where(mask_in[...] > 0, ids_in[...], -1)
    ids_pkt[0:FAN, :] = masked.astype(jnp.int16)
    ids_s32[3, 0:FAN, :] = masked
    for cp in w1_cps:
        cp.wait()
    w1t[0:HID, :] = ws1[...].T
    w1t[HID:, :] = wn1[...].T

    pl.semaphore_wait(barrier, 4)
    sends = []
    id_copies = [remote(ids_pkt, ids_rcv.at[s], ids_ss.at[s], ids_rs.at[s], peers[s]) for s in range(3)]
    for cp in id_copies:
        cp.start()
    sends += id_copies

    for cp in x_copies:
        cp.wait()
    y_copies, s_copies = [], []
    for i in range(4):
        b = 2 * i + 1 - core
        part = jnp.dot(w1t[...], x_v[b], preferred_element_type=F32)
        yown[b] = part[HID:].astype(BF)
        ssend[i] = part[:HID].astype(BF)
        y_copies.append(remote(yown.at[b], yrecv.at[b], y_ss.at[2 * i], y_rs.at[2 * i + 1], partner))
        s_copies.append(remote(ssend.at[i], srecv.at[i], s_ss.at[i], s_rs.at[i], partner))
        b2 = 2 * i + core
        part2 = jnp.dot(w1t[...], x_v[b2], preferred_element_type=F32)
        yown[b2] = part2[HID:].astype(BF)
        sown[i] = part2[:HID]
        y_copies.append(remote(yown.at[b2], yrecv.at[b2], y_ss.at[2 * i + 1], y_rs.at[2 * i], partner))
        y_copies[-2].start()
        s_copies[-1].start()
        y_copies[-1].start()
    sends += y_copies + s_copies

    spread_ids(ids_s32, idb, wb, inv, 3)

    def own_step(c, carry):
        for par in range(2):

            def put(half):
                def store(r, l, v):
                    v = v if half else v * jnp.array(16.0, BF)
                    a_own[half * 4 + c, par * TILE + r : par * TILE + r + 8, l : l + LANES] = v

                return store

            build_tile(2 * c + par, row_ids, idb, wb, 3, range(GROUPS), put(0), put(1))
        return carry

    lax.fori_loop(0, 4, own_step, 0)
    for cp in late_cps:
        cp.wait()
    w2st[...] = ws2[...].T
    w2nt[...] = wn2[...].T

    ring = ((lo0, hi0), (lo1, hi1), (lo2, hi2), (lo3, hi3))

    def build_into(tile, slot, g):
        lo, hi = ring[tile % 4]

        def put_into(ref):
            def store(r, l, v):
                ref[r : r + 8, :] = v

            return store

        build_tile(tile, row_ids, idb, wb, slot, (g,), put_into(lo), put_into(hi))

    def dot_from(tile):
        lo, hi = ring[tile % 4]
        cols = slice(tile % 2 * TILE, (tile % 2 + 1) * TILE)
        low = jnp.dot(ysum[tile // 2, :, cols], lo[...], preferred_element_type=F32)
        high = jnp.dot(ysum[4 + tile // 2, :, cols], hi[...], preferred_element_type=F32)
        return low, high

    def lanes(g):
        return slice(g * LANES, (g + 1) * LANES)

    def take_ids(s):
        id_copies[s].wait_recv()
        ids_s32[s] = ids_rcv[s].astype(jnp.int32)
        spread_ids(ids_s32, idb, wb, inv, s)

    def unit(u):
        return lax.rem(1 + 2 * lax.rem(u, 3), 3), lax.rem(u // 3, 2)

    def rs_copy(s, g, peer):
        return remote(rs_send.at[s, g], rs_recv.at[s, g], r_ss.at[2 * s + g], r_rs.at[2 * s + g], peer)

    take_ids(1)
    build_into(0, 1, 0)
    for cp in y_copies:
        cp.wait_recv()
    for cp in s_copies:
        cp.wait_recv()
    for b in range(N_DEV):
        ysum[b] = yown[b] + yrecv[b]

    def unit_step(u, carry):
        s, g = unit(u)
        after_s, after_g = unit(u + 1)

        @pl.when(u == 0)
        def _():
            take_ids(0)

        @pl.when(u == 1)
        def _():
            take_ids(2)

        low = high = None
        for tile in range(8):
            part = dot_from(tile)
            if tile < 7:
                build_into(tile + 1, s, g)
            else:
                build_into(0, after_s, after_g)
            low = part[0] if low is None else low + part[0]
            high = part[1] if high is None else high + part[1]
        peer = me + (1 - lax.rem(s, 2)) * (2 - 4 * cx) + (1 - s // 2) * (4 - 8 * cy)
        cols = pl.ds(pl.multiple_of(g * LANES, LANES), LANES)
        chip = peer // 2
        total = (low * 16.0 + high) * jnp.broadcast_to(inv[s, 0:1, cols], (HID, LANES))
        total = total + sown[chip, :, cols] + srecv[chip, :, cols].astype(F32)
        rs_send[s, g] = total.astype(BF)
        rs_copy(s, g, peer).start()
        return carry

    lax.fori_loop(0, 6, unit_step, 0)
    rs_copies = {(s, g): rs_copy(s, g, peers[s]) for s in range(3) for g in range(2)}
    sends += list(rs_copies.values())

    chip_me = me // 2
    inv_own = jnp.broadcast_to(inv[3, 0:1, :], (HID, BLK))

    def own_dot(h, b, p):
        return jnp.dot(h[b, p], a_own[b, p * TILE : (p + 1) * TILE, :], preferred_element_type=F32)

    def gather_start(h, ss, rs, p):
        outs = [remote(h.at[me, p], h.at[me, p], ss.at[7 * p + t], rs.at[7 * p + t], peers[t]) for t in range(3)]
        outs.append(remote(h.at[me, p], h.at[me, p], ss.at[7 * p + 3], rs.at[7 * p + 3], partner))
        for cp in outs:
            cp.start()
        return outs

    def gather_finish(h, ss, rs, started):
        acc[...] = own_dot(h, me, 0) + own_dot(h, me, 1)
        for p in range(2):
            started[p][3].wait_recv()
            acc[...] += own_dot(h, partner, p)
        forwards = []
        for p in range(2):
            for t in (1, 2, 0):
                started[p][t].wait_recv()
                fwd = remote(
                    h.at[peers[t], p], h.at[peers[t], p], ss.at[7 * p + 4 + t], rs.at[7 * p + 4 + t], partner
                )
                fwd.start()
                forwards.append((t, p, fwd))
            for t in (1, 2, 0):
                acc[...] += own_dot(h, peers[t], p)
        for t, p, fwd in forwards:
            fwd.wait_recv()
            acc[...] += own_dot(h, peers[t] + 1 - 2 * core, p)
        return started[0] + started[1] + [f for _, _, f in forwards]

    started1 = []
    for g in range(2):
        own = jnp.dot(ysum[0], a_own[0, :, lanes(g)], preferred_element_type=F32)
        for b in range(1, N_DEV):
            own = own + jnp.dot(ysum[b], a_own[b, :, lanes(g)], preferred_element_type=F32)
        z = own * inv_own[:, lanes(g)] + sown[chip_me, :, lanes(g)] + srecv[chip_me, :, lanes(g)].astype(F32)
        for t in (1, 0, 2):
            rs_copies[t, g].wait_recv()
            z = z + rs_recv[t, g].astype(F32)
        h1[me, g] = jnp.maximum(z, 0.0).astype(BF)
        started1.append(gather_start(h1, g1_ss, g1_rs, g))
    sends += gather_finish(h1, g1_ss, g1_rs, started1)

    started2 = []
    for g in range(2):
        mean1 = (acc[:, lanes(g)] * inv_own[:, lanes(g)]).astype(BF)
        pre2 = jnp.dot(w2st[...], h1[me, g], preferred_element_type=F32) + jnp.dot(
            w2nt[...], mean1, preferred_element_type=F32
        )
        h2[me, g] = jnp.maximum(pre2, 0.0).astype(BF)
        started2.append(gather_start(h2, g2_ss, g2_rs, g))
    sends += gather_finish(h2, g2_ss, g2_rs, started2)
    for g in range(2):
        mean2 = (acc[:, lanes(g)] * inv_own[:, lanes(g)]).astype(BF)
        out_ref[:, lanes(g)] = jnp.dot(ws3t[...], h2[me, g], preferred_element_type=F32) + jnp.dot(
            wn3t[...], mean2, preferred_element_type=F32
        )
    for cp in sends:
        cp.wait_send()


def solution(mesh):
    def device_step(feat, ws1, wn1, ids, mask, ws2, wn2, ws3, wn3):
        vm = pl.BlockSpec(memory_space=pltpu.VMEM)
        dma = pltpu.SemaphoreType.DMA
        out_t = pl.pallas_call(
            kernel,
            out_shape=jax.ShapeDtypeStruct((7, BLK), F32),
            in_specs=[pl.BlockSpec(memory_space=pl.ANY)] * 9,
            out_specs=vm,
            scratch_shapes=[
                pltpu.VMEM((N_DEV, 192, BLK), BF),
                pltpu.VMEM((192, HID), BF),
                pltpu.VMEM((192, HID), BF),
                pltpu.VMEM((FAN, BLK), jnp.int32),
                pltpu.VMEM((FAN, BLK), jnp.int32),
                pltpu.VMEM((HID, HID), BF),
                pltpu.VMEM((HID, HID), BF),
                pltpu.VMEM((7, HID), BF),
                pltpu.VMEM((7, HID), BF),
                pltpu.VMEM((2 * HID, 192), BF),
                pltpu.VMEM((HID, HID), BF),
                pltpu.VMEM((HID, HID), BF),
                pltpu.VMEM((N_DEV, HID, BLK), BF),
                pltpu.VMEM((N_DEV, HID, BLK), BF),
                pltpu.VMEM((N_DEV, HID, BLK), BF),
                pltpu.VMEM((4, HID, BLK), F32),
                pltpu.VMEM((4, HID, BLK), BF),
                pltpu.VMEM((4, HID, BLK), BF),
                pltpu.VMEM((16, BLK), jnp.int16),
                pltpu.VMEM((3, 16, BLK), jnp.int16),
                pltpu.VMEM((4, 16, BLK), jnp.int32),
                pltpu.VMEM((HALF // TILE, TILE // 8, 8, LANES), jnp.int16),
                pltpu.VMEM((4, GROUPS, FAN, 8, LANES), jnp.int16),
                pltpu.VMEM((4, GROUPS, FAN, 8, LANES), BF),
                pltpu.VMEM((4, 8, BLK), F32),
                pltpu.VMEM((TILE, LANES), BF),
                pltpu.VMEM((TILE, LANES), BF),
                pltpu.VMEM((TILE, LANES), BF),
                pltpu.VMEM((TILE, LANES), BF),
                pltpu.VMEM((TILE, LANES), BF),
                pltpu.VMEM((TILE, LANES), BF),
                pltpu.VMEM((TILE, LANES), BF),
                pltpu.VMEM((TILE, LANES), BF),
                pltpu.VMEM((N_DEV, BLK, BLK), BF),
                pltpu.VMEM((HID, BLK), F32),
                pltpu.VMEM((3, 2, HID, LANES), BF),
                pltpu.VMEM((3, 2, HID, LANES), BF),
                pltpu.VMEM((N_DEV, 2, HID, LANES), BF),
                pltpu.VMEM((N_DEV, 2, HID, LANES), BF),
                dma((8,)),
                dma((N_DEV,)),
                dma((3,)), dma((3,)),
                dma((8,)), dma((8,)),
                dma((4,)), dma((4,)),
                dma((6,)), dma((6,)),
                dma((14,)), dma((14,)),
                dma((14,)), dma((14,)),
            ],
            compiler_params=pltpu.CompilerParams(
                collective_id=0, has_side_effects=True, vmem_limit_bytes=60 * 1024 * 1024
            ),
            name="graphsage",
        )(feat.T, ws1, wn1, ids.T, mask.T, ws2, wn2, ws3.T, wn3.T)
        return out_t.T

    col_split = P(None, "g")
    row_split = P("g", None)
    replicated = P()
    return jax.shard_map(
        device_step,
        mesh=mesh,
        in_specs=(col_split, row_split, row_split, row_split, row_split, replicated, replicated, replicated, replicated),
        out_specs=row_split,
        check_vma=False,
    )
```

```python
import jax
import jax.numpy as jnp
from jax import lax
from jax.experimental import pallas as pl
from jax.experimental.pallas import tpu as pltpu
from jax.sharding import PartitionSpec as P

MESH = pl.DeviceIdType.MESH
N_DEV = 8
NODES = 4096
BLK = NODES // N_DEV
HALF = NODES // 2
FAN = 10
HID = 128
TILE = 256
LANES = 256
BF = jnp.bfloat16
F32 = jnp.float32


UNITS = (((2, 0), (1, 0)), ((0, 0), (0, 1)), ((2, 1), (1, 1)), ((0, 2), (0, 3)), ((2, 2), (1, 2)), ((2, 3), (1, 3)))
OWN = 6
RING = 6
Q = 128


def spread_ids(ids_s32, idb, wb, inv, u):
    words, weights = [], []
    degree = jnp.zeros((8, LANES), F32)
    for k in range(FAN):
        raw = jnp.broadcast_to(ids_s32[u, k : k + 1, :], (8, LANES))
        valid = raw >= 0
        degree += jnp.where(valid, 1.0, 0.0)
        upper = raw >= HALF
        word = jnp.where(upper, raw - HALF, raw)
        weight = jnp.where(valid, jnp.where(upper, 1.0, 0.0625), 0.0)
        for m in range(k):
            same = word == words[m]
            weights[m] = weights[m] + jnp.where(same, weight, 0.0)
            word = jnp.where(same, -1, word)
        words.append(word)
        weights.append(weight)
    inv[u] = 1.0 / degree
    for k in range(FAN):
        idb[u, k] = words[k].astype(jnp.int16)
        wb[u, k] = weights[k].astype(BF)


def build_tile(tile, row_ids, idb, wb, u, store_low, store_high):
    ids = [idb[u, k] for k in range(FAN)]
    wts = [wb[u, k] for k in range(FAN)]
    for r in range(0, TILE // 8, 8):
        rows = row_ids[tile, r : r + 8]
        acc = jnp.zeros((8, 8, LANES), BF)
        for k in range(FAN):
            acc = jnp.where(ids[k][None] == rows, wts[k][None], acc)
        high = jnp.floor(acc)
        store_high(r, high)
        store_low(r, acc - high)


def kernel(
    x_hbm, ws1_hbm, wn1_hbm, ids_hbm, mask_hbm, ws2_hbm, wn2_hbm, ws3_hbm, wn3_hbm, out_ref,
    x_v, ws1, wn1, ids_in, mask_in, ws2, wn2, ws3t, wn3t,
    w1t, w2st, w2nt, yown, yrecv, ysum, sown, ssend, srecv,
    ids_pkt, ids_rcv, ids_s32, row_ids, idb, wb, inv,
    ring, a_own, acc, zbase, rs_send, rs_recv, h1, h2,
    in_sem, x_sem, ids_ss, ids_rs, y_ss, y_rs, s_ss, s_rs, r_ss, r_rs, g1_ss, g1_rs, g2_ss, g2_rs,
):
    me = lax.axis_index("g")
    core = lax.rem(me, 2)
    cx = lax.rem(me // 2, 2)
    cy = me // 4
    partner = me + 1 - 2 * core
    peer_x = me + 2 - 4 * cx
    peer_y = me + 4 - 8 * cy
    peer_d = me + 6 - 4 * cx - 8 * cy
    peers = (peer_d, peer_y, peer_x)

    barrier = pltpu.get_barrier_semaphore()
    for peer in (peer_d, peer_y, peer_x, partner):
        pl.semaphore_signal(barrier, inc=1, device_id=(peer,), device_id_type=MESH)

    def fetch(src, dst, i):
        cp = pltpu.make_async_copy(src, dst, in_sem.at[i])
        cp.start()
        return cp

    ids_cp = fetch(ids_hbm, ids_in, 0)
    mask_cp = fetch(mask_hbm, mask_in, 1)
    w1_cps = [fetch(ws1_hbm, ws1, 2), fetch(wn1_hbm, wn1, 3)]
    x_copies = []
    for b in range(N_DEV):
        cp = pltpu.make_async_copy(x_hbm.at[:, pl.ds(b * BLK, BLK)], x_v.at[b], x_sem.at[b])
        cp.start()
        x_copies.append(cp)
    late_cps = [fetch(ws2_hbm, ws2, 4), fetch(wn2_hbm, wn2, 5), fetch(ws3_hbm, ws3t, 6), fetch(wn3_hbm, wn3t, 7)]

    def remote(src, dst, ss, rs, dev):
        return pltpu.make_async_remote_copy(
            src_ref=src, dst_ref=dst, send_sem=ss, recv_sem=rs, device_id=(dev,), device_id_type=MESH
        )

    row_shape = (TILE // 8, 8, LANES)
    row_base = lax.broadcasted_iota(jnp.int32, row_shape, 0) * 8 + lax.broadcasted_iota(jnp.int32, row_shape, 1)
    for tile in range(HALF // TILE):
        row_ids[tile] = (row_base + tile * TILE).astype(jnp.int16)
    ids_pkt[...] = jnp.full(ids_pkt.shape, -1, jnp.int16)
    ids_cp.wait()
    mask_cp.wait()
    masked = jnp.where(mask_in[...] > 0, ids_in[...], -1)
    ids_pkt[0:FAN, :] = masked.astype(jnp.int16)
    for g in range(2):
        ids_s32[OWN + g, 0:FAN, :] = masked[:, g * LANES : (g + 1) * LANES]
        spread_ids(ids_s32, idb, wb, inv, OWN + g)
    for cp in w1_cps:
        cp.wait()
    w1t[0:HID, :] = ws1[...].T
    w1t[HID:, :] = wn1[...].T

    pl.semaphore_wait(barrier, 4)
    sends = []
    id_copies = [remote(ids_pkt, ids_rcv.at[s], ids_ss.at[s], ids_rs.at[s], peers[s]) for s in range(3)]
    for cp in id_copies:
        cp.start()
    sends += id_copies

    def build_own(tile):
        def put(half, g):
            def store(r, v):
                v = v if half else v * jnp.array(16.0, BF)
                row = tile % 2 * (TILE // 8) + r
                a_own[half * 4 + tile // 2, row : row + 8, :, g * LANES : (g + 1) * LANES] = v

            return store

        for g in range(2):
            build_tile(tile, row_ids, idb, wb, OWN + g, put(0, g), put(1, g))

    for cp in x_copies:
        cp.wait()
    y_copies, s_copies = [], []
    for i in range(4):
        b = 2 * i + 1 - core
        part = jnp.dot(w1t[...], x_v[b], preferred_element_type=F32)
        yown[b] = part[HID:].astype(BF)
        ssend[i] = part[:HID].astype(BF)
        build_own(2 * i)
        y_copies.append(remote(yown.at[b], yrecv.at[b], y_ss.at[2 * i], y_rs.at[2 * i + 1], partner))
        s_copies.append(remote(ssend.at[i], srecv.at[i], s_ss.at[i], s_rs.at[i], partner))
        b2 = 2 * i + core
        part2 = jnp.dot(w1t[...], x_v[b2], preferred_element_type=F32)
        yown[b2] = part2[HID:].astype(BF)
        sown[i] = part2[:HID]
        y_copies.append(remote(yown.at[b2], yrecv.at[b2], y_ss.at[2 * i + 1], y_rs.at[2 * i], partner))
        y_copies[-2].start()
        y_copies[-1].start()
        build_own(2 * i + 1)
    for cp in s_copies:
        cp.start()
    sends += y_copies + s_copies
    for cp in late_cps:
        cp.wait()
    w2st[...] = ws2[...].T
    w2nt[...] = wn2[...].T

    def build_into(flat):
        def put(half):
            def store(r, v):
                ring[flat % RING, half, r : r + 8] = v

            return store

        build_tile(flat % 8, row_ids, idb, wb, flat // 8, put(0), put(1))

    def dot_from(flat):
        tile = flat % 8
        cols = slice(tile % 2 * TILE, (tile % 2 + 1) * TILE)
        low = ring[flat % RING, 0].reshape(TILE, LANES)
        high = ring[flat % RING, 1].reshape(TILE, LANES)
        return (
            jnp.dot(ysum[tile // 2, :, cols], low, preferred_element_type=F32),
            jnp.dot(ysum[4 + tile // 2, :, cols], high, preferred_element_type=F32),
        )

    def lanes(g):
        return slice(g * LANES, (g + 1) * LANES)

    def quarter(q):
        return slice(q * Q, (q + 1) * Q)

    def take_ids(s):
        id_copies[s].wait_recv()
        for u, pair in enumerate(UNITS):
            for half, (slot, q) in enumerate(pair):
                if slot == s:
                    ids_s32[u, :, quarter(half)] = ids_rcv[s, :, quarter(q)].astype(jnp.int32)

    chip_me = me // 2
    rs_copies = {}
    started1 = []

    def finish_unit(u, low, high):
        total = (low * 16.0 + high) * jnp.broadcast_to(inv[u, 0:1, :], (HID, LANES))
        for half, (s, q) in enumerate(UNITS[u]):
            chip = peers[s] // 2
            part = total[:, quarter(half)] + sown[chip, :, quarter(q)] + srecv[chip, :, quarter(q)].astype(F32)
            rs_send[s, q] = part.astype(BF)
            rs_copies[s, q] = remote(rs_send.at[s, q], rs_recv.at[s, q], r_ss.at[4 * s + q], r_rs.at[4 * s + q], peers[s])
            rs_copies[s, q].start()

    def gather_start(h, ss, rs, p):
        outs = [remote(h.at[me, p], h.at[me, p], ss.at[7 * p + t], rs.at[7 * p + t], peers[t]) for t in range(3)]
        outs.append(remote(h.at[me, p], h.at[me, p], ss.at[7 * p + 3], rs.at[7 * p + 3], partner))
        for cp in outs:
            cp.start()
        return outs

    def finish_quarter(q):
        z = zbase[q // 2, :, quarter(q % 2)]
        for t in (1, 2, 0):
            rs_copies[t, q].wait_recv()
            z = z + rs_recv[t, q].astype(F32)
        h1[me, q] = jnp.maximum(z, 0.0).astype(BF)
        started1.append(gather_start(h1, g1_ss, g1_rs, q))

    def own_base(g, own):
        base = own * jnp.broadcast_to(inv[OWN + g, 0:1, :], (HID, LANES))
        zbase[g] = base + sown[chip_me, :, lanes(g)] + srecv[chip_me, :, lanes(g)].astype(F32)

    take_ids(2)
    take_ids(1)
    spread_ids(ids_s32, idb, wb, inv, 0)
    lead = 3
    for flat in range(lead):
        build_into(flat)
    for cp in y_copies:
        cp.wait_recv()
    for b in range(N_DEV):
        ysum[b] = yown[b] + yrecv[b]
    take_ids(0)
    built = lead
    low = high = own = None
    for flat in range(48):
        u, tile = flat // 8, flat % 8
        while built < 48 and built - flat < 2 or (built < 48 and tile % 2 == 0 and built - flat < lead):
            if built % 8 == 0:
                spread_ids(ids_s32, idb, wb, inv, built // 8)
            build_into(built)
            built += 1
        part = dot_from(flat)
        low = part[0] if low is None else low + part[0]
        high = part[1] if high is None else high + part[1]
        if u in (1, 3):
            piece = jnp.dot(ysum[tile], a_own[tile, :, :, lanes(u // 2)].reshape(BLK, LANES), preferred_element_type=F32)
            own = piece if own is None else own + piece
        if tile == 7:
            if u == 0:
                for cp in s_copies:
                    cp.wait_recv()
            finish_unit(u, low, high)
            low = high = None
            if u in (1, 3):
                own_base(u // 2, own)
                own = None
            if u == 4:
                finish_quarter(0)
    finish_quarter(1)
    finish_quarter(2)
    finish_quarter(3)
    sends += list(rs_copies.values())

    inv_own = jnp.concatenate(
        [jnp.broadcast_to(inv[OWN + g, 0:1, :], (HID, LANES)) for g in range(2)], axis=1
    )

    def own_dot(h, b, p, size):
        rows = a_own[b, p * size // 8 : (p + 1) * size // 8].reshape(size, BLK)
        return jnp.dot(h[b, p], rows, preferred_element_type=F32)

    def gather_finish(h, ss, rs, started, size):
        pieces = BLK // size
        acc[...] = sum(own_dot(h, me, p, size) for p in range(pieces))
        forwards = []

        def take_forwards(p):
            for fwd in forwards[p]:
                fwd.wait_recv()
            acc[...] += sum(own_dot(h, peers[t] + 1 - 2 * core, p, size) for t in range(3))

        for p in range(pieces):
            group = []
            for t in (1, 2, 0):
                started[p][t].wait_recv()
                fwd = remote(
                    h.at[peers[t], p], h.at[peers[t], p], ss.at[7 * p + 4 + t], rs.at[7 * p + 4 + t], partner
                )
                fwd.start()
                group.append(fwd)
            forwards.append(group)
            started[p][3].wait_recv()
            acc[...] += sum(own_dot(h, dev, p, size) for dev in (*peers, partner))
            if p > 0:
                take_forwards(p - 1)
        take_forwards(pieces - 1)
        return [cp for outs in started for cp in outs] + [cp for group in forwards for cp in group]

    sends += gather_finish(h1, g1_ss, g1_rs, started1, Q)

    started2 = []
    for g in range(2):
        mean1 = (acc[:, lanes(g)] * inv_own[:, lanes(g)]).astype(BF)
        mine = jnp.concatenate([h1[me, 2 * g], h1[me, 2 * g + 1]], axis=1)
        pre2 = jnp.dot(w2st[...], mine, preferred_element_type=F32) + jnp.dot(
            w2nt[...], mean1, preferred_element_type=F32
        )
        h2[me, g] = jnp.maximum(pre2, 0.0).astype(BF)
        started2.append(gather_start(h2, g2_ss, g2_rs, g))
    for g in range(2):
        out_ref[:, lanes(g)] = jnp.dot(ws3t[...], h2[me, g], preferred_element_type=F32)
    sends += gather_finish(h2, g2_ss, g2_rs, started2, LANES)
    for g in range(2):
        mean2 = (acc[:, lanes(g)] * inv_own[:, lanes(g)]).astype(BF)
        out_ref[:, lanes(g)] += jnp.dot(wn3t[...], mean2, preferred_element_type=F32)
    for cp in sends:
        cp.wait_send()


def solution(mesh):
    def device_step(feat, ws1, wn1, ids, mask, ws2, wn2, ws3, wn3):
        vm = pl.BlockSpec(memory_space=pltpu.VMEM)
        dma = pltpu.SemaphoreType.DMA
        out_t = pl.pallas_call(
            kernel,
            out_shape=jax.ShapeDtypeStruct((7, BLK), F32),
            in_specs=[pl.BlockSpec(memory_space=pl.ANY)] * 9,
            out_specs=vm,
            scratch_shapes=[
                pltpu.VMEM((N_DEV, 192, BLK), BF),
                pltpu.VMEM((192, HID), BF),
                pltpu.VMEM((192, HID), BF),
                pltpu.VMEM((FAN, BLK), jnp.int32),
                pltpu.VMEM((FAN, BLK), jnp.int32),
                pltpu.VMEM((HID, HID), BF),
                pltpu.VMEM((HID, HID), BF),
                pltpu.VMEM((7, HID), BF),
                pltpu.VMEM((7, HID), BF),
                pltpu.VMEM((2 * HID, 192), BF),
                pltpu.VMEM((HID, HID), BF),
                pltpu.VMEM((HID, HID), BF),
                pltpu.VMEM((N_DEV, HID, BLK), BF),
                pltpu.VMEM((N_DEV, HID, BLK), BF),
                pltpu.VMEM((N_DEV, HID, BLK), BF),
                pltpu.VMEM((4, HID, BLK), F32),
                pltpu.VMEM((4, HID, BLK), BF),
                pltpu.VMEM((4, HID, BLK), BF),
                pltpu.VMEM((16, BLK), jnp.int16),
                pltpu.VMEM((3, 16, BLK), jnp.int16),
                pltpu.VMEM((8, 16, LANES), jnp.int32),
                pltpu.VMEM((HALF // TILE, TILE // 8, 8, LANES), jnp.int16),
                pltpu.VMEM((8, FAN, 8, LANES), jnp.int16),
                pltpu.VMEM((8, FAN, 8, LANES), BF),
                pltpu.VMEM((8, 8, LANES), F32),
                pltpu.VMEM((RING, 2, TILE // 8, 8, LANES), BF),
                pltpu.VMEM((N_DEV, BLK // 8, 8, BLK), BF),
                pltpu.VMEM((HID, BLK), F32),
                pltpu.VMEM((2, HID, LANES), F32),
                pltpu.VMEM((3, 4, HID, Q), BF),
                pltpu.VMEM((3, 4, HID, Q), BF),
                pltpu.VMEM((N_DEV, 4, HID, Q), BF),
                pltpu.VMEM((N_DEV, 2, HID, LANES), BF),
                dma((8,)),
                dma((N_DEV,)),
                dma((3,)), dma((3,)),
                dma((8,)), dma((8,)),
                dma((4,)), dma((4,)),
                dma((12,)), dma((12,)),
                dma((28,)), dma((28,)),
                dma((14,)), dma((14,)),
            ],
            compiler_params=pltpu.CompilerParams(
                collective_id=0, has_side_effects=True, vmem_limit_bytes=60 * 1024 * 1024
            ),
            name="graphsage",
        )(feat.T, ws1, wn1, ids.T, mask.T, ws2, wn2, ws3.T, wn3.T)
        return out_t.T

    col_split = P(None, "g")
    row_split = P("g", None)
    replicated = P()
    return jax.shard_map(
        device_step,
        mesh=mesh,
        in_specs=(col_split, row_split, row_split, row_split, row_split, replicated, replicated, replicated, replicated),
        out_specs=row_split,
        check_vma=False,
    )
```

```python
import jax
import jax.numpy as jnp
from jax import lax
from jax.experimental import pallas as pl
from jax.experimental.pallas import tpu as pltpu
from jax.sharding import PartitionSpec as P

MESH = pl.DeviceIdType.MESH
N_DEV = 8
NODES = 4096
BLK = NODES // N_DEV
HALF = NODES // 2
FAN = 10
HID = 128
TILE = 256
LANES = 256
BF = jnp.bfloat16
F32 = jnp.float32


UNITS = (((0, 0), (0, 1)), ((2, 0), (1, 0)), ((2, 1), (1, 1)), ((0, 2), (0, 3)), ((2, 2), (1, 2)), ((2, 3), (1, 3)))
OWN = 6
OWN_EARLY = 3
RING = 6
Q = 128


def spread_ids(ids_s32, idb, wb, inv, u):
    words, weights = [], []
    degree = jnp.zeros((8, LANES), F32)
    for k in range(FAN):
        raw = jnp.broadcast_to(ids_s32[u, k : k + 1, :], (8, LANES))
        valid = raw >= 0
        degree += jnp.where(valid, 1.0, 0.0)
        upper = raw >= HALF
        word = jnp.where(upper, raw - HALF, raw)
        weight = jnp.where(valid, jnp.where(upper, 1.0, 0.0625), 0.0)
        for m in range(k):
            same = word == words[m]
            weights[m] = weights[m] + jnp.where(same, weight, 0.0)
            word = jnp.where(same, -1, word)
        words.append(word)
        weights.append(weight)
    inv[u] = 1.0 / degree
    for k in range(FAN):
        idb[u, k] = words[k].astype(jnp.int16)
        wb[u, k] = weights[k].astype(BF)


def build_tile(tile, row_ids, idb, wb, u, store_low, store_high):
    ids = [idb[u, k] for k in range(FAN)]
    wts = [wb[u, k] for k in range(FAN)]
    for r in range(0, TILE // 8, 8):
        rows = row_ids[tile, r : r + 8]
        acc = jnp.zeros((8, 8, LANES), BF)
        for k in range(FAN):
            acc = jnp.where(ids[k][None] == rows, wts[k][None], acc)
        high = jnp.floor(acc)
        store_high(r, high)
        store_low(r, acc - high)


def kernel(
    x_hbm, ws1_hbm, wn1_hbm, ids_hbm, mask_hbm, ws2_hbm, wn2_hbm, ws3_hbm, wn3_hbm, out_ref,
    x_v, ws1, wn1, ids_in, mask_in, ws2, wn2, ws3t, wn3t,
    w1t, w2st, w2nt, yown, yrecv, ysum, sown, ssend, srecv,
    ids_pkt, ids_rcv, ids_s32, row_ids, idb, wb, inv,
    ring, a_own, acc, zbase, rs_send, rs_recv, h1, h2,
    in_sem, x_sem, ids_ss, ids_rs, y_ss, y_rs, s_ss, s_rs, r_ss, r_rs, g1_ss, g1_rs, g2_ss, g2_rs,
):
    me = lax.axis_index("g")
    core = lax.rem(me, 2)
    cx = lax.rem(me // 2, 2)
    cy = me // 4
    partner = me + 1 - 2 * core
    steps = (6 - 4 * cx - 8 * cy, 4 - 8 * cy, 2 - 4 * cx)
    peers = tuple(partner + step for step in steps)
    mates = tuple(me + step for step in steps)
    mine, theirs = (me, *peers), (partner, *mates)

    barrier = pltpu.get_barrier_semaphore()
    for peer in (*peers, partner):
        pl.semaphore_signal(barrier, inc=1, device_id=(peer,), device_id_type=MESH)

    def fetch(src, dst, i):
        cp = pltpu.make_async_copy(src, dst, in_sem.at[i])
        cp.start()
        return cp

    ids_cp = fetch(ids_hbm, ids_in, 0)
    mask_cp = fetch(mask_hbm, mask_in, 1)
    w1_cps = [fetch(ws1_hbm, ws1, 2), fetch(wn1_hbm, wn1, 3)]
    x_copies = []
    for b in range(N_DEV):
        cp = pltpu.make_async_copy(x_hbm.at[:, pl.ds(b * BLK, BLK)], x_v.at[b], x_sem.at[b])
        cp.start()
        x_copies.append(cp)
    late_cps = [fetch(ws2_hbm, ws2, 4), fetch(wn2_hbm, wn2, 5), fetch(ws3_hbm, ws3t, 6), fetch(wn3_hbm, wn3t, 7)]

    def remote(src, dst, ss, rs, dev):
        return pltpu.make_async_remote_copy(
            src_ref=src, dst_ref=dst, send_sem=ss, recv_sem=rs, device_id=(dev,), device_id_type=MESH
        )

    row_shape = (TILE // 8, 8, LANES)
    row_base = lax.broadcasted_iota(jnp.int32, row_shape, 0) * 8 + lax.broadcasted_iota(jnp.int32, row_shape, 1)
    for tile in range(HALF // TILE):
        row_ids[tile] = (row_base + tile * TILE).astype(jnp.int16)
    ids_pkt[...] = jnp.full(ids_pkt.shape, -1, jnp.int16)
    ids_cp.wait()
    mask_cp.wait()
    masked = jnp.where(mask_in[...] > 0, ids_in[...], -1)
    ids_pkt[0:FAN, :] = masked.astype(jnp.int16)
    for g in range(2):
        ids_s32[OWN + g, 0:FAN, :] = masked[:, g * LANES : (g + 1) * LANES]
        spread_ids(ids_s32, idb, wb, inv, OWN + g)
    for cp in w1_cps:
        cp.wait()
    w1t[0:HID, :] = ws1[...].T
    w1t[HID:, :] = wn1[...].T

    pl.semaphore_wait(barrier, 4)
    sends = []
    id_copies = [remote(ids_pkt, ids_rcv.at[s], ids_ss.at[s], ids_rs.at[s], peers[s]) for s in range(3)]
    for cp in id_copies:
        cp.start()
    sends += id_copies

    def build_own(tile):
        def put(half, g):
            def store(r, v):
                v = v if half else v * jnp.array(16.0, BF)
                row = tile % 2 * (TILE // 8) + r
                a_own[half * 4 + tile // 2, row : row + 8, :, g * LANES : (g + 1) * LANES] = v

            return store

        for g in range(2):
            build_tile(tile, row_ids, idb, wb, OWN + g, put(0, g), put(1, g))

    for cp in x_copies:
        cp.wait()
    y_copies, s_copies = [], []
    for i in range(4):
        part = jnp.dot(w1t[...], x_v[theirs[i]], preferred_element_type=F32)
        yown[theirs[i]] = part[HID:].astype(BF)
        ssend[i] = part[:HID].astype(BF)
        part2 = jnp.dot(w1t[...], x_v[mine[i]], preferred_element_type=F32)
        yown[mine[i]] = part2[HID:].astype(BF)
        sown[i] = part2[:HID]
        for j, b in enumerate((theirs[i], mine[i])):
            y_copies.append(remote(yown.at[b], yrecv.at[b], y_ss.at[2 * i + j], y_rs.at[2 * i + j], partner))
            y_copies[-1].start()
        s_copies.append(remote(ssend.at[i], srecv.at[i], s_ss.at[i], s_rs.at[i], partner))
        if i < OWN_EARLY:
            build_own(i)
    for cp in s_copies:
        cp.start()
    sends += y_copies + s_copies
    for tile in range(OWN_EARLY, 8):
        build_own(tile)
    for cp in late_cps:
        cp.wait()
    w2st[...] = ws2[...].T
    w2nt[...] = wn2[...].T

    def build_into(flat):
        def put(half):
            def store(r, v):
                ring[flat % RING, half, r : r + 8] = v

            return store

        build_tile(flat % 8, row_ids, idb, wb, flat // 8, put(0), put(1))

    def dot_from(flat):
        tile = flat % 8
        cols = slice(tile % 2 * TILE, (tile % 2 + 1) * TILE)
        low = ring[flat % RING, 0].reshape(TILE, LANES)
        high = ring[flat % RING, 1].reshape(TILE, LANES)
        return (
            jnp.dot(ysum[tile // 2, :, cols], low, preferred_element_type=F32),
            jnp.dot(ysum[4 + tile // 2, :, cols], high, preferred_element_type=F32),
        )

    def lanes(g):
        return slice(g * LANES, (g + 1) * LANES)

    def quarter(q):
        return slice(q * Q, (q + 1) * Q)

    def take_ids(s):
        id_copies[s].wait_recv()
        for u, pair in enumerate(UNITS):
            for half, (slot, q) in enumerate(pair):
                if slot == s:
                    ids_s32[u, :, quarter(half)] = ids_rcv[s, :, quarter(q)].astype(jnp.int32)

    rs_copies = {}
    started1 = []

    def finish_unit(u, low, high):
        total = (low * 16.0 + high) * jnp.broadcast_to(inv[u, 0:1, :], (HID, LANES))
        for half, (s, q) in enumerate(UNITS[u]):
            part = total[:, quarter(half)] + sown[1 + s, :, quarter(q)] + srecv[1 + s, :, quarter(q)].astype(F32)
            rs_send[s, q] = part.astype(BF)
            rs_copies[s, q] = remote(rs_send.at[s, q], rs_recv.at[s, q], r_ss.at[4 * s + q], r_rs.at[4 * s + q], peers[s])
            rs_copies[s, q].start()

    def gather_start(h, ss, rs, p):
        outs = [remote(h.at[me, p], h.at[me, p], ss.at[7 * p + t], rs.at[7 * p + t], peers[t]) for t in range(3)]
        outs.append(remote(h.at[me, p], h.at[me, p], ss.at[7 * p + 3], rs.at[7 * p + 3], partner))
        for cp in outs:
            cp.start()
        return outs

    def finish_quarter(q):
        z = zbase[q // 2, :, quarter(q % 2)]
        for t in (1, 2, 0):
            rs_copies[t, q].wait_recv()
            z = z + rs_recv[t, q].astype(F32)
        h1[me, q] = jnp.maximum(z, 0.0).astype(BF)
        started1.append(gather_start(h1, g1_ss, g1_rs, q))

    def own_base(g, own):
        base = own * jnp.broadcast_to(inv[OWN + g, 0:1, :], (HID, LANES))
        zbase[g] = base + sown[0, :, lanes(g)] + srecv[0, :, lanes(g)].astype(F32)

    take_ids(0)
    spread_ids(ids_s32, idb, wb, inv, 0)
    lead = 3
    for flat in range(lead):
        build_into(flat)
    for cp in y_copies:
        cp.wait_recv()
    for b in range(N_DEV):
        ysum[b] = yown[b] + yrecv[b]
    take_ids(2)
    take_ids(1)
    built = lead
    low = high = own = None
    for flat in range(48):
        u, tile = flat // 8, flat % 8
        while built < 48 and built - flat < 2 or (built < 48 and tile % 2 == 0 and built - flat < lead):
            if built % 8 == 0:
                spread_ids(ids_s32, idb, wb, inv, built // 8)
            build_into(built)
            built += 1
        part = dot_from(flat)
        low = part[0] if low is None else low + part[0]
        high = part[1] if high is None else high + part[1]
        if u in (1, 3):
            piece = jnp.dot(ysum[tile], a_own[tile, :, :, lanes(u // 2)].reshape(BLK, LANES), preferred_element_type=F32)
            own = piece if own is None else own + piece
        if tile == 7:
            if u == 0:
                for cp in s_copies:
                    cp.wait_recv()
            finish_unit(u, low, high)
            low = high = None
            if u in (1, 3):
                own_base(u // 2, own)
                own = None
            if u == 4:
                finish_quarter(0)
    finish_quarter(1)
    finish_quarter(2)
    finish_quarter(3)
    sends += list(rs_copies.values())

    inv_own = jnp.concatenate(
        [jnp.broadcast_to(inv[OWN + g, 0:1, :], (HID, LANES)) for g in range(2)], axis=1
    )

    def own_dot(h, b, p, size):
        rows = a_own[b, p * size // 8 : (p + 1) * size // 8].reshape(size, BLK)
        return jnp.dot(h[b, p], rows, preferred_element_type=F32)

    def gather_finish(h, ss, rs, started, size, old_sends):
        pieces = BLK // size
        acc[...] = sum(own_dot(h, me, p, size) for p in range(pieces))
        for cp in old_sends:
            cp.wait_send()
        forwards = []

        def take_forwards(p):
            for fwd in forwards[p]:
                fwd.wait_recv()
            acc[...] += sum(own_dot(h, mate, p, size) for mate in mates)

        for p in range(pieces):
            group = []
            for t in (1, 2, 0):
                started[p][t].wait_recv()
                fwd = remote(
                    h.at[peers[t], p], h.at[peers[t], p], ss.at[7 * p + 4 + t], rs.at[7 * p + 4 + t], partner
                )
                fwd.start()
                group.append(fwd)
            forwards.append(group)
            started[p][3].wait_recv()
            acc[...] += sum(own_dot(h, dev, p, size) for dev in (*peers, partner))
            if p > 0:
                take_forwards(p - 1)
        take_forwards(pieces - 1)
        return [cp for outs in started for cp in outs] + [cp for group in forwards for cp in group]

    sends = gather_finish(h1, g1_ss, g1_rs, started1, Q, sends)

    started2 = []
    for g in range(2):
        mean1 = (acc[:, lanes(g)] * inv_own[:, lanes(g)]).astype(BF)
        mine = jnp.concatenate([h1[me, 2 * g], h1[me, 2 * g + 1]], axis=1)
        pre2 = jnp.dot(w2st[...], mine, preferred_element_type=F32) + jnp.dot(
            w2nt[...], mean1, preferred_element_type=F32
        )
        h2[me, g] = jnp.maximum(pre2, 0.0).astype(BF)
        started2.append(gather_start(h2, g2_ss, g2_rs, g))
    for g in range(2):
        out_ref[:, lanes(g)] = jnp.dot(ws3t[...], h2[me, g], preferred_element_type=F32)
    sends = gather_finish(h2, g2_ss, g2_rs, started2, LANES, sends)
    for g in range(2):
        mean2 = (acc[:, lanes(g)] * inv_own[:, lanes(g)]).astype(BF)
        out_ref[:, lanes(g)] += jnp.dot(wn3t[...], mean2, preferred_element_type=F32)
    for cp in sends:
        cp.wait_send()


def solution(mesh):
    def device_step(feat, ws1, wn1, ids, mask, ws2, wn2, ws3, wn3):
        vm = pl.BlockSpec(memory_space=pltpu.VMEM)
        dma = pltpu.SemaphoreType.DMA
        out_t = pl.pallas_call(
            kernel,
            out_shape=jax.ShapeDtypeStruct((7, BLK), F32),
            in_specs=[pl.BlockSpec(memory_space=pl.ANY)] * 9,
            out_specs=vm,
            scratch_shapes=[
                pltpu.VMEM((N_DEV, 192, BLK), BF),
                pltpu.VMEM((192, HID), BF),
                pltpu.VMEM((192, HID), BF),
                pltpu.VMEM((FAN, BLK), jnp.int32),
                pltpu.VMEM((FAN, BLK), jnp.int32),
                pltpu.VMEM((HID, HID), BF),
                pltpu.VMEM((HID, HID), BF),
                pltpu.VMEM((7, HID), BF),
                pltpu.VMEM((7, HID), BF),
                pltpu.VMEM((2 * HID, 192), BF),
                pltpu.VMEM((HID, HID), BF),
                pltpu.VMEM((HID, HID), BF),
                pltpu.VMEM((N_DEV, HID, BLK), BF),
                pltpu.VMEM((N_DEV, HID, BLK), BF),
                pltpu.VMEM((N_DEV, HID, BLK), BF),
                pltpu.VMEM((4, HID, BLK), F32),
                pltpu.VMEM((4, HID, BLK), BF),
                pltpu.VMEM((4, HID, BLK), BF),
                pltpu.VMEM((16, BLK), jnp.int16),
                pltpu.VMEM((3, 16, BLK), jnp.int16),
                pltpu.VMEM((8, 16, LANES), jnp.int32),
                pltpu.VMEM((HALF // TILE, TILE // 8, 8, LANES), jnp.int16),
                pltpu.VMEM((8, FAN, 8, LANES), jnp.int16),
                pltpu.VMEM((8, FAN, 8, LANES), BF),
                pltpu.VMEM((8, 8, LANES), F32),
                pltpu.VMEM((RING, 2, TILE // 8, 8, LANES), BF),
                pltpu.VMEM((N_DEV, BLK // 8, 8, BLK), BF),
                pltpu.VMEM((HID, BLK), F32),
                pltpu.VMEM((2, HID, LANES), F32),
                pltpu.VMEM((3, 4, HID, Q), BF),
                pltpu.VMEM((3, 4, HID, Q), BF),
                pltpu.VMEM((N_DEV, 4, HID, Q), BF),
                pltpu.VMEM((N_DEV, 2, HID, LANES), BF),
                dma((8,)),
                dma((N_DEV,)),
                dma((3,)), dma((3,)),
                dma((8,)), dma((8,)),
                dma((4,)), dma((4,)),
                dma((12,)), dma((12,)),
                dma((28,)), dma((28,)),
                dma((14,)), dma((14,)),
            ],
            compiler_params=pltpu.CompilerParams(
                collective_id=0, has_side_effects=True, vmem_limit_bytes=60 * 1024 * 1024
            ),
            name="graphsage",
        )(feat.T, ws1, wn1, ids.T, mask.T, ws2, wn2, ws3.T, wn3.T)
        return out_t.T

    col_split = P(None, "g")
    row_split = P("g", None)
    replicated = P()
    return jax.shard_map(
        device_step,
        mesh=mesh,
        in_specs=(col_split, row_split, row_split, row_split, row_split, replicated, replicated, replicated, replicated),
        out_specs=row_split,
        check_vma=False,
    )
```

```python
import jax
import jax.numpy as jnp
from jax import lax
from jax.experimental import pallas as pl
from jax.experimental.pallas import tpu as pltpu
from jax.sharding import PartitionSpec as P

MESH = pl.DeviceIdType.MESH
N_DEV = 8
NODES = 4096
BLK = NODES // N_DEV
HALF = NODES // 2
FAN = 10
HID = 128
TILE = 256
LANES = 256
BF = jnp.bfloat16
F32 = jnp.float32


UNITS = (((2, 0), (1, 0)), ((0, 0), (0, 1)), ((0, 2), (0, 3)), ((2, 1), (1, 1)), ((2, 2), (1, 2)), ((2, 3), (1, 3)))
OWN = 6
OWN_EARLY = 3
RING = 6
PENDING = ((34, 0), (35, 1), (44, 2))
Q = 128


def spread_ids(ids_s32, idb, wb, inv, u):
    words, weights = [], []
    degree = jnp.zeros((8, LANES), F32)
    for k in range(FAN):
        raw = jnp.broadcast_to(ids_s32[u, k : k + 1, :], (8, LANES))
        valid = raw >= 0
        degree += jnp.where(valid, 1.0, 0.0)
        upper = raw >= HALF
        word = jnp.where(upper, raw - HALF, raw)
        weight = jnp.where(valid, jnp.where(upper, 1.0, 0.0625), 0.0)
        for m in range(k):
            same = word == words[m]
            weights[m] = weights[m] + jnp.where(same, weight, 0.0)
            word = jnp.where(same, -1, word)
        words.append(word)
        weights.append(weight)
    inv[u] = 1.0 / degree
    for k in range(FAN):
        idb[u, k] = words[k].astype(jnp.int16)
        wb[u, k] = weights[k].astype(BF)


def build_tile(tile, row_ids, idb, wb, u, store_low, store_high):
    ids = [idb[u, k] for k in range(FAN)]
    wts = [wb[u, k] for k in range(FAN)]
    for r in range(0, TILE // 8, 8):
        rows = row_ids[tile, r : r + 8]
        acc = jnp.zeros((8, 8, LANES), BF)
        for k in range(FAN):
            acc = jnp.where(ids[k][None] == rows, wts[k][None], acc)
        high = jnp.floor(acc)
        store_high(r, high)
        store_low(r, acc - high)


def kernel(
    x_hbm, ws1_hbm, wn1_hbm, ids_hbm, mask_hbm, ws2_hbm, wn2_hbm, ws3_hbm, wn3_hbm, out_ref,
    x_v, ws1, wn1, ids_in, mask_in, ws2, wn2, ws3t, wn3t,
    w1t, w2st, w2nt, yown, yrecv, ysum, sown, ssend, srecv,
    ids_pkt, ids_rcv, ids_s32, row_ids, idb, wb, inv,
    ring, a_own, acc, zbase, pend, rs_send, via, rs_recv, h1, h2,
    in_sem, x_sem, ids_ss, ids_rs, y_ss, y_rs, s_ss, s_rs, r_ss, r_rs, g1_ss, g1_rs, g2_ss, g2_rs,
):
    me = lax.axis_index("g")
    core = lax.rem(me, 2)
    cx = lax.rem(me // 2, 2)
    cy = me // 4
    partner = me + 1 - 2 * core
    steps = (6 - 4 * cx - 8 * cy, 4 - 8 * cy, 2 - 4 * cx)
    peers = (me + steps[0], partner + steps[1], partner + steps[2])
    mates = (partner + steps[0], me + steps[1], me + steps[2])
    mine, theirs = (me, *peers), (partner, *mates)

    barrier = pltpu.get_barrier_semaphore()
    for peer in (*peers, partner):
        pl.semaphore_signal(barrier, inc=1, device_id=(peer,), device_id_type=MESH)

    def fetch(src, dst, i):
        cp = pltpu.make_async_copy(src, dst, in_sem.at[i])
        cp.start()
        return cp

    ids_cp = fetch(ids_hbm, ids_in, 0)
    mask_cp = fetch(mask_hbm, mask_in, 1)
    w1_cps = [fetch(ws1_hbm, ws1, 2), fetch(wn1_hbm, wn1, 3)]
    for b in range(N_DEV):
        cp = pltpu.make_async_copy(x_hbm.at[:, pl.ds(b * BLK, BLK)], x_v.at[b], x_sem)
        cp.start()
    late_cps = [fetch(ws2_hbm, ws2, 4), fetch(wn2_hbm, wn2, 5), fetch(ws3_hbm, ws3t, 6), fetch(wn3_hbm, wn3t, 7)]

    def remote(src, dst, ss, rs, dev):
        return pltpu.make_async_remote_copy(
            src_ref=src, dst_ref=dst, send_sem=ss, recv_sem=rs, device_id=(dev,), device_id_type=MESH
        )

    def drain(ref, sem):
        pltpu.make_async_copy(ref, ref, sem).wait()

    row_shape = (TILE // 8, 8, LANES)
    row_base = lax.broadcasted_iota(jnp.int32, row_shape, 0) * 8 + lax.broadcasted_iota(jnp.int32, row_shape, 1)
    for tile in range(HALF // TILE):
        row_ids[tile] = (row_base + tile * TILE).astype(jnp.int16)
    ids_pkt[...] = jnp.full(ids_pkt.shape, -1, jnp.int16)
    ids_cp.wait()
    mask_cp.wait()
    masked = jnp.where(mask_in[...] > 0, ids_in[...], -1)
    ids_pkt[0:FAN, :] = masked.astype(jnp.int16)
    for g in range(2):
        ids_s32[OWN + g, 0:FAN, :] = masked[:, g * LANES : (g + 1) * LANES]
        spread_ids(ids_s32, idb, wb, inv, OWN + g)
    for cp in w1_cps:
        cp.wait()
    w1t[0:HID, :] = ws1[...].T
    w1t[HID:, :] = wn1[...].T

    pl.semaphore_wait(barrier, 4)
    id_copies = [remote(ids_pkt, ids_rcv.at[s], ids_ss, ids_rs.at[s], peers[s]) for s in range(3)]
    for cp in id_copies:
        cp.start()

    def build_own(tile):
        def put(half, g):
            def store(r, v):
                v = v if half else v * jnp.array(16.0, BF)
                row = tile % 2 * (TILE // 8) + r
                a_own[half * 4 + tile // 2, row : row + 8, :, g * LANES : (g + 1) * LANES] = v

            return store

        for g in range(2):
            build_tile(tile, row_ids, idb, wb, OWN + g, put(0, g), put(1, g))

    drain(x_v, x_sem)
    for i in range(4):
        part = jnp.dot(w1t[...], x_v[theirs[i]], preferred_element_type=F32)
        yown[theirs[i]] = part[HID:].astype(BF)
        ssend[i] = part[:HID].astype(BF)
        part2 = jnp.dot(w1t[...], x_v[mine[i]], preferred_element_type=F32)
        yown[mine[i]] = part2[HID:].astype(BF)
        sown[i] = part2[:HID]
        for b in (theirs[i], mine[i]):
            remote(yown.at[b], yrecv.at[b], y_ss, y_rs, partner).start()
        if i < OWN_EARLY:
            build_own(i)
    for i in range(4):
        remote(ssend.at[i], srecv.at[i], s_ss, s_rs, partner).start()
    for tile in range(OWN_EARLY, 8):
        build_own(tile)
    for cp in late_cps:
        cp.wait()
    w2st[...] = ws2[...].T
    w2nt[...] = wn2[...].T

    def build_into(flat):
        def put(half):
            def store(r, v):
                ring[flat % RING, half, r : r + 8] = v

            return store

        build_tile(flat % 8, row_ids, idb, wb, flat // 8, put(0), put(1))

    def dot_from(flat):
        tile = flat % 8
        cols = slice(tile % 2 * TILE, (tile % 2 + 1) * TILE)
        low = ring[flat % RING, 0].reshape(TILE, LANES)
        high = ring[flat % RING, 1].reshape(TILE, LANES)
        return (
            jnp.dot(ysum[tile // 2, :, cols], low, preferred_element_type=F32),
            jnp.dot(ysum[4 + tile // 2, :, cols], high, preferred_element_type=F32),
        )

    def lanes(g):
        return slice(g * LANES, (g + 1) * LANES)

    def quarter(q):
        return slice(q * Q, (q + 1) * Q)

    def take_ids(s):
        id_copies[s].wait_recv()
        for u, pair in enumerate(UNITS):
            for half, (slot, q) in enumerate(pair):
                if slot == s:
                    ids_s32[u, :, quarter(half)] = ids_rcv[s, :, quarter(q)].astype(jnp.int32)

    rs_copies = {}

    def rs_start(s, q, part):
        rs_send[s, q] = part.astype(BF)
        if s == 0:
            copy = remote(rs_send.at[0, q], via.at[q], r_ss, r_rs.at[q], peers[1 if q % 2 else 2])
        else:
            copy = remote(rs_send.at[s, q], rs_recv.at[s - 1, q], r_ss, r_rs.at[4 * s + q], peers[s])
        rs_copies[s, q] = copy
        copy.start()

    def via_slot(q):
        return 2 if q % 2 else 1

    def finish_unit(u, low, high):
        total = (low * 16.0 + high) * jnp.broadcast_to(inv[u, 0:1, :], (HID, LANES))
        for half, (s, q) in enumerate(UNITS[u]):
            part = total[:, quarter(half)] + sown[1 + s, :, quarter(q)] + srecv[1 + s, :, quarter(q)].astype(F32)
            if s == via_slot(q):
                pend[q] = part
            else:
                rs_start(s, q, part)

    def finish_pending(q):
        rs_copies[0, q].wait_recv()
        rs_start(via_slot(q), q, pend[q] + via[q].astype(F32))

    def own_base(g, own):
        base = own * jnp.broadcast_to(inv[OWN + g, 0:1, :], (HID, LANES))
        zbase[g] = base + sown[0, :, lanes(g)] + srecv[0, :, lanes(g)].astype(F32)

    def own_dot(h, b, p):
        rows = a_own[b, p * Q // 8 : (p + 1) * Q // 8].reshape(Q, BLK)
        return jnp.dot(h[b, p], rows, preferred_element_type=F32)

    class Gather:
        def __init__(self, h, ss, rs, direct):
            self.h, self.ss, self.rs, self.direct = h, ss, rs, direct
            self.copies, self.forwards, self.ready = {}, [], []

        def copy(self, block, p, slot, dev):
            return remote(self.h.at[block, p], self.h.at[block, p], self.ss, self.rs.at[7 * p + slot], dev)

        def send(self, slot, p):
            dev = partner if slot == 3 else peers[slot]
            self.copies[slot, p] = self.copy(me, p, slot, dev)
            self.copies[slot, p].start()

        def take(self, slot, p):
            self.copies[slot, p].wait_recv()
            block = partner if slot == 3 else peers[slot]
            if p not in self.direct and slot == (1 if p % 2 else 2):
                self.copies[0, p] = self.copy(block, p, 0, peers[3 - slot])
                self.copies[0, p].start()
            if slot < 3:
                fwd = self.copy(block, p, 4 + slot, partner)
                fwd.start()
                self.forwards.append((slot, p, fwd))
            self.ready.append((block, p))

        def take_forwards(self, n):
            for slot, p, fwd in self.forwards[:n]:
                fwd.wait_recv()
                self.ready.append((mates[slot], p))
            self.forwards = self.forwards[n:]

        def own(self, pieces):
            acc[...] = sum(own_dot(self.h, me, p) for p in range(pieces))

        def add(self):
            acc[...] += sum(own_dot(self.h, b, p) for b, p in self.ready)
            self.ready = []

    g1 = Gather(h1, g1_ss, g1_rs, direct=(3,))
    g2 = Gather(h2, g2_ss, g2_rs, direct=())

    def finish_quarter(q):
        z = zbase[q // 2, :, quarter(q % 2)]
        for t in (1, 2):
            rs_copies[t, q].wait_recv()
            z = z + rs_recv[t - 1, q].astype(F32)
        h1[me, q] = jnp.maximum(z, 0.0).astype(BF)
        for slot in (0, 2, 1, 3) if q in g1.direct else (2, 1, 3):
            g1.send(slot, q)

    take_ids(2)
    take_ids(1)
    spread_ids(ids_s32, idb, wb, inv, 0)
    lead = 3
    for flat in range(lead):
        build_into(flat)
    drain(yrecv, y_rs)
    for b in range(N_DEV):
        ysum[b] = yown[b] + yrecv[b]
    take_ids(0)
    built = lead
    low = high = own = None
    for flat in range(48):
        u, tile = flat // 8, flat % 8
        while built < 48 and built - flat < 2 or (built < 48 and tile % 2 == 0 and built - flat < lead):
            if built % 8 == 0:
                spread_ids(ids_s32, idb, wb, inv, built // 8)
            build_into(built)
            built += 1
        part = dot_from(flat)
        low = part[0] if low is None else low + part[0]
        high = part[1] if high is None else high + part[1]
        if u in (1, 3):
            piece = jnp.dot(ysum[tile], a_own[tile, :, :, lanes(u // 2)].reshape(BLK, LANES), preferred_element_type=F32)
            own = piece if own is None else own + piece
        if tile == 7:
            if u == 0:
                drain(srecv, s_rs)
            finish_unit(u, low, high)
            low = high = None
            if u in (1, 3):
                own_base(u // 2, own)
                own = None
        for when, q in PENDING:
            if flat == when:
                finish_pending(q)
    finish_pending(3)
    finish_quarter(0)
    finish_quarter(1)
    finish_quarter(2)
    g1.own(3)
    g1.take(2, 0)
    g1.take(1, 0)
    finish_quarter(3)
    g1.ready.append((me, 3))
    for slot, p in ((1, 1), (2, 1), (2, 2), (1, 2)):
        g1.take(slot, p)
    for p in range(4):
        g1.take(3, p)
    g1.add()
    g1.take(0, 0)
    g1.take(0, 1)
    g1.take_forwards(6)
    g1.add()
    for slot, p in ((2, 3), (1, 3), (0, 3), (0, 2)):
        g1.take(slot, p)
    g1.add()
    g1.take_forwards(4)
    g1.add()
    g1.take_forwards(2)
    g1.add()

    inv_own = jnp.concatenate(
        [jnp.broadcast_to(inv[OWN + g, 0:1, :], (HID, LANES)) for g in range(2)], axis=1
    )
    for g in range(2):
        mean1 = (acc[:, lanes(g)] * inv_own[:, lanes(g)]).astype(BF)
        block = jnp.concatenate([h1[me, 2 * g], h1[me, 2 * g + 1]], axis=1)
        pre2 = jnp.dot(w2st[...], block, preferred_element_type=F32) + jnp.dot(
            w2nt[...], mean1, preferred_element_type=F32
        )
        for half in range(2):
            h2[me, 2 * g + half] = jnp.maximum(pre2[:, quarter(half)], 0.0).astype(BF)
        g2.send(2, 2 * g)
        g2.send(1, 2 * g + 1)
    for slot, p in ((2, 1), (1, 0), (2, 3), (1, 2)):
        g2.send(slot, p)
    for p in range(4):
        g2.send(3, p)
    g2.own(4)
    for g in range(2):
        block = jnp.concatenate([h2[me, 2 * g], h2[me, 2 * g + 1]], axis=1)
        out_ref[:, lanes(g)] = jnp.dot(ws3t[...], block, preferred_element_type=F32)
    drain(ids_rcv, ids_ss)
    drain(yown, y_ss)
    drain(ssend, s_ss)
    drain(rs_send, r_ss)
    drain(h1.at[0:7], g1_ss)
    for p in range(4):
        g2.take(3, p)
    g2.add()
    for slot, p in ((2, 0), (1, 1), (2, 2), (1, 3)):
        g2.take(slot, p)
    g2.add()
    for slot, p in ((2, 1), (1, 0), (2, 3), (1, 2)):
        g2.take(slot, p)
    g2.take_forwards(4)
    g2.add()
    g2.take(0, 0)
    g2.take(0, 1)
    g2.take_forwards(4)
    g2.add()
    g2.take(0, 2)
    g2.take(0, 3)
    g2.take_forwards(2)
    g2.add()
    g2.take_forwards(2)
    g2.add()
    for g in range(2):
        mean2 = (acc[:, lanes(g)] * inv_own[:, lanes(g)]).astype(BF)
        out_ref[:, lanes(g)] += jnp.dot(wn3t[...], mean2, preferred_element_type=F32)
    drain(h2.at[0:7], g2_ss)


def solution(mesh):
    def device_step(feat, ws1, wn1, ids, mask, ws2, wn2, ws3, wn3):
        operands = (feat.T, ws1, wn1, ids.T, mask.T, ws2, wn2, ws3.T, wn3.T)
        vm = pl.BlockSpec(memory_space=pltpu.VMEM)
        dma = pltpu.SemaphoreType.DMA
        out_t = pl.pallas_call(
            kernel,
            out_shape=jax.ShapeDtypeStruct((7, BLK), F32),
            in_specs=[pl.BlockSpec(memory_space=pltpu.HBM)] * 9,
            out_specs=vm,
            scratch_shapes=[
                pltpu.VMEM((N_DEV, 192, BLK), BF),
                pltpu.VMEM((192, HID), BF),
                pltpu.VMEM((192, HID), BF),
                pltpu.VMEM((FAN, BLK), jnp.int32),
                pltpu.VMEM((FAN, BLK), jnp.int32),
                pltpu.VMEM((HID, HID), BF),
                pltpu.VMEM((HID, HID), BF),
                pltpu.VMEM((7, HID), BF),
                pltpu.VMEM((7, HID), BF),
                pltpu.VMEM((2 * HID, 192), BF),
                pltpu.VMEM((HID, HID), BF),
                pltpu.VMEM((HID, HID), BF),
                pltpu.VMEM((N_DEV, HID, BLK), BF),
                pltpu.VMEM((N_DEV, HID, BLK), BF),
                pltpu.VMEM((N_DEV, HID, BLK), BF),
                pltpu.VMEM((4, HID, BLK), F32),
                pltpu.VMEM((4, HID, BLK), BF),
                pltpu.VMEM((4, HID, BLK), BF),
                pltpu.VMEM((16, BLK), jnp.int16),
                pltpu.VMEM((3, 16, BLK), jnp.int16),
                pltpu.VMEM((8, 16, LANES), jnp.int32),
                pltpu.VMEM((HALF // TILE, TILE // 8, 8, LANES), jnp.int16),
                pltpu.VMEM((8, FAN, 8, LANES), jnp.int16),
                pltpu.VMEM((8, FAN, 8, LANES), BF),
                pltpu.VMEM((8, 8, LANES), F32),
                pltpu.VMEM((RING, 2, TILE // 8, 8, LANES), BF),
                pltpu.VMEM((N_DEV, BLK // 8, 8, BLK), BF),
                pltpu.VMEM((HID, BLK), F32),
                pltpu.VMEM((2, HID, LANES), F32),
                pltpu.VMEM((4, HID, Q), F32),
                pltpu.VMEM((3, 4, HID, Q), BF),
                pltpu.VMEM((4, HID, Q), BF),
                pltpu.VMEM((2, 4, HID, Q), BF),
                pltpu.VMEM((N_DEV, 4, HID, Q), BF),
                pltpu.VMEM((N_DEV, 4, HID, Q), BF),
                dma((8,)),
                dma,
                dma, dma((3,)),
                dma, dma,
                dma, dma,
                dma, dma((12,)),
                dma, dma((28,)),
                dma, dma((28,)),
            ],
            compiler_params=pltpu.CompilerParams(
                collective_id=0, has_side_effects=True, vmem_limit_bytes=32 * 1024 * 1024
            ),
            name="graphsage",
        )(*(pltpu.with_memory_space_constraint(a, pltpu.HBM) for a in operands))
        return out_t.T

    col_split = P(None, "g")
    row_split = P("g", None)
    replicated = P()
    return jax.shard_map(
        device_step,
        mesh=mesh,
        in_specs=(col_split, row_split, row_split, row_split, row_split, replicated, replicated, replicated, replicated),
        out_specs=row_split,
        check_vma=False,
    )
```

```python
import jax
import jax.numpy as jnp
from jax import lax
from jax.experimental import pallas as pl
from jax.experimental.pallas import tpu as pltpu
from jax.sharding import PartitionSpec as P

MESH = pl.DeviceIdType.MESH
N_DEV = 8
NODES = 4096
BLK = NODES // N_DEV
HALF = NODES // 2
FAN = 10
HID = 128
TILE = 256
LANES = 256
BF = jnp.bfloat16
F32 = jnp.float32


UNITS = (((2, 2), (1, 2)), ((0, 0), (0, 1)), ((0, 2), (0, 3)), ((2, 0), (1, 0)), ((2, 1), (1, 1)), ((2, 3), (1, 3)))
OWN = 6
OWN_EARLY = 3
RING = 6
PENDING = ((40, 0), (41, 1), (47, 2), (47, 3))
Q = 128


def spread_ids(ids_s32, idb, wb, inv, u):
    words, weights = [], []
    degree = jnp.zeros((8, LANES), F32)
    for k in range(FAN):
        raw = jnp.broadcast_to(ids_s32[u, k : k + 1, :], (8, LANES))
        valid = raw >= 0
        degree += jnp.where(valid, 1.0, 0.0)
        upper = raw >= HALF
        word = jnp.where(upper, raw - HALF, raw)
        weight = jnp.where(valid, jnp.where(upper, 1.0, 0.0625), 0.0)
        for m in range(k):
            same = word == words[m]
            weights[m] = weights[m] + jnp.where(same, weight, 0.0)
            word = jnp.where(same, -1, word)
        words.append(word)
        weights.append(weight)
    inv[u] = 1.0 / degree
    for k in range(FAN):
        idb[u, k] = words[k].astype(jnp.int16)
        wb[u, k] = weights[k].astype(BF)


def build_tile(tile, row_ids, idb, wb, u, store_low, store_high):
    ids = [idb[u, k] for k in range(FAN)]
    wts = [wb[u, k] for k in range(FAN)]
    for r in range(0, TILE // 8, 8):
        rows = row_ids[tile, r : r + 8]
        acc = jnp.zeros((8, 8, LANES), BF)
        for k in range(FAN):
            acc = jnp.where(ids[k][None] == rows, wts[k][None], acc)
        high = jnp.floor(acc)
        store_high(r, high)
        store_low(r, acc - high)


def kernel(
    x_hbm, ws1_hbm, wn1_hbm, ids_hbm, mask_hbm, ws2_hbm, wn2_hbm, ws3_hbm, wn3_hbm, out_ref,
    x_v, ws1, wn1, ids_in, mask_in, ws2, wn2, ws3t, wn3t,
    w1t, w2st, w2nt, yown, yrecv, ysum, sown, ssend, srecv,
    ids_pkt, ids_rcv, ids_s32, row_ids, idb, wb, inv,
    ring, a_own, acc, zbase, pend, rs_send, via, rs_recv, h1, h2,
    in_sem, x_sem, ids_ss, ids_rs, y_ss, y_rs, s_ss, s_rs, r_ss, r_rs, g1_ss, g1_rs, g2_ss, g2_rs,
):
    me = lax.axis_index("g")
    core = lax.rem(me, 2)
    cx = lax.rem(me // 2, 2)
    cy = me // 4
    partner = me + 1 - 2 * core
    steps = (6 - 4 * cx - 8 * cy, 4 - 8 * cy, 2 - 4 * cx)
    peers = (me + steps[0], partner + steps[1], partner + steps[2])
    mates = (partner + steps[0], me + steps[1], me + steps[2])
    mine, theirs = (me, *peers), (partner, *mates)

    barrier = pltpu.get_barrier_semaphore()
    for peer in (*peers, partner):
        pl.semaphore_signal(barrier, inc=1, device_id=(peer,), device_id_type=MESH)

    def fetch(src, dst, i):
        cp = pltpu.make_async_copy(src, dst, in_sem.at[i])
        cp.start()
        return cp

    ids_cp = fetch(ids_hbm, ids_in, 0)
    mask_cp = fetch(mask_hbm, mask_in, 1)
    w1_cps = [fetch(ws1_hbm, ws1, 2), fetch(wn1_hbm, wn1, 3)]
    for b in range(N_DEV):
        cp = pltpu.make_async_copy(x_hbm.at[:, pl.ds(b * BLK, BLK)], x_v.at[b], x_sem)
        cp.start()
    late_cps = [fetch(ws2_hbm, ws2, 4), fetch(wn2_hbm, wn2, 5), fetch(ws3_hbm, ws3t, 6), fetch(wn3_hbm, wn3t, 7)]

    def remote(src, dst, ss, rs, dev):
        return pltpu.make_async_remote_copy(
            src_ref=src, dst_ref=dst, send_sem=ss, recv_sem=rs, device_id=(dev,), device_id_type=MESH
        )

    def drain(ref, sem):
        pltpu.make_async_copy(ref, ref, sem).wait()

    row_shape = (TILE // 8, 8, LANES)
    row_base = lax.broadcasted_iota(jnp.int32, row_shape, 0) * 8 + lax.broadcasted_iota(jnp.int32, row_shape, 1)
    for tile in range(HALF // TILE):
        row_ids[tile] = (row_base + tile * TILE).astype(jnp.int16)
    ids_pkt[...] = jnp.full(ids_pkt.shape, -1, jnp.int16)
    ids_cp.wait()
    mask_cp.wait()
    masked = jnp.where(mask_in[...] > 0, ids_in[...], -1)
    ids_pkt[0:FAN, :] = masked.astype(jnp.int16)
    for g in range(2):
        ids_s32[OWN + g, 0:FAN, :] = masked[:, g * LANES : (g + 1) * LANES]
        spread_ids(ids_s32, idb, wb, inv, OWN + g)
    for cp in w1_cps:
        cp.wait()
    w1t[0:HID, :] = ws1[...].T
    w1t[HID:, :] = wn1[...].T

    pl.semaphore_wait(barrier, 4)
    id_copies = [remote(ids_pkt, ids_rcv.at[s], ids_ss, ids_rs.at[s], peers[s]) for s in range(3)]
    for cp in id_copies:
        cp.start()

    def build_own(tile):
        def put(half, g):
            def store(r, v):
                v = v if half else v * jnp.array(16.0, BF)
                row = tile % 2 * (TILE // 8) + r
                a_own[half * 4 + tile // 2, row : row + 8, :, g * LANES : (g + 1) * LANES] = v

            return store

        for g in range(2):
            build_tile(tile, row_ids, idb, wb, OWN + g, put(0, g), put(1, g))

    drain(x_v, x_sem)
    for i in range(4):
        part = jnp.dot(w1t[...], x_v[theirs[i]], preferred_element_type=F32)
        yown[theirs[i]] = part[HID:].astype(BF)
        ssend[i] = part[:HID].astype(BF)
        part2 = jnp.dot(w1t[...], x_v[mine[i]], preferred_element_type=F32)
        yown[mine[i]] = part2[HID:].astype(BF)
        sown[i] = part2[:HID]
        for b in (theirs[i], mine[i]):
            remote(yown.at[b], yrecv.at[b], y_ss, y_rs, partner).start()
        if i < OWN_EARLY:
            build_own(i)
    for i in range(4):
        remote(ssend.at[i], srecv.at[i], s_ss, s_rs, partner).start()
    for tile in range(OWN_EARLY, 8):
        build_own(tile)
    for cp in late_cps:
        cp.wait()
    w2st[...] = ws2[...].T
    w2nt[...] = wn2[...].T

    def build_into(flat):
        def put(half):
            def store(r, v):
                ring[flat % RING, half, r : r + 8] = v

            return store

        build_tile(flat % 8, row_ids, idb, wb, flat // 8, put(0), put(1))

    def dot_from(flat):
        tile = flat % 8
        cols = slice(tile % 2 * TILE, (tile % 2 + 1) * TILE)
        low = ring[flat % RING, 0].reshape(TILE, LANES)
        high = ring[flat % RING, 1].reshape(TILE, LANES)
        return (
            jnp.dot(ysum[tile // 2, :, cols], low, preferred_element_type=F32),
            jnp.dot(ysum[4 + tile // 2, :, cols], high, preferred_element_type=F32),
        )

    def lanes(g):
        return slice(g * LANES, (g + 1) * LANES)

    def quarter(q):
        return slice(q * Q, (q + 1) * Q)

    def take_ids(s):
        id_copies[s].wait_recv()
        for u, pair in enumerate(UNITS):
            for half, (slot, q) in enumerate(pair):
                if slot == s:
                    ids_s32[u, :, quarter(half)] = ids_rcv[s, :, quarter(q)].astype(jnp.int32)

    rs_copies = {}

    def rs_start(s, q, part):
        rs_send[s, q] = part.astype(BF)
        if s == 0:
            copy = remote(rs_send.at[0, q], via.at[q], r_ss, r_rs.at[q], peers[1 if q % 2 else 2])
        else:
            copy = remote(rs_send.at[s, q], rs_recv.at[s - 1, q], r_ss, r_rs.at[4 * s + q], peers[s])
        rs_copies[s, q] = copy
        copy.start()

    def via_slot(q):
        return 2 if q % 2 else 1

    def finish_unit(u, low, high):
        total = (low * 16.0 + high) * jnp.broadcast_to(inv[u, 0:1, :], (HID, LANES))
        for half, (s, q) in enumerate(UNITS[u]):
            part = total[:, quarter(half)] + sown[1 + s, :, quarter(q)] + srecv[1 + s, :, quarter(q)].astype(F32)
            if s == via_slot(q):
                pend[q] = part
            else:
                rs_start(s, q, part)

    def finish_pending(q):
        rs_copies[0, q].wait_recv()
        rs_start(via_slot(q), q, pend[q] + via[q].astype(F32))

    def own_base(g, own):
        base = own * jnp.broadcast_to(inv[OWN + g, 0:1, :], (HID, LANES))
        zbase[g] = base + sown[0, :, lanes(g)] + srecv[0, :, lanes(g)].astype(F32)

    def own_dot(h, b, p):
        rows = a_own[b, p * Q // 8 : (p + 1) * Q // 8].reshape(Q, BLK)
        return jnp.dot(h[b, p], rows, preferred_element_type=F32)

    class Gather:
        def __init__(self, h, ss, rs, direct):
            self.h, self.ss, self.rs, self.direct = h, ss, rs, direct
            self.copies, self.forwards, self.ready = {}, [], []

        def copy(self, block, p, slot, dev):
            return remote(self.h.at[block, p], self.h.at[block, p], self.ss, self.rs.at[7 * p + slot], dev)

        def send(self, slot, p):
            dev = partner if slot == 3 else peers[slot]
            self.copies[slot, p] = self.copy(me, p, slot, dev)
            self.copies[slot, p].start()

        def take(self, slot, p):
            self.copies[slot, p].wait_recv()
            block = partner if slot == 3 else peers[slot]
            if p not in self.direct and slot == (1 if p % 2 else 2):
                self.copies[0, p] = self.copy(block, p, 0, peers[3 - slot])
                self.copies[0, p].start()
            if slot < 3:
                fwd = self.copy(block, p, 4 + slot, partner)
                fwd.start()
                self.forwards.append((slot, p, fwd))
            self.ready.append((block, p))

        def take_forwards(self, n):
            for slot, p, fwd in self.forwards[:n]:
                fwd.wait_recv()
                self.ready.append((mates[slot], p))
            self.forwards = self.forwards[n:]

        def own(self, pieces):
            acc[...] = sum(own_dot(self.h, me, p) for p in range(pieces))

        def add(self):
            acc[...] += sum(own_dot(self.h, b, p) for b, p in self.ready)
            self.ready = []

    g1 = Gather(h1, g1_ss, g1_rs, direct=(3,))
    g2 = Gather(h2, g2_ss, g2_rs, direct=())

    def finish_quarter(q):
        z = zbase[q // 2, :, quarter(q % 2)]
        for t in (1, 2):
            rs_copies[t, q].wait_recv()
            z = z + rs_recv[t - 1, q].astype(F32)
        h1[me, q] = jnp.maximum(z, 0.0).astype(BF)
        for slot in (0, 2, 1, 3) if q in g1.direct else (2, 1, 3):
            g1.send(slot, q)

    take_ids(2)
    take_ids(1)
    spread_ids(ids_s32, idb, wb, inv, 0)
    lead = 3
    for flat in range(lead):
        build_into(flat)
    drain(yrecv, y_rs)
    for b in range(N_DEV):
        ysum[b] = yown[b] + yrecv[b]
    built = lead
    low = high = own = None
    for flat in range(48):
        u, tile = flat // 8, flat % 8
        while built < 48 and built - flat < 2 or (built < 48 and tile % 2 == 0 and built - flat < lead):
            if built == 8:
                take_ids(0)
            if built % 8 == 0:
                spread_ids(ids_s32, idb, wb, inv, built // 8)
            build_into(built)
            built += 1
        part = dot_from(flat)
        low = part[0] if low is None else low + part[0]
        high = part[1] if high is None else high + part[1]
        if u in (1, 3):
            piece = jnp.dot(ysum[tile], a_own[tile, :, :, lanes(u // 2)].reshape(BLK, LANES), preferred_element_type=F32)
            own = piece if own is None else own + piece
        if tile == 7:
            if u == 0:
                drain(srecv, s_rs)
            finish_unit(u, low, high)
            low = high = None
            if u in (1, 3):
                own_base(u // 2, own)
                own = None
        for when, q in PENDING:
            if flat == when:
                finish_pending(q)
    finish_quarter(0)
    finish_quarter(1)
    finish_quarter(2)
    finish_quarter(3)
    g1.own(4)
    for slot, p in ((2, 0), (1, 0), (1, 1), (2, 1), (2, 2), (1, 2)):
        g1.take(slot, p)
    for p in range(4):
        g1.take(3, p)
    g1.add()
    g1.take(0, 0)
    g1.take(0, 1)
    g1.take_forwards(6)
    g1.add()
    for slot, p in ((2, 3), (1, 3), (0, 3), (0, 2)):
        g1.take(slot, p)
    g1.add()
    g1.take_forwards(4)
    g1.add()
    g1.take_forwards(2)
    g1.add()

    inv_own = jnp.concatenate(
        [jnp.broadcast_to(inv[OWN + g, 0:1, :], (HID, LANES)) for g in range(2)], axis=1
    )
    for g in range(2):
        mean1 = (acc[:, lanes(g)] * inv_own[:, lanes(g)]).astype(BF)
        block = jnp.concatenate([h1[me, 2 * g], h1[me, 2 * g + 1]], axis=1)
        pre2 = jnp.dot(w2st[...], block, preferred_element_type=F32) + jnp.dot(
            w2nt[...], mean1, preferred_element_type=F32
        )
        for half in range(2):
            h2[me, 2 * g + half] = jnp.maximum(pre2[:, quarter(half)], 0.0).astype(BF)
        g2.send(2, 2 * g)
        g2.send(1, 2 * g + 1)
    for slot, p in ((2, 1), (1, 0), (2, 3), (1, 2)):
        g2.send(slot, p)
    for p in range(4):
        g2.send(3, p)
    g2.own(4)
    for g in range(2):
        block = jnp.concatenate([h2[me, 2 * g], h2[me, 2 * g + 1]], axis=1)
        out_ref[:, lanes(g)] = jnp.dot(ws3t[...], block, preferred_element_type=F32)
    drain(ids_rcv, ids_ss)
    drain(yown, y_ss)
    drain(ssend, s_ss)
    drain(rs_send, r_ss)
    drain(h1.at[0:7], g1_ss)
    for p in range(4):
        g2.take(3, p)
    g2.add()
    for slot, p in ((2, 0), (1, 1), (2, 2), (1, 3)):
        g2.take(slot, p)
    g2.add()
    for slot, p in ((2, 1), (1, 0), (2, 3), (1, 2)):
        g2.take(slot, p)
    g2.take_forwards(4)
    g2.add()
    g2.take(0, 0)
    g2.take(0, 1)
    g2.take_forwards(4)
    g2.add()
    g2.take(0, 2)
    g2.take(0, 3)
    g2.take_forwards(2)
    g2.add()
    g2.take_forwards(2)
    g2.add()
    for g in range(2):
        mean2 = (acc[:, lanes(g)] * inv_own[:, lanes(g)]).astype(BF)
        out_ref[:, lanes(g)] += jnp.dot(wn3t[...], mean2, preferred_element_type=F32)
    drain(h2.at[0:7], g2_ss)


def solution(mesh):
    def device_step(feat, ws1, wn1, ids, mask, ws2, wn2, ws3, wn3):
        operands = (feat.T, ws1, wn1, ids.T, mask.T, ws2, wn2, ws3.T, wn3.T)
        vm = pl.BlockSpec(memory_space=pltpu.VMEM)
        dma = pltpu.SemaphoreType.DMA
        out_t = pl.pallas_call(
            kernel,
            out_shape=jax.ShapeDtypeStruct((7, BLK), F32),
            in_specs=[pl.BlockSpec(memory_space=pltpu.HBM)] * 9,
            out_specs=vm,
            scratch_shapes=[
                pltpu.VMEM((N_DEV, 192, BLK), BF),
                pltpu.VMEM((192, HID), BF),
                pltpu.VMEM((192, HID), BF),
                pltpu.VMEM((FAN, BLK), jnp.int32),
                pltpu.VMEM((FAN, BLK), jnp.int32),
                pltpu.VMEM((HID, HID), BF),
                pltpu.VMEM((HID, HID), BF),
                pltpu.VMEM((7, HID), BF),
                pltpu.VMEM((7, HID), BF),
                pltpu.VMEM((2 * HID, 192), BF),
                pltpu.VMEM((HID, HID), BF),
                pltpu.VMEM((HID, HID), BF),
                pltpu.VMEM((N_DEV, HID, BLK), BF),
                pltpu.VMEM((N_DEV, HID, BLK), BF),
                pltpu.VMEM((N_DEV, HID, BLK), BF),
                pltpu.VMEM((4, HID, BLK), F32),
                pltpu.VMEM((4, HID, BLK), BF),
                pltpu.VMEM((4, HID, BLK), BF),
                pltpu.VMEM((16, BLK), jnp.int16),
                pltpu.VMEM((3, 16, BLK), jnp.int16),
                pltpu.VMEM((8, 16, LANES), jnp.int32),
                pltpu.VMEM((HALF // TILE, TILE // 8, 8, LANES), jnp.int16),
                pltpu.VMEM((8, FAN, 8, LANES), jnp.int16),
                pltpu.VMEM((8, FAN, 8, LANES), BF),
                pltpu.VMEM((8, 8, LANES), F32),
                pltpu.VMEM((RING, 2, TILE // 8, 8, LANES), BF),
                pltpu.VMEM((N_DEV, BLK // 8, 8, BLK), BF),
                pltpu.VMEM((HID, BLK), F32),
                pltpu.VMEM((2, HID, LANES), F32),
                pltpu.VMEM((4, HID, Q), F32),
                pltpu.VMEM((3, 4, HID, Q), BF),
                pltpu.VMEM((4, HID, Q), BF),
                pltpu.VMEM((2, 4, HID, Q), BF),
                pltpu.VMEM((N_DEV, 4, HID, Q), BF),
                pltpu.VMEM((N_DEV, 4, HID, Q), BF),
                dma((8,)),
                dma,
                dma, dma((3,)),
                dma, dma,
                dma, dma,
                dma, dma((12,)),
                dma, dma((28,)),
                dma, dma((28,)),
            ],
            compiler_params=pltpu.CompilerParams(
                collective_id=0, has_side_effects=True, vmem_limit_bytes=32 * 1024 * 1024
            ),
            name="graphsage",
        )(*(pltpu.with_memory_space_constraint(a, pltpu.HBM) for a in operands))
        return out_t.T

    col_split = P(None, "g")
    row_split = P("g", None)
    replicated = P()
    return jax.shard_map(
        device_step,
        mesh=mesh,
        in_specs=(col_split, row_split, row_split, row_split, row_split, replicated, replicated, replicated, replicated),
        out_specs=row_split,
        check_vma=False,
    )
```

```python
import jax
import jax.numpy as jnp
from jax import lax
from jax.experimental import pallas as pl
from jax.experimental.pallas import tpu as pltpu
from jax.sharding import PartitionSpec as P

MESH = pl.DeviceIdType.MESH
N_DEV = 8
NODES = 4096
BLK = NODES // N_DEV
HALF = NODES // 2
FAN = 10
HID = 128
TILE = 256
LANES = 256
BF = jnp.bfloat16
F32 = jnp.float32


UNITS = (((2, 0), (1, 0)), ((0, 0), (0, 1)), ((2, 1), (1, 1)), ((0, 2), (0, 3)), ((2, 2), (1, 2)), ((2, 3), (1, 3)))
OWN = 6
OWN_EARLY = 3
RING = 6
Q = 128


def spread_ids(ids_s32, idb, wb, inv, u):
    words, weights = [], []
    degree = jnp.zeros((8, LANES), F32)
    for k in range(FAN):
        raw = jnp.broadcast_to(ids_s32[u, k : k + 1, :], (8, LANES))
        valid = raw >= 0
        degree += jnp.where(valid, 1.0, 0.0)
        upper = raw >= HALF
        word = jnp.where(upper, raw - HALF, raw)
        weight = jnp.where(valid, jnp.where(upper, 1.0, 0.0625), 0.0)
        for m in range(k):
            same = word == words[m]
            weights[m] = weights[m] + jnp.where(same, weight, 0.0)
            word = jnp.where(same, -1, word)
        words.append(word)
        weights.append(weight)
    inv[u] = 1.0 / degree
    for k in range(FAN):
        idb[u, k] = words[k].astype(jnp.int16)
        wb[u, k] = weights[k].astype(BF)


def build_tile(tile, row_ids, idb, wb, u, store_low, store_high):
    ids = [idb[u, k] for k in range(FAN)]
    wts = [wb[u, k] for k in range(FAN)]
    for r in range(0, TILE // 8, 8):
        rows = row_ids[tile, r : r + 8]
        acc = jnp.zeros((8, 8, LANES), BF)
        for k in range(FAN):
            acc = jnp.where(ids[k][None] == rows, wts[k][None], acc)
        high = jnp.floor(acc)
        store_high(r, high)
        store_low(r, acc - high)


def kernel(
    x_hbm, ws1_hbm, wn1_hbm, ids_hbm, mask_hbm, ws2_hbm, wn2_hbm, ws3_hbm, wn3_hbm, out_ref,
    x_v, ws1, wn1, ids_in, mask_in, ws2, wn2, ws3t, wn3t,
    w1t, w2st, w2nt, yown, yrecv, ysum, sown, ssend, srecv,
    ids_pkt, ids_rcv, ids_s32, row_ids, idb, wb, inv,
    ring, a_own, acc, zbase, rs_send, rs_recv, h1, h2,
    in_sem, x_sem, ids_ss, ids_rs, y_ss, y_rs, s_ss, s_rs, r_ss, r_rs, g1_ss, g1_rs, g2_ss, g2_rs,
):
    me = lax.axis_index("g")
    core = lax.rem(me, 2)
    cx = lax.rem(me // 2, 2)
    cy = me // 4
    partner = me + 1 - 2 * core
    steps = (6 - 4 * cx - 8 * cy, 4 - 8 * cy, 2 - 4 * cx)
    peers = tuple(partner + step for step in steps)
    mates = tuple(me + step for step in steps)
    mine, theirs = (me, *peers), (partner, *mates)

    barrier = pltpu.get_barrier_semaphore()
    for peer in (*peers, partner):
        pl.semaphore_signal(barrier, inc=1, device_id=(peer,), device_id_type=MESH)

    def fetch(src, dst, i):
        cp = pltpu.make_async_copy(src, dst, in_sem.at[i])
        cp.start()
        return cp

    ids_cp = fetch(ids_hbm, ids_in, 0)
    mask_cp = fetch(mask_hbm, mask_in, 1)
    w1_cps = [fetch(ws1_hbm, ws1, 2), fetch(wn1_hbm, wn1, 3)]
    for b in range(N_DEV):
        cp = pltpu.make_async_copy(x_hbm.at[:, pl.ds(b * BLK, BLK)], x_v.at[b], x_sem)
        cp.start()
    late_cps = [fetch(ws2_hbm, ws2, 4), fetch(wn2_hbm, wn2, 5), fetch(ws3_hbm, ws3t, 6), fetch(wn3_hbm, wn3t, 7)]

    def remote(src, dst, ss, rs, dev):
        return pltpu.make_async_remote_copy(
            src_ref=src, dst_ref=dst, send_sem=ss, recv_sem=rs, device_id=(dev,), device_id_type=MESH
        )

    def drain(ref, sem):
        pltpu.make_async_copy(ref, ref, sem).wait()

    row_shape = (TILE // 8, 8, LANES)
    row_base = lax.broadcasted_iota(jnp.int32, row_shape, 0) * 8 + lax.broadcasted_iota(jnp.int32, row_shape, 1)
    for tile in range(HALF // TILE):
        row_ids[tile] = (row_base + tile * TILE).astype(jnp.int16)
    ids_pkt[...] = jnp.full(ids_pkt.shape, -1, jnp.int16)
    ids_cp.wait()
    mask_cp.wait()
    masked = jnp.where(mask_in[...] > 0, ids_in[...], -1)
    ids_pkt[0:FAN, :] = masked.astype(jnp.int16)
    for g in range(2):
        ids_s32[OWN + g, 0:FAN, :] = masked[:, g * LANES : (g + 1) * LANES]
        spread_ids(ids_s32, idb, wb, inv, OWN + g)
    for cp in w1_cps:
        cp.wait()
    w1t[0:HID, :] = ws1[...].T
    w1t[HID:, :] = wn1[...].T

    pl.semaphore_wait(barrier, 4)
    id_copies = [remote(ids_pkt, ids_rcv.at[s], ids_ss, ids_rs.at[s], peers[s]) for s in range(3)]
    for cp in id_copies:
        cp.start()

    def build_own(tile):
        def put(half, g):
            def store(r, v):
                v = v if half else v * jnp.array(16.0, BF)
                row = tile % 2 * (TILE // 8) + r
                a_own[half * 4 + tile // 2, row : row + 8, :, g * LANES : (g + 1) * LANES] = v

            return store

        for g in range(2):
            build_tile(tile, row_ids, idb, wb, OWN + g, put(0, g), put(1, g))

    drain(x_v, x_sem)
    for i in range(4):
        part = jnp.dot(w1t[...], x_v[theirs[i]], preferred_element_type=F32)
        yown[theirs[i]] = part[HID:].astype(BF)
        ssend[i] = part[:HID].astype(BF)
        part2 = jnp.dot(w1t[...], x_v[mine[i]], preferred_element_type=F32)
        yown[mine[i]] = part2[HID:].astype(BF)
        sown[i] = part2[:HID]
        for b in (theirs[i], mine[i]):
            remote(yown.at[b], yrecv.at[b], y_ss, y_rs, partner).start()
        if i < OWN_EARLY:
            build_own(i)
    for i in range(4):
        remote(ssend.at[i], srecv.at[i], s_ss, s_rs, partner).start()
    for tile in range(OWN_EARLY, 8):
        build_own(tile)
    for cp in late_cps:
        cp.wait()
    w2st[...] = ws2[...].T
    w2nt[...] = wn2[...].T

    def build_into(flat):
        def put(half):
            def store(r, v):
                ring[flat % RING, half, r : r + 8] = v

            return store

        build_tile(flat % 8, row_ids, idb, wb, flat // 8, put(0), put(1))

    def dot_from(flat):
        tile = flat % 8
        cols = slice(tile % 2 * TILE, (tile % 2 + 1) * TILE)
        low = ring[flat % RING, 0].reshape(TILE, LANES)
        high = ring[flat % RING, 1].reshape(TILE, LANES)
        return (
            jnp.dot(ysum[tile // 2, :, cols], low, preferred_element_type=F32),
            jnp.dot(ysum[4 + tile // 2, :, cols], high, preferred_element_type=F32),
        )

    def lanes(g):
        return slice(g * LANES, (g + 1) * LANES)

    def quarter(q):
        return slice(q * Q, (q + 1) * Q)

    def take_ids(s):
        id_copies[s].wait_recv()
        for u, pair in enumerate(UNITS):
            for half, (slot, q) in enumerate(pair):
                if slot == s:
                    ids_s32[u, :, quarter(half)] = ids_rcv[s, :, quarter(q)].astype(jnp.int32)

    rs_copies = {}

    def finish_unit(u, low, high):
        total = (low * 16.0 + high) * jnp.broadcast_to(inv[u, 0:1, :], (HID, LANES))
        for half, (s, q) in enumerate(UNITS[u]):
            part = total[:, quarter(half)] + sown[1 + s, :, quarter(q)] + srecv[1 + s, :, quarter(q)].astype(F32)
            rs_send[s, q] = part.astype(BF)
            rs_copies[s, q] = remote(rs_send.at[s, q], rs_recv.at[s, q], r_ss, r_rs.at[4 * s + q], peers[s])
            rs_copies[s, q].start()

    def own_base(g, own):
        base = own * jnp.broadcast_to(inv[OWN + g, 0:1, :], (HID, LANES))
        zbase[g] = base + sown[0, :, lanes(g)] + srecv[0, :, lanes(g)].astype(F32)

    def own_dot(h, b, p):
        rows = a_own[b, p * Q // 8 : (p + 1) * Q // 8].reshape(Q, BLK)
        return jnp.dot(h[b, p], rows, preferred_element_type=F32)

    class Gather:
        def __init__(self, h, ss, rs, direct):
            self.h, self.ss, self.rs, self.direct = h, ss, rs, direct
            self.copies, self.forwards, self.ready = {}, [], []

        def copy(self, block, p, slot, dev):
            return remote(self.h.at[block, p], self.h.at[block, p], self.ss, self.rs.at[7 * p + slot], dev)

        def send(self, slot, p):
            dev = partner if slot == 3 else peers[slot]
            self.copies[slot, p] = self.copy(me, p, slot, dev)
            self.copies[slot, p].start()

        def take(self, slot, p):
            self.copies[slot, p].wait_recv()
            block = partner if slot == 3 else mates[0] if slot == 0 and p not in self.direct else peers[slot]
            if p not in self.direct and slot == (1 if p % 2 else 2):
                self.copies[0, p] = self.copy(block, p, 0, peers[3 - slot])
                self.copies[0, p].start()
            if slot < 3:
                fwd = self.copy(block, p, 4 + slot, partner)
                fwd.start()
                self.forwards.append((slot, p, fwd))
            self.ready.append((block, p))

        def take_forwards(self, n):
            for slot, p, fwd in self.forwards[:n]:
                fwd.wait_recv()
                relayed = slot == 0 and p not in self.direct
                self.ready.append((peers[0] if relayed else mates[slot], p))
            self.forwards = self.forwards[n:]

        def own(self, pieces):
            acc[...] = sum(own_dot(self.h, me, p) for p in range(pieces))

        def add(self):
            acc[...] += sum(own_dot(self.h, b, p) for b, p in self.ready)
            self.ready = []

    g1 = Gather(h1, g1_ss, g1_rs, direct=(3,))
    g2 = Gather(h2, g2_ss, g2_rs, direct=())

    def finish_quarter(q):
        z = zbase[q // 2, :, quarter(q % 2)]
        for t in (1, 2, 0):
            rs_copies[t, q].wait_recv()
            z = z + rs_recv[t, q].astype(F32)
        h1[me, q] = jnp.maximum(z, 0.0).astype(BF)
        for slot in (0, 2, 1, 3) if q in g1.direct else (2, 1, 3):
            g1.send(slot, q)

    take_ids(2)
    take_ids(1)
    spread_ids(ids_s32, idb, wb, inv, 0)
    lead = 3
    for flat in range(lead):
        build_into(flat)
    drain(yrecv, y_rs)
    for b in range(N_DEV):
        ysum[b] = yown[b] + yrecv[b]
    built = lead
    low = high = own = None
    for flat in range(48):
        u, tile = flat // 8, flat % 8
        while built < 48 and built - flat < 2 or (built < 48 and tile % 2 == 0 and built - flat < lead):
            if built == 8:
                take_ids(0)
            if built % 8 == 0:
                spread_ids(ids_s32, idb, wb, inv, built // 8)
            build_into(built)
            built += 1
        part = dot_from(flat)
        low = part[0] if low is None else low + part[0]
        high = part[1] if high is None else high + part[1]
        if u in (1, 3):
            piece = jnp.dot(ysum[tile], a_own[tile, :, :, lanes(u // 2)].reshape(BLK, LANES), preferred_element_type=F32)
            own = piece if own is None else own + piece
        if tile == 7:
            if u == 0:
                drain(srecv, s_rs)
            finish_unit(u, low, high)
            low = high = None
            if u in (1, 3):
                own_base(u // 2, own)
                own = None
    finish_quarter(0)
    finish_quarter(1)
    finish_quarter(2)
    finish_quarter(3)
    g1.own(4)
    for slot, p in ((2, 0), (1, 0), (1, 1), (2, 1), (2, 2), (1, 2)):
        g1.take(slot, p)
    for p in range(4):
        g1.take(3, p)
    g1.add()
    g1.take(0, 0)
    g1.take(0, 1)
    g1.take_forwards(6)
    g1.add()
    for slot, p in ((2, 3), (1, 3), (0, 3), (0, 2)):
        g1.take(slot, p)
    g1.add()
    g1.take_forwards(4)
    g1.add()
    g1.take_forwards(2)
    g1.add()

    inv_own = jnp.concatenate(
        [jnp.broadcast_to(inv[OWN + g, 0:1, :], (HID, LANES)) for g in range(2)], axis=1
    )
    for g in range(2):
        mean1 = (acc[:, lanes(g)] * inv_own[:, lanes(g)]).astype(BF)
        block = jnp.concatenate([h1[me, 2 * g], h1[me, 2 * g + 1]], axis=1)
        pre2 = jnp.dot(w2st[...], block, preferred_element_type=F32) + jnp.dot(
            w2nt[...], mean1, preferred_element_type=F32
        )
        for half in range(2):
            h2[me, 2 * g + half] = jnp.maximum(pre2[:, quarter(half)], 0.0).astype(BF)
        g2.send(2, 2 * g)
        g2.send(1, 2 * g + 1)
    for slot, p in ((2, 1), (1, 0), (2, 3), (1, 2)):
        g2.send(slot, p)
    for p in range(4):
        g2.send(3, p)
    g2.own(4)
    for g in range(2):
        block = jnp.concatenate([h2[me, 2 * g], h2[me, 2 * g + 1]], axis=1)
        out_ref[:, lanes(g)] = jnp.dot(ws3t[...], block, preferred_element_type=F32)
    drain(ids_rcv, ids_ss)
    drain(yown, y_ss)
    drain(ssend, s_ss)
    drain(rs_send, r_ss)
    drain(h1.at[0:7], g1_ss)
    for p in range(4):
        g2.take(3, p)
    g2.add()
    for slot, p in ((2, 0), (1, 1), (2, 2), (1, 3)):
        g2.take(slot, p)
    g2.add()
    for slot, p in ((2, 1), (1, 0), (2, 3), (1, 2)):
        g2.take(slot, p)
    g2.take_forwards(4)
    g2.add()
    g2.take(0, 0)
    g2.take(0, 1)
    g2.take_forwards(4)
    g2.add()
    g2.take(0, 2)
    g2.take(0, 3)
    g2.take_forwards(2)
    g2.add()
    g2.take_forwards(2)
    g2.add()
    for g in range(2):
        mean2 = (acc[:, lanes(g)] * inv_own[:, lanes(g)]).astype(BF)
        out_ref[:, lanes(g)] += jnp.dot(wn3t[...], mean2, preferred_element_type=F32)
    drain(h2.at[0:7], g2_ss)


def solution(mesh):
    def device_step(feat, ws1, wn1, ids, mask, ws2, wn2, ws3, wn3):
        operands = (feat.T, ws1, wn1, ids.T, mask.T, ws2, wn2, ws3.T, wn3.T)
        vm = pl.BlockSpec(memory_space=pltpu.VMEM)
        dma = pltpu.SemaphoreType.DMA
        out_t = pl.pallas_call(
            kernel,
            out_shape=jax.ShapeDtypeStruct((7, BLK), F32),
            in_specs=[pl.BlockSpec(memory_space=pltpu.HBM)] * 9,
            out_specs=vm,
            scratch_shapes=[
                pltpu.VMEM((N_DEV, 192, BLK), BF),
                pltpu.VMEM((192, HID), BF),
                pltpu.VMEM((192, HID), BF),
                pltpu.VMEM((FAN, BLK), jnp.int32),
                pltpu.VMEM((FAN, BLK), jnp.int32),
                pltpu.VMEM((HID, HID), BF),
                pltpu.VMEM((HID, HID), BF),
                pltpu.VMEM((7, HID), BF),
                pltpu.VMEM((7, HID), BF),
                pltpu.VMEM((2 * HID, 192), BF),
                pltpu.VMEM((HID, HID), BF),
                pltpu.VMEM((HID, HID), BF),
                pltpu.VMEM((N_DEV, HID, BLK), BF),
                pltpu.VMEM((N_DEV, HID, BLK), BF),
                pltpu.VMEM((N_DEV, HID, BLK), BF),
                pltpu.VMEM((4, HID, BLK), F32),
                pltpu.VMEM((4, HID, BLK), BF),
                pltpu.VMEM((4, HID, BLK), BF),
                pltpu.VMEM((16, BLK), jnp.int16),
                pltpu.VMEM((3, 16, BLK), jnp.int16),
                pltpu.VMEM((8, 16, LANES), jnp.int32),
                pltpu.VMEM((HALF // TILE, TILE // 8, 8, LANES), jnp.int16),
                pltpu.VMEM((8, FAN, 8, LANES), jnp.int16),
                pltpu.VMEM((8, FAN, 8, LANES), BF),
                pltpu.VMEM((8, 8, LANES), F32),
                pltpu.VMEM((RING, 2, TILE // 8, 8, LANES), BF),
                pltpu.VMEM((N_DEV, BLK // 8, 8, BLK), BF),
                pltpu.VMEM((HID, BLK), F32),
                pltpu.VMEM((2, HID, LANES), F32),
                pltpu.VMEM((3, 4, HID, Q), BF),
                pltpu.VMEM((3, 4, HID, Q), BF),
                pltpu.VMEM((N_DEV, 4, HID, Q), BF),
                pltpu.VMEM((N_DEV, 4, HID, Q), BF),
                dma((8,)),
                dma,
                dma, dma((3,)),
                dma, dma,
                dma, dma,
                dma, dma((12,)),
                dma, dma((28,)),
                dma, dma((28,)),
            ],
            compiler_params=pltpu.CompilerParams(
                collective_id=0, has_side_effects=True, vmem_limit_bytes=32 * 1024 * 1024
            ),
            name="graphsage",
        )(*(pltpu.with_memory_space_constraint(a, pltpu.HBM) for a in operands))
        return out_t.T

    col_split = P(None, "g")
    row_split = P("g", None)
    replicated = P()
    return jax.shard_map(
        device_step,
        mesh=mesh,
        in_specs=(col_split, row_split, row_split, row_split, row_split, replicated, replicated, replicated, replicated),
        out_specs=row_split,
        check_vma=False,
    )
```

```python
import jax
import jax.numpy as jnp
from jax import lax
from jax.experimental import pallas as pl
from jax.experimental.pallas import tpu as pltpu
from jax.sharding import PartitionSpec as P

MESH = pl.DeviceIdType.MESH
N_DEV = 8
NODES = 4096
BLK = NODES // N_DEV
HALF = NODES // 2
FAN = 10
HID = 128
TILE = 256
LANES = 256
BF = jnp.bfloat16
F32 = jnp.float32


UNITS = (((2, 0), (1, 0)), ((0, 0), (0, 1)), ((2, 1), (1, 1)), ((0, 2), (0, 3)), ((2, 2), (1, 2)), ((2, 3), (1, 3)))
OWN = 6
OWN_EARLY = 3
RING = 6
Q = 128


def spread_ids(ids_s32, idb, wb, inv, u):
    words, weights = [], []
    degree = jnp.zeros((8, LANES), F32)
    for k in range(FAN):
        raw = jnp.broadcast_to(ids_s32[u, k : k + 1, :], (8, LANES))
        valid = raw >= 0
        degree += jnp.where(valid, 1.0, 0.0)
        upper = raw >= HALF
        word = jnp.where(upper, raw - HALF, raw)
        weight = jnp.where(valid, jnp.where(upper, 1.0, 0.0625), 0.0)
        for m in range(k):
            same = word == words[m]
            weights[m] = weights[m] + jnp.where(same, weight, 0.0)
            word = jnp.where(same, -1, word)
        words.append(word)
        weights.append(weight)
    inv[u] = 1.0 / degree
    for k in range(FAN):
        idb[u, k] = words[k].astype(jnp.int16)
        wb[u, k] = weights[k].astype(BF)


def build_tile(tile, row_ids, idb, wb, u, store_low, store_high):
    ids = [idb[u, k] for k in range(FAN)]
    wts = [wb[u, k] for k in range(FAN)]
    for r in range(0, TILE // 8, 8):
        rows = row_ids[tile, r : r + 8]
        acc = jnp.zeros((8, 8, LANES), BF)
        for k in range(FAN):
            acc = jnp.where(ids[k][None] == rows, wts[k][None], acc)
        high = jnp.floor(acc)
        store_high(r, high)
        store_low(r, acc - high)


def kernel(
    x_hbm, ws1_hbm, wn1_hbm, ids_hbm, mask_hbm, ws2_hbm, wn2_hbm, ws3_hbm, wn3_hbm, out_ref,
    x_v, ws1, wn1, ids_in, mask_in, ws2, wn2, ws3t, wn3t,
    w1t, w2st, w2nt, yown, yrecv, ysum, sown, ssend, srecv,
    ids_pkt, ids_rcv, ids_s32, row_ids, idb, wb, inv,
    ring, a_own, acc, zbase, rs_send, rs_recv, h1, h2,
    in_sem, x_sem, ids_ss, ids_rs, y_ss, y_rs, s_ss, s_rs, r_ss, r_rs, g1_ss, g1_rs, g2_ss, g2_rs,
):
    me = lax.axis_index("g")
    core = lax.rem(me, 2)
    cx = lax.rem(me // 2, 2)
    cy = me // 4
    partner = me + 1 - 2 * core
    steps = (6 - 4 * cx - 8 * cy, 4 - 8 * cy, 2 - 4 * cx)
    peers = tuple(partner + step for step in steps)
    mates = tuple(me + step for step in steps)
    mine, theirs = (me, *peers), (partner, *mates)

    barrier = pltpu.get_barrier_semaphore()
    for peer in (*peers, partner):
        pl.semaphore_signal(barrier, inc=1, device_id=(peer,), device_id_type=MESH)

    def fetch(src, dst, i):
        cp = pltpu.make_async_copy(src, dst, in_sem.at[i])
        cp.start()
        return cp

    ids_cp = fetch(ids_hbm, ids_in, 0)
    mask_cp = fetch(mask_hbm, mask_in, 1)
    w1_cps = [fetch(ws1_hbm, ws1, 2), fetch(wn1_hbm, wn1, 3)]
    for b in range(N_DEV):
        cp = pltpu.make_async_copy(x_hbm.at[:, pl.ds(b * BLK, BLK)], x_v.at[b], x_sem)
        cp.start()
    late_cps = [fetch(ws2_hbm, ws2, 4), fetch(wn2_hbm, wn2, 5), fetch(ws3_hbm, ws3t, 6), fetch(wn3_hbm, wn3t, 7)]

    def remote(src, dst, ss, rs, dev):
        return pltpu.make_async_remote_copy(
            src_ref=src, dst_ref=dst, send_sem=ss, recv_sem=rs, device_id=(dev,), device_id_type=MESH
        )

    def drain(ref, sem):
        pltpu.make_async_copy(ref, ref, sem).wait()

    row_shape = (TILE // 8, 8, LANES)
    row_base = lax.broadcasted_iota(jnp.int32, row_shape, 0) * 8 + lax.broadcasted_iota(jnp.int32, row_shape, 1)
    for tile in range(HALF // TILE):
        row_ids[tile] = (row_base + tile * TILE).astype(jnp.int16)
    ids_pkt[...] = jnp.full(ids_pkt.shape, -1, jnp.int16)
    ids_cp.wait()
    mask_cp.wait()
    masked = jnp.where(mask_in[...] > 0, ids_in[...], -1)
    ids_pkt[0:FAN, :] = masked.astype(jnp.int16)
    for g in range(2):
        ids_s32[OWN + g, 0:FAN, :] = masked[:, g * LANES : (g + 1) * LANES]
        spread_ids(ids_s32, idb, wb, inv, OWN + g)
    for cp in w1_cps:
        cp.wait()
    w1t[0:HID, :] = ws1[...].T
    w1t[HID:, :] = wn1[...].T

    pl.semaphore_wait(barrier, 4)
    id_copies = [remote(ids_pkt, ids_rcv.at[s], ids_ss, ids_rs.at[s], peers[s]) for s in range(3)]
    for cp in id_copies:
        cp.start()

    def build_own(tile):
        def put(half, g):
            def store(r, v):
                v = v if half else v * jnp.array(16.0, BF)
                row = tile % 2 * (TILE // 8) + r
                a_own[half * 4 + tile // 2, row : row + 8, :, g * LANES : (g + 1) * LANES] = v

            return store

        for g in range(2):
            build_tile(tile, row_ids, idb, wb, OWN + g, put(0, g), put(1, g))

    drain(x_v, x_sem)
    for i in range(4):
        part = jnp.dot(w1t[...], x_v[theirs[i]], preferred_element_type=F32)
        yown[theirs[i]] = part[HID:].astype(BF)
        ssend[i] = part[:HID].astype(BF)
        part2 = jnp.dot(w1t[...], x_v[mine[i]], preferred_element_type=F32)
        yown[mine[i]] = part2[HID:].astype(BF)
        sown[i] = part2[:HID]
        for b in (theirs[i], mine[i]):
            remote(yown.at[b], yrecv.at[b], y_ss, y_rs, partner).start()
        if i < OWN_EARLY:
            build_own(i)
    for i in range(4):
        remote(ssend.at[i], srecv.at[i], s_ss, s_rs, partner).start()
    for tile in range(OWN_EARLY, 8):
        build_own(tile)
    for cp in late_cps:
        cp.wait()
    w2st[...] = ws2[...].T
    w2nt[...] = wn2[...].T

    def build_into(flat):
        def put(half):
            def store(r, v):
                ring[flat % RING, half, r : r + 8] = v

            return store

        build_tile(flat % 8, row_ids, idb, wb, flat // 8, put(0), put(1))

    def dot_from(flat):
        tile = flat % 8
        cols = slice(tile % 2 * TILE, (tile % 2 + 1) * TILE)
        low = ring[flat % RING, 0].reshape(TILE, LANES)
        high = ring[flat % RING, 1].reshape(TILE, LANES)
        return (
            jnp.dot(ysum[tile // 2, :, cols], low, preferred_element_type=F32),
            jnp.dot(ysum[4 + tile // 2, :, cols], high, preferred_element_type=F32),
        )

    def lanes(g):
        return slice(g * LANES, (g + 1) * LANES)

    def quarter(q):
        return slice(q * Q, (q + 1) * Q)

    def take_ids(s):
        id_copies[s].wait_recv()
        for u, pair in enumerate(UNITS):
            for half, (slot, q) in enumerate(pair):
                if slot == s:
                    ids_s32[u, :, quarter(half)] = ids_rcv[s, :, quarter(q)].astype(jnp.int32)

    rs_copies = {}

    def finish_unit(u, low, high):
        total = (low * 16.0 + high) * jnp.broadcast_to(inv[u, 0:1, :], (HID, LANES))
        for half, (s, q) in enumerate(UNITS[u]):
            part = total[:, quarter(half)] + sown[1 + s, :, quarter(q)] + srecv[1 + s, :, quarter(q)].astype(F32)
            rs_send[s, q] = part.astype(BF)
            rs_copies[s, q] = remote(rs_send.at[s, q], rs_recv.at[s, q], r_ss, r_rs.at[4 * s + q], peers[s])
            rs_copies[s, q].start()

    def own_base(g, own):
        base = own * jnp.broadcast_to(inv[OWN + g, 0:1, :], (HID, LANES))
        zbase[g] = base + sown[0, :, lanes(g)] + srecv[0, :, lanes(g)].astype(F32)

    def own_dot(h, b, p):
        rows = a_own[b, p * Q // 8 : (p + 1) * Q // 8].reshape(Q, BLK)
        return jnp.dot(h[b, p], rows, preferred_element_type=F32)

    class Gather:
        def __init__(self, h, ss, rs, direct):
            self.h, self.ss, self.rs, self.direct = h, ss, rs, direct
            self.copies, self.forwards, self.ready = {}, [], []

        def copy(self, block, p, slot, dev):
            return remote(self.h.at[block, p], self.h.at[block, p], self.ss, self.rs.at[7 * p + slot], dev)

        def send(self, slot, p):
            dev = partner if slot == 3 else peers[slot]
            self.copies[slot, p] = self.copy(me, p, slot, dev)
            self.copies[slot, p].start()

        def take(self, slot, p):
            self.copies[slot, p].wait_recv()
            block = partner if slot == 3 else mates[0] if slot == 0 and p not in self.direct else peers[slot]
            if p not in self.direct and slot == (1 if p % 2 else 2):
                self.copies[0, p] = self.copy(block, p, 0, peers[3 - slot])
                self.copies[0, p].start()
            if slot < 3:
                fwd = self.copy(block, p, 4 + slot, partner)
                fwd.start()
                self.forwards.append((slot, p, fwd))
            self.ready.append((block, p))

        def take_forwards(self, n):
            for slot, p, fwd in self.forwards[:n]:
                fwd.wait_recv()
                relayed = slot == 0 and p not in self.direct
                self.ready.append((peers[0] if relayed else mates[slot], p))
            self.forwards = self.forwards[n:]

        def own(self, pieces):
            acc[...] = sum(own_dot(self.h, me, p) for p in range(pieces))

        def add(self):
            acc[...] += sum(own_dot(self.h, b, p) for b, p in self.ready)
            self.ready = []

    g1 = Gather(h1, g1_ss, g1_rs, direct=(3,))
    g2 = Gather(h2, g2_ss, g2_rs, direct=())

    def finish_quarter(q):
        z = zbase[q // 2, :, quarter(q % 2)]
        for t in (1, 2, 0):
            rs_copies[t, q].wait_recv()
            z = z + rs_recv[t, q].astype(F32)
        h1[me, q] = jnp.maximum(z, 0.0).astype(BF)
        for slot in (0, 2, 1, 3) if q in g1.direct else (2, 1, 3):
            g1.send(slot, q)

    take_ids(2)
    take_ids(1)
    spread_ids(ids_s32, idb, wb, inv, 0)
    lead = 3
    for flat in range(lead):
        build_into(flat)
    drain(yrecv, y_rs)
    for b in range(N_DEV):
        ysum[b] = yown[b] + yrecv[b]
    built = lead
    low = high = own = None
    for flat in range(48):
        u, tile = flat // 8, flat % 8
        while built < 48 and built - flat < 2 or (built < 48 and tile % 2 == 0 and built - flat < lead):
            if built == 8:
                take_ids(0)
            if built % 8 == 0:
                spread_ids(ids_s32, idb, wb, inv, built // 8)
            build_into(built)
            built += 1
        part = dot_from(flat)
        low = part[0] if low is None else low + part[0]
        high = part[1] if high is None else high + part[1]
        if u in (1, 3):
            piece = jnp.dot(ysum[tile], a_own[tile, :, :, lanes(u // 2)].reshape(BLK, LANES), preferred_element_type=F32)
            own = piece if own is None else own + piece
        if tile == 7:
            if u == 0:
                drain(srecv, s_rs)
            finish_unit(u, low, high)
            low = high = None
            if u in (1, 3):
                own_base(u // 2, own)
                own = None
    finish_quarter(0)
    finish_quarter(1)
    g1.take(2, 0)
    g1.take(1, 0)
    finish_quarter(2)
    g1.take(1, 1)
    g1.take(2, 1)
    finish_quarter(3)
    g1.own(4)
    for slot, p in ((2, 2), (1, 2)):
        g1.take(slot, p)
    for p in range(4):
        g1.take(3, p)
    g1.add()
    g1.take(0, 0)
    g1.take(0, 1)
    g1.take_forwards(6)
    g1.add()
    for slot, p in ((2, 3), (1, 3), (0, 3), (0, 2)):
        g1.take(slot, p)
    g1.add()
    g1.take_forwards(4)
    g1.add()
    g1.take_forwards(2)
    g1.add()

    inv_own = jnp.concatenate(
        [jnp.broadcast_to(inv[OWN + g, 0:1, :], (HID, LANES)) for g in range(2)], axis=1
    )
    for g in range(2):
        mean1 = (acc[:, lanes(g)] * inv_own[:, lanes(g)]).astype(BF)
        block = jnp.concatenate([h1[me, 2 * g], h1[me, 2 * g + 1]], axis=1)
        pre2 = jnp.dot(w2st[...], block, preferred_element_type=F32) + jnp.dot(
            w2nt[...], mean1, preferred_element_type=F32
        )
        for half in range(2):
            h2[me, 2 * g + half] = jnp.maximum(pre2[:, quarter(half)], 0.0).astype(BF)
        g2.send(2, 2 * g)
        g2.send(1, 2 * g + 1)
    for slot, p in ((2, 1), (1, 0), (2, 3), (1, 2)):
        g2.send(slot, p)
    for p in range(4):
        g2.send(3, p)
    g2.own(4)
    for g in range(2):
        block = jnp.concatenate([h2[me, 2 * g], h2[me, 2 * g + 1]], axis=1)
        out_ref[:, lanes(g)] = jnp.dot(ws3t[...], block, preferred_element_type=F32)
    drain(ids_rcv, ids_ss)
    drain(yown, y_ss)
    drain(ssend, s_ss)
    drain(rs_send, r_ss)
    drain(h1.at[0:7], g1_ss)
    for p in range(4):
        g2.take(3, p)
    g2.add()
    for slot, p in ((2, 0), (1, 1), (2, 2), (1, 3)):
        g2.take(slot, p)
    g2.add()
    for slot, p in ((2, 1), (1, 0), (2, 3), (1, 2)):
        g2.take(slot, p)
    g2.take_forwards(4)
    g2.add()
    g2.take(0, 0)
    g2.take(0, 1)
    g2.take_forwards(4)
    g2.add()
    g2.take(0, 2)
    g2.take(0, 3)
    g2.take_forwards(2)
    g2.add()
    g2.take_forwards(2)
    g2.add()
    for g in range(2):
        mean2 = (acc[:, lanes(g)] * inv_own[:, lanes(g)]).astype(BF)
        out_ref[:, lanes(g)] += jnp.dot(wn3t[...], mean2, preferred_element_type=F32)
    drain(h2.at[0:7], g2_ss)


def solution(mesh):
    def device_step(feat, ws1, wn1, ids, mask, ws2, wn2, ws3, wn3):
        operands = (feat.T, ws1, wn1, ids.T, mask.T, ws2, wn2, ws3.T, wn3.T)
        vm = pl.BlockSpec(memory_space=pltpu.VMEM)
        dma = pltpu.SemaphoreType.DMA
        out_t = pl.pallas_call(
            kernel,
            out_shape=jax.ShapeDtypeStruct((7, BLK), F32),
            in_specs=[pl.BlockSpec(memory_space=pltpu.HBM)] * 9,
            out_specs=vm,
            scratch_shapes=[
                pltpu.VMEM((N_DEV, 192, BLK), BF),
                pltpu.VMEM((192, HID), BF),
                pltpu.VMEM((192, HID), BF),
                pltpu.VMEM((FAN, BLK), jnp.int32),
                pltpu.VMEM((FAN, BLK), jnp.int32),
                pltpu.VMEM((HID, HID), BF),
                pltpu.VMEM((HID, HID), BF),
                pltpu.VMEM((7, HID), BF),
                pltpu.VMEM((7, HID), BF),
                pltpu.VMEM((2 * HID, 192), BF),
                pltpu.VMEM((HID, HID), BF),
                pltpu.VMEM((HID, HID), BF),
                pltpu.VMEM((N_DEV, HID, BLK), BF),
                pltpu.VMEM((N_DEV, HID, BLK), BF),
                pltpu.VMEM((N_DEV, HID, BLK), BF),
                pltpu.VMEM((4, HID, BLK), F32),
                pltpu.VMEM((4, HID, BLK), BF),
                pltpu.VMEM((4, HID, BLK), BF),
                pltpu.VMEM((16, BLK), jnp.int16),
                pltpu.VMEM((3, 16, BLK), jnp.int16),
                pltpu.VMEM((8, 16, LANES), jnp.int32),
                pltpu.VMEM((HALF // TILE, TILE // 8, 8, LANES), jnp.int16),
                pltpu.VMEM((8, FAN, 8, LANES), jnp.int16),
                pltpu.VMEM((8, FAN, 8, LANES), BF),
                pltpu.VMEM((8, 8, LANES), F32),
                pltpu.VMEM((RING, 2, TILE // 8, 8, LANES), BF),
                pltpu.VMEM((N_DEV, BLK // 8, 8, BLK), BF),
                pltpu.VMEM((HID, BLK), F32),
                pltpu.VMEM((2, HID, LANES), F32),
                pltpu.VMEM((3, 4, HID, Q), BF),
                pltpu.VMEM((3, 4, HID, Q), BF),
                pltpu.VMEM((N_DEV, 4, HID, Q), BF),
                pltpu.VMEM((N_DEV, 4, HID, Q), BF),
                dma((8,)),
                dma,
                dma, dma((3,)),
                dma, dma,
                dma, dma,
                dma, dma((12,)),
                dma, dma((28,)),
                dma, dma((28,)),
            ],
            compiler_params=pltpu.CompilerParams(
                collective_id=0, has_side_effects=True, vmem_limit_bytes=32 * 1024 * 1024
            ),
            name="graphsage",
        )(*(pltpu.with_memory_space_constraint(a, pltpu.HBM) for a in operands))
        return out_t.T

    col_split = P(None, "g")
    row_split = P("g", None)
    replicated = P()
    return jax.shard_map(
        device_step,
        mesh=mesh,
        in_specs=(col_split, row_split, row_split, row_split, row_split, replicated, replicated, replicated, replicated),
        out_specs=row_split,
        check_vma=False,
    )
```

```python
import jax
import jax.numpy as jnp
from jax import lax
from jax.experimental import pallas as pl
from jax.experimental.pallas import tpu as pltpu
from jax.sharding import PartitionSpec as P

MESH = pl.DeviceIdType.MESH
N_DEV = 8
NODES = 4096
BLK = NODES // N_DEV
HALF = NODES // 2
FAN = 10
HID = 128
TILE = 256
LANES = 256
BF = jnp.bfloat16
F32 = jnp.float32


UNITS = (((2, 0), (1, 0)), ((0, 0), (0, 1)), ((2, 1), (1, 1)), ((0, 2), (0, 3)), ((2, 2), (1, 2)), ((2, 3), (1, 3)))
OWN = 6
RING = 6
Q = 128


def spread_ids(ids_s32, idb, wb, inv, u):
    words, weights = [], []
    degree = jnp.zeros((8, LANES), F32)
    for k in range(FAN):
        raw = jnp.broadcast_to(ids_s32[u, k : k + 1, :], (8, LANES))
        valid = raw >= 0
        degree += jnp.where(valid, 1.0, 0.0)
        upper = raw >= HALF
        word = jnp.where(upper, raw - HALF, raw)
        weight = jnp.where(valid, jnp.where(upper, 1.0, 0.0625), 0.0)
        for m in range(k):
            same = word == words[m]
            weights[m] = weights[m] + jnp.where(same, weight, 0.0)
            word = jnp.where(same, -1, word)
        words.append(word)
        weights.append(weight)
    inv[u] = 1.0 / degree
    for k in range(FAN):
        idb[u, k] = words[k].astype(jnp.int16)
        wb[u, k] = weights[k].astype(BF)


def build_tile(tile, row_ids, idb, wb, u, store_low, store_high):
    ids = [idb[u, k] for k in range(FAN)]
    wts = [wb[u, k] for k in range(FAN)]
    for r in range(0, TILE // 8, 8):
        rows = row_ids[tile, r : r + 8]
        acc = jnp.zeros((8, 8, LANES), BF)
        for k in range(FAN):
            acc = jnp.where(ids[k][None] == rows, wts[k][None], acc)
        high = jnp.floor(acc)
        store_high(r, high)
        store_low(r, acc - high)


def kernel(
    x_hbm, ws1_hbm, wn1_hbm, ids_hbm, mask_hbm, ws2_hbm, wn2_hbm, ws3_hbm, wn3_hbm, out_ref,
    x_v, ws1, wn1, ids_in, mask_in, ws2, wn2, ws3t, wn3t,
    w1t, w2st, w2nt, yown, yrecv, ysum, sown, ssend, srecv,
    ids_pkt, ids_rcv, ids_s32, row_ids, idb, wb, inv,
    ring, a_own, acc, zbase, rs_send, rs_recv, h1, h2,
    in_sem, x_sem, ids_ss, ids_rs, y_ss, y_rs, s_ss, s_rs, r_ss, r_rs, g1_ss, g1_rs, g2_ss, g2_rs,
):
    me = lax.axis_index("g")
    core = lax.rem(me, 2)
    cx = lax.rem(me // 2, 2)
    cy = me // 4
    partner = me + 1 - 2 * core
    steps = (6 - 4 * cx - 8 * cy, 4 - 8 * cy, 2 - 4 * cx)
    peers = tuple(partner + step for step in steps)
    mates = tuple(me + step for step in steps)
    mine, theirs = (me, *peers), (partner, *mates)

    barrier = pltpu.get_barrier_semaphore()
    for peer in (*peers, partner):
        pl.semaphore_signal(barrier, inc=1, device_id=(peer,), device_id_type=MESH)

    def fetch(src, dst, i):
        cp = pltpu.make_async_copy(src, dst, in_sem.at[i])
        cp.start()
        return cp

    ids_cp = fetch(ids_hbm, ids_in, 0)
    mask_cp = fetch(mask_hbm, mask_in, 1)
    w1_cps = [fetch(ws1_hbm, ws1, 2), fetch(wn1_hbm, wn1, 3)]
    for b in range(N_DEV):
        cp = pltpu.make_async_copy(x_hbm.at[:, pl.ds(b * BLK, BLK)], x_v.at[b], x_sem)
        cp.start()
    late_cps = [fetch(ws2_hbm, ws2, 4), fetch(wn2_hbm, wn2, 5), fetch(ws3_hbm, ws3t, 6), fetch(wn3_hbm, wn3t, 7)]

    def remote(src, dst, ss, rs, dev):
        return pltpu.make_async_remote_copy(
            src_ref=src, dst_ref=dst, send_sem=ss, recv_sem=rs, device_id=(dev,), device_id_type=MESH
        )

    def drain(ref, sem):
        pltpu.make_async_copy(ref, ref, sem).wait()

    row_shape = (TILE // 8, 8, LANES)
    row_base = lax.broadcasted_iota(jnp.int32, row_shape, 0) * 8 + lax.broadcasted_iota(jnp.int32, row_shape, 1)
    for tile in range(HALF // TILE):
        row_ids[tile] = (row_base + tile * TILE).astype(jnp.int16)
    ids_pkt[...] = jnp.full(ids_pkt.shape, -1, jnp.int16)
    ids_cp.wait()
    mask_cp.wait()
    masked = jnp.where(mask_in[...] > 0, ids_in[...], -1)
    ids_pkt[0:FAN, :] = masked.astype(jnp.int16)
    pl.semaphore_wait(barrier, 4)
    id_copies = [remote(ids_pkt, ids_rcv.at[s], ids_ss, ids_rs.at[s], peers[s]) for s in range(3)]
    for s in (2, 1, 0):
        id_copies[s].start()
    for g in range(2):
        ids_s32[OWN + g, 0:FAN, :] = masked[:, g * LANES : (g + 1) * LANES]
        spread_ids(ids_s32, idb, wb, inv, OWN + g)
    for cp in w1_cps:
        cp.wait()
    w1t[0:HID, :] = ws1[...].T
    w1t[HID:, :] = wn1[...].T

    def build_own(tile, g):
        def put(half):
            def store(r, v):
                v = v if half else v * jnp.array(16.0, BF)
                row = tile % 2 * (TILE // 8) + r
                a_own[half * 4 + tile // 2, row : row + 8, :, g * LANES : (g + 1) * LANES] = v

            return store

        build_tile(tile, row_ids, idb, wb, OWN + g, put(0), put(1))

    drain(x_v, x_sem)
    for i in range(4):
        part = jnp.dot(w1t[...], x_v[theirs[i]], preferred_element_type=F32)
        yown[theirs[i]] = part[HID:].astype(BF)
        ssend[i] = part[:HID].astype(BF)
        part2 = jnp.dot(w1t[...], x_v[mine[i]], preferred_element_type=F32)
        yown[mine[i]] = part2[HID:].astype(BF)
        sown[i] = part2[:HID]
        for b in (theirs[i], mine[i]):
            remote(yown.at[b], yrecv.at[b], y_ss, y_rs, partner).start()
        build_own(2 * i, 0)
    for i in range(4):
        remote(ssend.at[i], srecv.at[i], s_ss, s_rs, partner).start()
    for tile in range(1, 8, 2):
        build_own(tile, 0)
    for cp in late_cps:
        cp.wait()
    w2st[...] = ws2[...].T
    w2nt[...] = wn2[...].T

    def build_into(flat):
        def put(half):
            def store(r, v):
                ring[flat % RING, half, r : r + 8] = v

            return store

        build_tile(flat % 8, row_ids, idb, wb, flat // 8, put(0), put(1))

    def dot_from(flat):
        tile = flat % 8
        cols = slice(tile % 2 * TILE, (tile % 2 + 1) * TILE)
        low = ring[flat % RING, 0].reshape(TILE, LANES)
        high = ring[flat % RING, 1].reshape(TILE, LANES)
        return (
            jnp.dot(ysum[tile // 2, :, cols], low, preferred_element_type=F32),
            jnp.dot(ysum[4 + tile // 2, :, cols], high, preferred_element_type=F32),
        )

    def lanes(g):
        return slice(g * LANES, (g + 1) * LANES)

    def quarter(q):
        return slice(q * Q, (q + 1) * Q)

    def take_ids(s):
        id_copies[s].wait_recv()
        for u, pair in enumerate(UNITS):
            for half, (slot, q) in enumerate(pair):
                if slot == s:
                    ids_s32[u, :, quarter(half)] = ids_rcv[s, :, quarter(q)].astype(jnp.int32)

    rs_copies = {}

    def finish_unit(u, low, high):
        total = (low * 16.0 + high) * jnp.broadcast_to(inv[u, 0:1, :], (HID, LANES))
        for half, (s, q) in enumerate(UNITS[u]):
            part = total[:, quarter(half)] + sown[1 + s, :, quarter(q)] + srecv[1 + s, :, quarter(q)].astype(F32)
            rs_send[s, q] = part.astype(BF)
            rs_copies[s, q] = remote(rs_send.at[s, q], rs_recv.at[s, q], r_ss, r_rs.at[4 * s + q], peers[s])
            rs_copies[s, q].start()

    def own_piece(b, g):
        return jnp.dot(ysum[b], a_own[b, :, :, lanes(g)].reshape(BLK, LANES), preferred_element_type=F32)

    def own_base(g, own):
        base = own * jnp.broadcast_to(inv[OWN + g, 0:1, :], (HID, LANES))
        zbase[g] = base + sown[0, :, lanes(g)] + srecv[0, :, lanes(g)].astype(F32)

    def own_dot(h, b, p):
        rows = a_own[b, p * Q // 8 : (p + 1) * Q // 8].reshape(Q, BLK)
        return jnp.dot(h[b, p], rows, preferred_element_type=F32)

    class Gather:
        def __init__(self, h, ss, rs, direct):
            self.h, self.ss, self.rs, self.direct = h, ss, rs, direct
            self.copies, self.forwards, self.ready = {}, [], []

        def copy(self, block, p, slot, dev):
            return remote(self.h.at[block, p], self.h.at[block, p], self.ss, self.rs.at[7 * p + slot], dev)

        def send(self, slot, p):
            dev = partner if slot == 3 else peers[slot]
            self.copies[slot, p] = self.copy(me, p, slot, dev)
            self.copies[slot, p].start()

        def take(self, slot, p):
            self.copies[slot, p].wait_recv()
            block = partner if slot == 3 else mates[0] if slot == 0 and p not in self.direct else peers[slot]
            if p not in self.direct and slot == (1 if p % 2 else 2):
                self.copies[0, p] = self.copy(block, p, 0, peers[3 - slot])
                self.copies[0, p].start()
            if slot < 3:
                fwd = self.copy(block, p, 4 + slot, partner)
                fwd.start()
                self.forwards.append((slot, p, fwd))
            self.ready.append((block, p))

        def take_forwards(self, n):
            for slot, p, fwd in self.forwards[:n]:
                fwd.wait_recv()
                relayed = slot == 0 and p not in self.direct
                self.ready.append((peers[0] if relayed else mates[slot], p))
            self.forwards = self.forwards[n:]

        def own(self, pieces):
            acc[...] = sum(own_dot(self.h, me, p) for p in range(pieces))

        def add(self):
            acc[...] += sum(own_dot(self.h, b, p) for b, p in self.ready)
            self.ready = []

    g1 = Gather(h1, g1_ss, g1_rs, direct=(3,))
    g2 = Gather(h2, g2_ss, g2_rs, direct=())

    def finish_quarter(q):
        z = zbase[q // 2, :, quarter(q % 2)]
        for t in (1, 2, 0):
            rs_copies[t, q].wait_recv()
            z = z + rs_recv[t, q].astype(F32)
        h1[me, q] = jnp.maximum(z, 0.0).astype(BF)
        for slot in (0, 2, 1, 3) if q in g1.direct else (2, 1, 3):
            g1.send(slot, q)

    take_ids(2)
    take_ids(1)
    spread_ids(ids_s32, idb, wb, inv, 0)
    lead = 3
    for flat in range(lead):
        build_into(flat)
    drain(yrecv, y_rs)
    for b in range(N_DEV):
        ysum[b] = yown[b] + yrecv[b]
    built = lead
    low = high = own = None
    for flat in range(48):
        u, tile = flat // 8, flat % 8
        while built < 48 and built - flat < 2 or (built < 48 and tile % 2 == 0 and built - flat < lead):
            if built == 8:
                take_ids(0)
            if built % 8 == 0:
                spread_ids(ids_s32, idb, wb, inv, built // 8)
            build_into(built)
            built += 1
        part = dot_from(flat)
        low = part[0] if low is None else low + part[0]
        high = part[1] if high is None else high + part[1]
        if u == 1:
            own = own_piece(tile, 0) if own is None else own + own_piece(tile, 0)
        if tile == 7:
            if u == 0:
                drain(srecv, s_rs)
            finish_unit(u, low, high)
            low = high = None
            if u == 1:
                own_base(0, own)
    finish_quarter(0)
    finish_quarter(1)
    for tile in range(8):
        build_own(tile, 1)
    own_base(1, sum(own_piece(b, 1) for b in range(N_DEV)))
    finish_quarter(2)
    finish_quarter(3)
    g1.own(4)
    for g in range(2):
        block = jnp.concatenate([h1[me, 2 * g], h1[me, 2 * g + 1]], axis=1)
        zbase[g] = jnp.dot(w2st[...], block, preferred_element_type=F32)
    for slot, p in ((2, 0), (1, 0), (1, 1), (2, 1), (2, 2), (1, 2)):
        g1.take(slot, p)
    for p in range(4):
        g1.take(3, p)
    g1.add()
    g1.take(0, 0)
    g1.take(0, 1)
    g1.take_forwards(6)
    g1.add()
    for slot, p in ((2, 3), (1, 3), (0, 3), (0, 2)):
        g1.take(slot, p)
    g1.add()
    g1.take_forwards(4)
    g1.add()
    g1.take_forwards(2)
    g1.add()

    inv_own = jnp.concatenate(
        [jnp.broadcast_to(inv[OWN + g, 0:1, :], (HID, LANES)) for g in range(2)], axis=1
    )
    for g in range(2):
        mean1 = (acc[:, lanes(g)] * inv_own[:, lanes(g)]).astype(BF)
        pre2 = zbase[g] + jnp.dot(w2nt[...], mean1, preferred_element_type=F32)
        for half in range(2):
            h2[me, 2 * g + half] = jnp.maximum(pre2[:, quarter(half)], 0.0).astype(BF)
        g2.send(2, 2 * g)
        g2.send(1, 2 * g + 1)
    for slot, p in ((2, 1), (1, 0), (2, 3), (1, 2)):
        g2.send(slot, p)
    for p in range(4):
        g2.send(3, p)
    g2.own(4)
    for g in range(2):
        block = jnp.concatenate([h2[me, 2 * g], h2[me, 2 * g + 1]], axis=1)
        out_ref[:, lanes(g)] = jnp.dot(ws3t[...], block, preferred_element_type=F32)
    drain(ids_rcv, ids_ss)
    drain(yown, y_ss)
    drain(ssend, s_ss)
    drain(rs_send, r_ss)
    drain(h1.at[0:7], g1_ss)
    for p in range(4):
        g2.take(3, p)
    g2.add()
    for slot, p in ((2, 0), (1, 1), (2, 2), (1, 3)):
        g2.take(slot, p)
    g2.add()
    for slot, p in ((2, 1), (1, 0), (2, 3), (1, 2)):
        g2.take(slot, p)
    g2.take_forwards(4)
    g2.add()
    g2.take(0, 0)
    g2.take(0, 1)
    g2.take_forwards(4)
    g2.add()
    g2.take(0, 2)
    g2.take(0, 3)
    g2.take_forwards(2)
    g2.add()
    g2.take_forwards(2)
    g2.add()
    for g in range(2):
        mean2 = (acc[:, lanes(g)] * inv_own[:, lanes(g)]).astype(BF)
        out_ref[:, lanes(g)] += jnp.dot(wn3t[...], mean2, preferred_element_type=F32)
    drain(h2.at[0:7], g2_ss)


def solution(mesh):
    def device_step(feat, ws1, wn1, ids, mask, ws2, wn2, ws3, wn3):
        operands = (feat.T, ws1, wn1, ids.T, mask.T, ws2, wn2, ws3.T, wn3.T)
        vm = pl.BlockSpec(memory_space=pltpu.VMEM)
        dma = pltpu.SemaphoreType.DMA
        out_t = pl.pallas_call(
            kernel,
            out_shape=jax.ShapeDtypeStruct((7, BLK), F32),
            in_specs=[pl.BlockSpec(memory_space=pltpu.HBM)] * 9,
            out_specs=vm,
            scratch_shapes=[
                pltpu.VMEM((N_DEV, 192, BLK), BF),
                pltpu.VMEM((192, HID), BF),
                pltpu.VMEM((192, HID), BF),
                pltpu.VMEM((FAN, BLK), jnp.int32),
                pltpu.VMEM((FAN, BLK), jnp.int32),
                pltpu.VMEM((HID, HID), BF),
                pltpu.VMEM((HID, HID), BF),
                pltpu.VMEM((7, HID), BF),
                pltpu.VMEM((7, HID), BF),
                pltpu.VMEM((2 * HID, 192), BF),
                pltpu.VMEM((HID, HID), BF),
                pltpu.VMEM((HID, HID), BF),
                pltpu.VMEM((N_DEV, HID, BLK), BF),
                pltpu.VMEM((N_DEV, HID, BLK), BF),
                pltpu.VMEM((N_DEV, HID, BLK), BF),
                pltpu.VMEM((4, HID, BLK), F32),
                pltpu.VMEM((4, HID, BLK), BF),
                pltpu.VMEM((4, HID, BLK), BF),
                pltpu.VMEM((16, BLK), jnp.int16),
                pltpu.VMEM((3, 16, BLK), jnp.int16),
                pltpu.VMEM((8, 16, LANES), jnp.int32),
                pltpu.VMEM((HALF // TILE, TILE // 8, 8, LANES), jnp.int16),
                pltpu.VMEM((8, FAN, 8, LANES), jnp.int16),
                pltpu.VMEM((8, FAN, 8, LANES), BF),
                pltpu.VMEM((8, 8, LANES), F32),
                pltpu.VMEM((RING, 2, TILE // 8, 8, LANES), BF),
                pltpu.VMEM((N_DEV, BLK // 8, 8, BLK), BF),
                pltpu.VMEM((HID, BLK), F32),
                pltpu.VMEM((2, HID, LANES), F32),
                pltpu.VMEM((3, 4, HID, Q), BF),
                pltpu.VMEM((3, 4, HID, Q), BF),
                pltpu.VMEM((N_DEV, 4, HID, Q), BF),
                pltpu.VMEM((N_DEV, 4, HID, Q), BF),
                dma((8,)),
                dma,
                dma, dma((3,)),
                dma, dma,
                dma, dma,
                dma, dma((12,)),
                dma, dma((28,)),
                dma, dma((28,)),
            ],
            compiler_params=pltpu.CompilerParams(
                collective_id=0, has_side_effects=True, vmem_limit_bytes=32 * 1024 * 1024
            ),
            name="graphsage",
        )(*(pltpu.with_memory_space_constraint(a, pltpu.HBM) for a in operands))
        return out_t.T

    col_split = P(None, "g")
    row_split = P("g", None)
    replicated = P()
    return jax.shard_map(
        device_step,
        mesh=mesh,
        in_specs=(col_split, row_split, row_split, row_split, row_split, replicated, replicated, replicated, replicated),
        out_specs=row_split,
        check_vma=False,
    )
```

```python
import jax
import jax.numpy as jnp
from jax import lax
from jax.experimental import pallas as pl
from jax.experimental.pallas import tpu as pltpu
from jax.sharding import PartitionSpec as P

MESH = pl.DeviceIdType.MESH
N_DEV = 8
NODES = 4096
BLK = NODES // N_DEV
HALF = NODES // 2
FAN = 10
HID = 128
TILE = 256
LANES = 256
BF = jnp.bfloat16
F32 = jnp.float32


UNITS = (((2, 0), (1, 0)), ((0, 0), (0, 1)), ((2, 1), (1, 1)), ((0, 2), (0, 3)), ((2, 2), (1, 2)), ((2, 3), (1, 3)))
OWN = 6
RING = 6
Q = 128


def spread_ids(ids_s32, idb, wb, inv, u):
    words, weights = [], []
    degree = jnp.zeros((8, LANES), F32)
    for k in range(FAN):
        raw = jnp.broadcast_to(ids_s32[u, k : k + 1, :], (8, LANES))
        valid = raw >= 0
        degree += jnp.where(valid, 1.0, 0.0)
        upper = raw >= HALF
        word = jnp.where(upper, raw - HALF, raw)
        weight = jnp.where(valid, jnp.where(upper, 1.0, 0.0625), 0.0)
        for m in range(k):
            same = word == words[m]
            weights[m] = weights[m] + jnp.where(same, weight, 0.0)
            word = jnp.where(same, -1, word)
        words.append(word)
        weights.append(weight)
    inv[u] = 1.0 / degree
    for k in range(FAN):
        idb[u, k] = words[k].astype(jnp.int16)
        wb[u, k] = weights[k].astype(BF)


def build_tile(tile, row_ids, idb, wb, u, store_low, store_high):
    ids = [idb[u, k] for k in range(FAN)]
    wts = [wb[u, k] for k in range(FAN)]
    for r in range(0, TILE // 8, 8):
        rows = row_ids[tile, r : r + 8]
        acc = jnp.zeros((8, 8, LANES), BF)
        for k in range(FAN):
            acc = jnp.where(ids[k][None] == rows, wts[k][None], acc)
        high = jnp.floor(acc)
        store_high(r, high)
        store_low(r, acc - high)


def kernel(
    x_hbm, ws1_hbm, wn1_hbm, ids_hbm, mask_hbm, ws2_hbm, wn2_hbm, ws3_hbm, wn3_hbm, out_ref,
    x_v, ws1, wn1, ids_in, mask_in, ws2, wn2, ws3t, wn3t,
    w1t, w2st, w2nt, yown, yrecv, ysum, sown, ssend, srecv,
    ids_pkt, ids_rcv, ids_s32, row_ids, idb, wb, inv,
    ring, a_own, acc, zbase, rs_send, rs_recv, h1, h2,
    in_sem, x_sem, ids_ss, ids_rs, y_ss, y_rs, s_ss, s_rs, r_ss, r_rs, g1_ss, g1_rs, g2_ss, g2_rs,
):
    me = lax.axis_index("g")
    core = lax.rem(me, 2)
    cx = lax.rem(me // 2, 2)
    cy = me // 4
    partner = me + 1 - 2 * core
    steps = (6 - 4 * cx - 8 * cy, 4 - 8 * cy, 2 - 4 * cx)
    peers = tuple(partner + step for step in steps)
    mates = tuple(me + step for step in steps)
    mine, theirs = (me, *peers), (partner, *mates)

    barrier = pltpu.get_barrier_semaphore()
    for peer in (*peers, partner):
        pl.semaphore_signal(barrier, inc=1, device_id=(peer,), device_id_type=MESH)

    def fetch(src, dst, i):
        cp = pltpu.make_async_copy(src, dst, in_sem.at[i])
        cp.start()
        return cp

    ids_cp = fetch(ids_hbm, ids_in, 0)
    mask_cp = fetch(mask_hbm, mask_in, 1)
    w1_cps = [fetch(ws1_hbm, ws1, 2), fetch(wn1_hbm, wn1, 3)]
    for b in range(N_DEV):
        cp = pltpu.make_async_copy(x_hbm.at[:, pl.ds(b * BLK, BLK)], x_v.at[b], x_sem)
        cp.start()
    late_cps = [fetch(ws2_hbm, ws2, 4), fetch(wn2_hbm, wn2, 5), fetch(ws3_hbm, ws3t, 6), fetch(wn3_hbm, wn3t, 7)]

    def remote(src, dst, ss, rs, dev):
        return pltpu.make_async_remote_copy(
            src_ref=src, dst_ref=dst, send_sem=ss, recv_sem=rs, device_id=(dev,), device_id_type=MESH
        )

    def drain(ref, sem):
        pltpu.make_async_copy(ref, ref, sem).wait()

    row_shape = (TILE // 8, 8, LANES)
    row_base = lax.broadcasted_iota(jnp.int32, row_shape, 0) * 8 + lax.broadcasted_iota(jnp.int32, row_shape, 1)
    for tile in range(HALF // TILE):
        row_ids[tile] = (row_base + tile * TILE).astype(jnp.int16)
    ids_pkt[...] = jnp.full(ids_pkt.shape, -1, jnp.int16)
    ids_cp.wait()
    mask_cp.wait()
    masked = jnp.where(mask_in[...] > 0, ids_in[...], -1)
    ids_pkt[0:FAN, :] = masked.astype(jnp.int16)
    pl.semaphore_wait(barrier, 4)
    id_copies = [remote(ids_pkt, ids_rcv.at[s], ids_ss, ids_rs.at[s], peers[s]) for s in range(3)]
    for s in (2, 1, 0):
        id_copies[s].start()
    for g in range(2):
        ids_s32[OWN + g, 0:FAN, :] = masked[:, g * LANES : (g + 1) * LANES]
        spread_ids(ids_s32, idb, wb, inv, OWN + g)
    for cp in w1_cps:
        cp.wait()
    w1t[0:HID, :] = ws1[...].T
    w1t[HID:, :] = wn1[...].T

    def build_own(tile, g):
        def put(half):
            def store(r, v):
                v = v if half else v * jnp.array(16.0, BF)
                row = tile % 2 * (TILE // 8) + r
                a_own[half * 4 + tile // 2, row : row + 8, :, g * LANES : (g + 1) * LANES] = v

            return store

        build_tile(tile, row_ids, idb, wb, OWN + g, put(0), put(1))

    drain(x_v, x_sem)
    for i in range(4):
        part = jnp.dot(w1t[...], x_v[theirs[i]], preferred_element_type=F32)
        yown[theirs[i]] = part[HID:].astype(BF)
        ssend[i] = part[:HID].astype(BF)
        part2 = jnp.dot(w1t[...], x_v[mine[i]], preferred_element_type=F32)
        yown[mine[i]] = part2[HID:].astype(BF)
        sown[i] = part2[:HID]
        for b in (theirs[i], mine[i]):
            remote(yown.at[b], yrecv.at[b], y_ss, y_rs, partner).start()
        build_own(2 * i, 0)
    for i in range(4):
        remote(ssend.at[i], srecv.at[i], s_ss, s_rs, partner).start()
    for tile in range(1, 8, 2):
        build_own(tile, 0)
    for cp in late_cps:
        cp.wait()
    w2st[...] = ws2[...].T
    w2nt[...] = wn2[...].T

    def build_into(flat):
        def put(half):
            def store(r, v):
                ring[flat % RING, half, r : r + 8] = v

            return store

        build_tile(flat % 8, row_ids, idb, wb, flat // 8, put(0), put(1))

    def dot_from(flat):
        tile = flat % 8
        cols = slice(tile % 2 * TILE, (tile % 2 + 1) * TILE)
        low = ring[flat % RING, 0].reshape(TILE, LANES)
        high = ring[flat % RING, 1].reshape(TILE, LANES)
        return (
            jnp.dot(ysum[tile // 2, :, cols], low, preferred_element_type=F32),
            jnp.dot(ysum[4 + tile // 2, :, cols], high, preferred_element_type=F32),
        )

    def lanes(g):
        return slice(g * LANES, (g + 1) * LANES)

    def quarter(q):
        return slice(q * Q, (q + 1) * Q)

    def take_ids(s):
        id_copies[s].wait_recv()
        for u, pair in enumerate(UNITS):
            for half, (slot, q) in enumerate(pair):
                if slot == s:
                    ids_s32[u, :, quarter(half)] = ids_rcv[s, :, quarter(q)].astype(jnp.int32)

    rs_copies = {}

    def finish_unit(u, low, high):
        total = (low * 16.0 + high) * jnp.broadcast_to(inv[u, 0:1, :], (HID, LANES))
        for half, (s, q) in enumerate(UNITS[u]):
            part = total[:, quarter(half)] + sown[1 + s, :, quarter(q)] + srecv[1 + s, :, quarter(q)].astype(F32)
            rs_send[s, q] = part.astype(BF)
            rs_copies[s, q] = remote(rs_send.at[s, q], rs_recv.at[s, q], r_ss, r_rs.at[4 * s + q], peers[s])
            rs_copies[s, q].start()

    def own_piece(b, g):
        return jnp.dot(ysum[b], a_own[b, :, :, lanes(g)].reshape(BLK, LANES), preferred_element_type=F32)

    def own_base(g, own):
        base = own * jnp.broadcast_to(inv[OWN + g, 0:1, :], (HID, LANES))
        zbase[g] = base + sown[0, :, lanes(g)] + srecv[0, :, lanes(g)].astype(F32)

    def own_dot(h, b, p):
        rows = a_own[b, p * Q // 8 : (p + 1) * Q // 8].reshape(Q, BLK)
        return jnp.dot(h[b, p], rows, preferred_element_type=F32)

    class Gather:
        def __init__(self, h, ss, rs, direct):
            self.h, self.ss, self.rs, self.direct = h, ss, rs, direct
            self.copies, self.forwards, self.ready = {}, [], []

        def copy(self, block, p, slot, dev):
            return remote(self.h.at[block, p], self.h.at[block, p], self.ss, self.rs.at[7 * p + slot], dev)

        def send(self, slot, p):
            dev = partner if slot == 3 else peers[slot]
            self.copies[slot, p] = self.copy(me, p, slot, dev)
            self.copies[slot, p].start()

        def take(self, slot, p):
            self.copies[slot, p].wait_recv()
            block = partner if slot == 3 else mates[0] if slot == 0 and p not in self.direct else peers[slot]
            if p not in self.direct and slot == (1 if p % 2 else 2):
                self.copies[0, p] = self.copy(block, p, 0, peers[3 - slot])
                self.copies[0, p].start()
            if slot < 3:
                fwd = self.copy(block, p, 4 + slot, partner)
                fwd.start()
                self.forwards.append((slot, p, fwd))
            self.ready.append((block, p))

        def take_forwards(self, n):
            for slot, p, fwd in self.forwards[:n]:
                fwd.wait_recv()
                relayed = slot == 0 and p not in self.direct
                self.ready.append((peers[0] if relayed else mates[slot], p))
            self.forwards = self.forwards[n:]

        def own(self, pieces):
            acc[...] = sum(own_dot(self.h, me, p) for p in range(pieces))

        def add(self):
            acc[...] += sum(own_dot(self.h, b, p) for b, p in self.ready)
            self.ready = []

    g1 = Gather(h1, g1_ss, g1_rs, direct=(3,))
    g2 = Gather(h2, g2_ss, g2_rs, direct=())

    def finish_quarter(q):
        z = zbase[q // 2, :, quarter(q % 2)]
        for t in (1, 2, 0):
            rs_copies[t, q].wait_recv()
            z = z + rs_recv[t, q].astype(F32)
        h1[me, q] = jnp.maximum(z, 0.0).astype(BF)
        for slot in (0, 2, 1, 3) if q in g1.direct else (2, 1, 3):
            g1.send(slot, q)

    take_ids(2)
    take_ids(1)
    spread_ids(ids_s32, idb, wb, inv, 0)
    lead = 3
    for flat in range(lead):
        build_into(flat)
    drain(yrecv, y_rs)
    for b in range(N_DEV):
        ysum[b] = yown[b] + yrecv[b]
    built = lead
    low = high = own = None
    for flat in range(48):
        u, tile = flat // 8, flat % 8
        while built < 48 and built - flat < 2 or (built < 48 and tile % 2 == 0 and built - flat < lead):
            if built == 8:
                take_ids(0)
            if built % 8 == 0:
                spread_ids(ids_s32, idb, wb, inv, built // 8)
            build_into(built)
            built += 1
        part = dot_from(flat)
        low = part[0] if low is None else low + part[0]
        high = part[1] if high is None else high + part[1]
        if u == 1:
            own = own_piece(tile, 0) if own is None else own + own_piece(tile, 0)
        if tile == 7:
            if u == 0:
                drain(srecv, s_rs)
            finish_unit(u, low, high)
            low = high = None
            if u == 1:
                own_base(0, own)
    for tile in range(8):
        build_own(tile, 1)
    finish_quarter(0)
    finish_quarter(1)
    own_base(1, sum(own_piece(b, 1) for b in range(N_DEV)))
    finish_quarter(2)
    finish_quarter(3)
    g1.own(4)
    for g in range(2):
        block = jnp.concatenate([h1[me, 2 * g], h1[me, 2 * g + 1]], axis=1)
        zbase[g] = jnp.dot(w2st[...], block, preferred_element_type=F32)
    for slot, p in ((2, 0), (1, 0), (1, 1), (2, 1), (2, 2), (1, 2)):
        g1.take(slot, p)
    for p in range(4):
        g1.take(3, p)
    g1.add()
    g1.take(0, 0)
    g1.take(0, 1)
    g1.take_forwards(6)
    g1.add()
    for slot, p in ((2, 3), (1, 3), (0, 3), (0, 2)):
        g1.take(slot, p)
    g1.add()
    g1.take_forwards(4)
    g1.add()
    g1.take_forwards(2)
    g1.add()

    inv_own = jnp.concatenate(
        [jnp.broadcast_to(inv[OWN + g, 0:1, :], (HID, LANES)) for g in range(2)], axis=1
    )
    for g in range(2):
        mean1 = (acc[:, lanes(g)] * inv_own[:, lanes(g)]).astype(BF)
        pre2 = zbase[g] + jnp.dot(w2nt[...], mean1, preferred_element_type=F32)
        for half in range(2):
            h2[me, 2 * g + half] = jnp.maximum(pre2[:, quarter(half)], 0.0).astype(BF)
        g2.send(2, 2 * g)
        g2.send(1, 2 * g + 1)
    for slot, p in ((2, 1), (1, 0), (2, 3), (1, 2)):
        g2.send(slot, p)
    for p in range(4):
        g2.send(3, p)
    g2.own(4)
    for g in range(2):
        block = jnp.concatenate([h2[me, 2 * g], h2[me, 2 * g + 1]], axis=1)
        out_ref[:, lanes(g)] = jnp.dot(ws3t[...], block, preferred_element_type=F32)
    drain(ids_rcv, ids_ss)
    drain(yown, y_ss)
    drain(ssend, s_ss)
    drain(rs_send, r_ss)
    drain(h1.at[0:7], g1_ss)
    for p in range(4):
        g2.take(3, p)
    g2.add()
    for slot, p in ((2, 0), (1, 1), (2, 2), (1, 3)):
        g2.take(slot, p)
    g2.add()
    for slot, p in ((2, 1), (1, 0), (2, 3), (1, 2)):
        g2.take(slot, p)
    g2.take_forwards(4)
    g2.add()
    g2.take(0, 0)
    g2.take(0, 1)
    g2.take_forwards(4)
    g2.add()
    g2.take(0, 2)
    g2.take(0, 3)
    g2.take_forwards(2)
    g2.add()
    g2.take_forwards(2)
    g2.add()
    for g in range(2):
        mean2 = (acc[:, lanes(g)] * inv_own[:, lanes(g)]).astype(BF)
        out_ref[:, lanes(g)] += jnp.dot(wn3t[...], mean2, preferred_element_type=F32)
    drain(h2.at[0:7], g2_ss)


def solution(mesh):
    def device_step(feat, ws1, wn1, ids, mask, ws2, wn2, ws3, wn3):
        operands = (feat.T, ws1, wn1, ids.T, mask.T, ws2, wn2, ws3.T, wn3.T)
        vm = pl.BlockSpec(memory_space=pltpu.VMEM)
        dma = pltpu.SemaphoreType.DMA
        out_t = pl.pallas_call(
            kernel,
            out_shape=jax.ShapeDtypeStruct((7, BLK), F32),
            in_specs=[pl.BlockSpec(memory_space=pltpu.HBM)] * 9,
            out_specs=vm,
            scratch_shapes=[
                pltpu.VMEM((N_DEV, 192, BLK), BF),
                pltpu.VMEM((192, HID), BF),
                pltpu.VMEM((192, HID), BF),
                pltpu.VMEM((FAN, BLK), jnp.int32),
                pltpu.VMEM((FAN, BLK), jnp.int32),
                pltpu.VMEM((HID, HID), BF),
                pltpu.VMEM((HID, HID), BF),
                pltpu.VMEM((7, HID), BF),
                pltpu.VMEM((7, HID), BF),
                pltpu.VMEM((2 * HID, 192), BF),
                pltpu.VMEM((HID, HID), BF),
                pltpu.VMEM((HID, HID), BF),
                pltpu.VMEM((N_DEV, HID, BLK), BF),
                pltpu.VMEM((N_DEV, HID, BLK), BF),
                pltpu.VMEM((N_DEV, HID, BLK), BF),
                pltpu.VMEM((4, HID, BLK), F32),
                pltpu.VMEM((4, HID, BLK), BF),
                pltpu.VMEM((4, HID, BLK), BF),
                pltpu.VMEM((16, BLK), jnp.int16),
                pltpu.VMEM((3, 16, BLK), jnp.int16),
                pltpu.VMEM((8, 16, LANES), jnp.int32),
                pltpu.VMEM((HALF // TILE, TILE // 8, 8, LANES), jnp.int16),
                pltpu.VMEM((8, FAN, 8, LANES), jnp.int16),
                pltpu.VMEM((8, FAN, 8, LANES), BF),
                pltpu.VMEM((8, 8, LANES), F32),
                pltpu.VMEM((RING, 2, TILE // 8, 8, LANES), BF),
                pltpu.VMEM((N_DEV, BLK // 8, 8, BLK), BF),
                pltpu.VMEM((HID, BLK), F32),
                pltpu.VMEM((2, HID, LANES), F32),
                pltpu.VMEM((3, 4, HID, Q), BF),
                pltpu.VMEM((3, 4, HID, Q), BF),
                pltpu.VMEM((N_DEV, 4, HID, Q), BF),
                pltpu.VMEM((N_DEV, 4, HID, Q), BF),
                dma((8,)),
                dma,
                dma, dma((3,)),
                dma, dma,
                dma, dma,
                dma, dma((12,)),
                dma, dma((28,)),
                dma, dma((28,)),
            ],
            compiler_params=pltpu.CompilerParams(
                collective_id=0, has_side_effects=True, vmem_limit_bytes=32 * 1024 * 1024
            ),
            name="graphsage",
        )(*(pltpu.with_memory_space_constraint(a, pltpu.HBM) for a in operands))
        return out_t.T

    col_split = P(None, "g")
    row_split = P("g", None)
    replicated = P()
    return jax.shard_map(
        device_step,
        mesh=mesh,
        in_specs=(col_split, row_split, row_split, row_split, row_split, replicated, replicated, replicated, replicated),
        out_specs=row_split,
        check_vma=False,
    )
```

```python
import jax
import jax.numpy as jnp
from jax import lax
from jax.experimental import pallas as pl
from jax.experimental.pallas import tpu as pltpu
from jax.sharding import PartitionSpec as P

MESH = pl.DeviceIdType.MESH
N_DEV = 8
NODES = 4096
BLK = NODES // N_DEV
HALF = NODES // 2
FAN = 10
HID = 128
TILE = 256
LANES = 256
BF = jnp.bfloat16
F32 = jnp.float32


UNITS = (((2, 0), (1, 0)), ((2, 1), (1, 1)), ((0, 0), (0, 1)), ((0, 2), (0, 3)), ((2, 2), (1, 2)), ((2, 3), (1, 3)))
OWN = 6
RING = 6
Q = 128


def spread_ids(ids_s32, idb, wb, inv, u):
    words, weights = [], []
    degree = jnp.zeros((8, LANES), F32)
    for k in range(FAN):
        raw = jnp.broadcast_to(ids_s32[u, k : k + 1, :], (8, LANES))
        valid = raw >= 0
        degree += jnp.where(valid, 1.0, 0.0)
        upper = raw >= HALF
        word = jnp.where(upper, raw - HALF, raw)
        weight = jnp.where(valid, jnp.where(upper, 1.0, 0.0625), 0.0)
        for m in range(k):
            same = word == words[m]
            weights[m] = weights[m] + jnp.where(same, weight, 0.0)
            word = jnp.where(same, -1, word)
        words.append(word)
        weights.append(weight)
    inv[u] = 1.0 / degree
    for k in range(FAN):
        idb[u, k] = words[k].astype(jnp.int16)
        wb[u, k] = weights[k].astype(BF)


def build_tile(tile, row_ids, idb, wb, u, store_low, store_high):
    ids = [idb[u, k] for k in range(FAN)]
    wts = [wb[u, k] for k in range(FAN)]
    for r in range(0, TILE // 8, 8):
        rows = row_ids[tile, r : r + 8]
        acc = jnp.zeros((8, 8, LANES), BF)
        for k in range(FAN):
            acc = jnp.where(ids[k][None] == rows, wts[k][None], acc)
        high = jnp.floor(acc)
        store_high(r, high)
        store_low(r, acc - high)


def kernel(
    x_hbm, ws1_hbm, wn1_hbm, ids_hbm, mask_hbm, ws2_hbm, wn2_hbm, ws3_hbm, wn3_hbm, out_ref,
    x_v, ws1, wn1, ids_in, mask_in, ws2, wn2, ws3t, wn3t,
    w1t, w2st, w2nt, yown, yrecv, ysum, sown, ssend, srecv,
    ids_pkt, ids_rcv, ids_s32, row_ids, idb, wb, inv,
    ring, a_own, acc, zbase, rs_send, rs_recv, h1, h2,
    in_sem, x_sem, ids_ss, ids_rs, y_ss, y_rs, s_ss, s_rs, r_ss, r_rs, g1_ss, g1_rs, g2_ss, g2_rs, go_sem,
):
    me = lax.axis_index("g")
    core = lax.rem(me, 2)
    cx = lax.rem(me // 2, 2)
    cy = me // 4
    partner = me + 1 - 2 * core
    steps = (6 - 4 * cx - 8 * cy, 4 - 8 * cy, 2 - 4 * cx)
    peers = (me + steps[0], partner + steps[1], partner + steps[2])
    mates = (partner + steps[0], me + steps[1], me + steps[2])
    mine, theirs = (me, *peers), (partner, *mates)

    barrier = pltpu.get_barrier_semaphore()
    for peer in (peers[1], peers[2], partner):
        pl.semaphore_signal(barrier, inc=1, device_id=(peer,), device_id_type=MESH)

    def fetch(src, dst, i):
        cp = pltpu.make_async_copy(src, dst, in_sem.at[i])
        cp.start()
        return cp

    ids_cp = fetch(ids_hbm, ids_in, 0)
    mask_cp = fetch(mask_hbm, mask_in, 1)
    w1_cps = [fetch(ws1_hbm, ws1, 2), fetch(wn1_hbm, wn1, 3)]
    for b in range(N_DEV):
        cp = pltpu.make_async_copy(x_hbm.at[:, pl.ds(b * BLK, BLK)], x_v.at[b], x_sem)
        cp.start()
    late_cps = [fetch(ws2_hbm, ws2, 4), fetch(wn2_hbm, wn2, 5), fetch(ws3_hbm, ws3t, 6), fetch(wn3_hbm, wn3t, 7)]

    def remote(src, dst, ss, rs, dev):
        return pltpu.make_async_remote_copy(
            src_ref=src, dst_ref=dst, send_sem=ss, recv_sem=rs, device_id=(dev,), device_id_type=MESH
        )

    def drain(ref, sem):
        pltpu.make_async_copy(ref, ref, sem).wait()

    row_shape = (TILE // 8, 8, LANES)
    row_base = lax.broadcasted_iota(jnp.int32, row_shape, 0) * 8 + lax.broadcasted_iota(jnp.int32, row_shape, 1)
    for tile in range(HALF // TILE):
        row_ids[tile] = (row_base + tile * TILE).astype(jnp.int16)
    ids_pkt[...] = jnp.full(ids_pkt.shape, -1, jnp.int16)
    ids_cp.wait()
    mask_cp.wait()
    masked = jnp.where(mask_in[...] > 0, ids_in[...], -1)
    ids_pkt[0:FAN, :] = masked.astype(jnp.int16)
    pl.semaphore_wait(barrier, 3)
    pl.semaphore_signal(go_sem, inc=1, device_id=(peers[2],), device_id_type=MESH)
    id_copies = [remote(ids_pkt, ids_rcv.at[s], ids_ss, ids_rs.at[s], peers[s]) for s in range(3)]
    for s in (2, 1):
        id_copies[s].start()
    for g in range(2):
        ids_s32[OWN + g, 0:FAN, :] = masked[:, g * LANES : (g + 1) * LANES]
        spread_ids(ids_s32, idb, wb, inv, OWN + g)
    for cp in w1_cps:
        cp.wait()
    w1t[0:HID, :] = ws1[...].T
    w1t[HID:, :] = wn1[...].T

    def build_own(tile, g):
        def put(half):
            def store(r, v):
                v = v if half else v * jnp.array(16.0, BF)
                row = tile % 2 * (TILE // 8) + r
                a_own[half * 4 + tile // 2, row : row + 8, :, g * LANES : (g + 1) * LANES] = v

            return store

        build_tile(tile, row_ids, idb, wb, OWN + g, put(0), put(1))

    drain(x_v, x_sem)
    for i in range(4):
        part = jnp.dot(w1t[...], x_v[theirs[i]], preferred_element_type=F32)
        yown[theirs[i]] = part[HID:].astype(BF)
        ssend[i] = part[:HID].astype(BF)
        part2 = jnp.dot(w1t[...], x_v[mine[i]], preferred_element_type=F32)
        yown[mine[i]] = part2[HID:].astype(BF)
        sown[i] = part2[:HID]
        for b in (theirs[i], mine[i]):
            remote(yown.at[b], yrecv.at[b], y_ss, y_rs, partner).start()
        build_own(2 * i, 0)
        if i == 1:
            pl.semaphore_wait(go_sem, 1)
            id_copies[0].start()
    for i in range(4):
        remote(ssend.at[i], srecv.at[i], s_ss, s_rs, partner).start()
    for tile in range(1, 8, 2):
        build_own(tile, 0)
    for cp in late_cps:
        cp.wait()
    w2st[...] = ws2[...].T
    w2nt[...] = wn2[...].T

    def build_into(flat):
        def put(half):
            def store(r, v):
                ring[flat % RING, half, r : r + 8] = v

            return store

        build_tile(flat % 8, row_ids, idb, wb, flat // 8, put(0), put(1))

    def dot_from(flat):
        tile = flat % 8
        cols = slice(tile % 2 * TILE, (tile % 2 + 1) * TILE)
        low = ring[flat % RING, 0].reshape(TILE, LANES)
        high = ring[flat % RING, 1].reshape(TILE, LANES)
        return (
            jnp.dot(ysum[tile // 2, :, cols], low, preferred_element_type=F32),
            jnp.dot(ysum[4 + tile // 2, :, cols], high, preferred_element_type=F32),
        )

    def lanes(g):
        return slice(g * LANES, (g + 1) * LANES)

    def quarter(q):
        return slice(q * Q, (q + 1) * Q)

    def take_ids(s):
        id_copies[s].wait_recv()
        for u, pair in enumerate(UNITS):
            for half, (slot, q) in enumerate(pair):
                if slot == s:
                    ids_s32[u, :, quarter(half)] = ids_rcv[s, :, quarter(q)].astype(jnp.int32)

    rs_copies = {}

    def finish_unit(u, low, high):
        total = (low * 16.0 + high) * jnp.broadcast_to(inv[u, 0:1, :], (HID, LANES))
        for half, (s, q) in enumerate(UNITS[u]):
            part = total[:, quarter(half)] + sown[1 + s, :, quarter(q)] + srecv[1 + s, :, quarter(q)].astype(F32)
            rs_send[s, q] = part.astype(BF)
            rs_copies[s, q] = remote(rs_send.at[s, q], rs_recv.at[s, q], r_ss, r_rs.at[4 * s + q], peers[s])
            rs_copies[s, q].start()

    def own_piece(b, g):
        return jnp.dot(ysum[b], a_own[b, :, :, lanes(g)].reshape(BLK, LANES), preferred_element_type=F32)

    def own_base(g, own):
        base = own * jnp.broadcast_to(inv[OWN + g, 0:1, :], (HID, LANES))
        zbase[g] = base + sown[0, :, lanes(g)] + srecv[0, :, lanes(g)].astype(F32)

    def own_dot(h, b, p):
        rows = a_own[b, p * Q // 8 : (p + 1) * Q // 8].reshape(Q, BLK)
        return jnp.dot(h[b, p], rows, preferred_element_type=F32)

    class Gather:
        def __init__(self, h, ss, rs, direct):
            self.h, self.ss, self.rs, self.direct = h, ss, rs, direct
            self.copies, self.forwards, self.ready = {}, [], []

        def copy(self, block, p, slot, dev):
            return remote(self.h.at[block, p], self.h.at[block, p], self.ss, self.rs.at[7 * p + slot], dev)

        def send(self, slot, p):
            dev = partner if slot == 3 else peers[slot]
            self.copies[slot, p] = self.copy(me, p, slot, dev)
            self.copies[slot, p].start()

        def take(self, slot, p):
            self.copies[slot, p].wait_recv()
            block = partner if slot == 3 else peers[slot]
            if p not in self.direct and slot == (1 if p % 2 else 2):
                self.copies[0, p] = self.copy(block, p, 0, peers[3 - slot])
                self.copies[0, p].start()
            if slot < 3:
                fwd = self.copy(block, p, 4 + slot, partner)
                fwd.start()
                self.forwards.append((slot, p, fwd))
            self.ready.append((block, p))

        def take_forwards(self, n):
            for slot, p, fwd in self.forwards[:n]:
                fwd.wait_recv()
                self.ready.append((mates[slot], p))
            self.forwards = self.forwards[n:]

        def own(self, pieces):
            acc[...] = sum(own_dot(self.h, me, p) for p in range(pieces))

        def add(self):
            acc[...] += sum(own_dot(self.h, b, p) for b, p in self.ready)
            self.ready = []

    g1 = Gather(h1, g1_ss, g1_rs, direct=(3,))
    g2 = Gather(h2, g2_ss, g2_rs, direct=())

    def finish_quarter(q):
        z = zbase[q // 2, :, quarter(q % 2)]
        for t in (1, 2, 0):
            rs_copies[t, q].wait_recv()
            z = z + rs_recv[t, q].astype(F32)
        h1[me, q] = jnp.maximum(z, 0.0).astype(BF)
        for slot in (0, 2, 1, 3) if q in g1.direct else (2, 1, 3):
            g1.send(slot, q)

    take_ids(2)
    take_ids(1)
    spread_ids(ids_s32, idb, wb, inv, 0)
    lead = 3
    for flat in range(lead):
        build_into(flat)
    drain(yrecv, y_rs)
    for b in range(N_DEV):
        ysum[b] = yown[b] + yrecv[b]
    built = lead
    low = high = own = None
    for flat in range(48):
        u, tile = flat // 8, flat % 8
        while built < 48 and built - flat < 2 or (built < 48 and tile % 2 == 0 and built - flat < lead):
            if built == 16:
                take_ids(0)
            if built % 8 == 0:
                spread_ids(ids_s32, idb, wb, inv, built // 8)
            build_into(built)
            built += 1
        part = dot_from(flat)
        low = part[0] if low is None else low + part[0]
        high = part[1] if high is None else high + part[1]
        if u == 1:
            own = own_piece(tile, 0) if own is None else own + own_piece(tile, 0)
        if tile == 7:
            if u == 0:
                drain(srecv, s_rs)
            finish_unit(u, low, high)
            low = high = None
            if u == 1:
                own_base(0, own)
    for tile in range(8):
        build_own(tile, 1)
    finish_quarter(0)
    finish_quarter(1)
    own_base(1, sum(own_piece(b, 1) for b in range(N_DEV)))
    finish_quarter(2)
    finish_quarter(3)
    g1.own(4)
    for g in range(2):
        block = jnp.concatenate([h1[me, 2 * g], h1[me, 2 * g + 1]], axis=1)
        zbase[g] = jnp.dot(w2st[...], block, preferred_element_type=F32)
    for slot, p in ((2, 0), (1, 0), (1, 1), (2, 1), (2, 2), (1, 2)):
        g1.take(slot, p)
    for p in range(4):
        g1.take(3, p)
    g1.add()
    g1.take(0, 0)
    g1.take(0, 1)
    g1.take_forwards(6)
    g1.add()
    for slot, p in ((2, 3), (1, 3), (0, 3), (0, 2)):
        g1.take(slot, p)
    g1.add()
    g1.take_forwards(4)
    g1.add()
    g1.take_forwards(2)
    g1.add()

    inv_own = jnp.concatenate(
        [jnp.broadcast_to(inv[OWN + g, 0:1, :], (HID, LANES)) for g in range(2)], axis=1
    )
    for g in range(2):
        mean1 = (acc[:, lanes(g)] * inv_own[:, lanes(g)]).astype(BF)
        pre2 = zbase[g] + jnp.dot(w2nt[...], mean1, preferred_element_type=F32)
        for half in range(2):
            h2[me, 2 * g + half] = jnp.maximum(pre2[:, quarter(half)], 0.0).astype(BF)
        g2.send(2, 2 * g)
        g2.send(1, 2 * g + 1)
    for slot, p in ((2, 1), (1, 0), (2, 3), (1, 2)):
        g2.send(slot, p)
    for p in range(4):
        g2.send(3, p)
    g2.own(4)
    for g in range(2):
        block = jnp.concatenate([h2[me, 2 * g], h2[me, 2 * g + 1]], axis=1)
        out_ref[:, lanes(g)] = jnp.dot(ws3t[...], block, preferred_element_type=F32)
    drain(ids_rcv, ids_ss)
    drain(yown, y_ss)
    drain(ssend, s_ss)
    drain(rs_send, r_ss)
    drain(h1.at[0:7], g1_ss)
    for p in range(4):
        g2.take(3, p)
    g2.add()
    for slot, p in ((2, 0), (1, 1), (2, 2), (1, 3)):
        g2.take(slot, p)
    g2.add()
    for slot, p in ((2, 1), (1, 0), (2, 3), (1, 2)):
        g2.take(slot, p)
    g2.take_forwards(4)
    g2.add()
    g2.take(0, 0)
    g2.take(0, 1)
    g2.take_forwards(4)
    g2.add()
    g2.take(0, 2)
    g2.take(0, 3)
    g2.take_forwards(2)
    g2.add()
    g2.take_forwards(2)
    g2.add()
    for g in range(2):
        mean2 = (acc[:, lanes(g)] * inv_own[:, lanes(g)]).astype(BF)
        out_ref[:, lanes(g)] += jnp.dot(wn3t[...], mean2, preferred_element_type=F32)
    drain(h2.at[0:7], g2_ss)


def solution(mesh):
    def device_step(feat, ws1, wn1, ids, mask, ws2, wn2, ws3, wn3):
        operands = (feat.T, ws1, wn1, ids.T, mask.T, ws2, wn2, ws3.T, wn3.T)
        vm = pl.BlockSpec(memory_space=pltpu.VMEM)
        dma = pltpu.SemaphoreType.DMA
        out_t = pl.pallas_call(
            kernel,
            out_shape=jax.ShapeDtypeStruct((7, BLK), F32),
            in_specs=[pl.BlockSpec(memory_space=pltpu.HBM)] * 9,
            out_specs=vm,
            scratch_shapes=[
                pltpu.VMEM((N_DEV, 192, BLK), BF),
                pltpu.VMEM((192, HID), BF),
                pltpu.VMEM((192, HID), BF),
                pltpu.VMEM((FAN, BLK), jnp.int32),
                pltpu.VMEM((FAN, BLK), jnp.int32),
                pltpu.VMEM((HID, HID), BF),
                pltpu.VMEM((HID, HID), BF),
                pltpu.VMEM((7, HID), BF),
                pltpu.VMEM((7, HID), BF),
                pltpu.VMEM((2 * HID, 192), BF),
                pltpu.VMEM((HID, HID), BF),
                pltpu.VMEM((HID, HID), BF),
                pltpu.VMEM((N_DEV, HID, BLK), BF),
                pltpu.VMEM((N_DEV, HID, BLK), BF),
                pltpu.VMEM((N_DEV, HID, BLK), BF),
                pltpu.VMEM((4, HID, BLK), F32),
                pltpu.VMEM((4, HID, BLK), BF),
                pltpu.VMEM((4, HID, BLK), BF),
                pltpu.VMEM((16, BLK), jnp.int16),
                pltpu.VMEM((3, 16, BLK), jnp.int16),
                pltpu.VMEM((8, 16, LANES), jnp.int32),
                pltpu.VMEM((HALF // TILE, TILE // 8, 8, LANES), jnp.int16),
                pltpu.VMEM((8, FAN, 8, LANES), jnp.int16),
                pltpu.VMEM((8, FAN, 8, LANES), BF),
                pltpu.VMEM((8, 8, LANES), F32),
                pltpu.VMEM((RING, 2, TILE // 8, 8, LANES), BF),
                pltpu.VMEM((N_DEV, BLK // 8, 8, BLK), BF),
                pltpu.VMEM((HID, BLK), F32),
                pltpu.VMEM((2, HID, LANES), F32),
                pltpu.VMEM((3, 4, HID, Q), BF),
                pltpu.VMEM((3, 4, HID, Q), BF),
                pltpu.VMEM((N_DEV, 4, HID, Q), BF),
                pltpu.VMEM((N_DEV, 4, HID, Q), BF),
                dma((8,)),
                dma,
                dma, dma((3,)),
                dma, dma,
                dma, dma,
                dma, dma((12,)),
                dma, dma((28,)),
                dma, dma((28,)),
                pltpu.SemaphoreType.REGULAR,
            ],
            compiler_params=pltpu.CompilerParams(
                collective_id=0, has_side_effects=True, vmem_limit_bytes=32 * 1024 * 1024
            ),
            name="graphsage",
        )(*(pltpu.with_memory_space_constraint(a, pltpu.HBM) for a in operands))
        return out_t.T

    col_split = P(None, "g")
    row_split = P("g", None)
    replicated = P()
    return jax.shard_map(
        device_step,
        mesh=mesh,
        in_specs=(col_split, row_split, row_split, row_split, row_split, replicated, replicated, replicated, replicated),
        out_specs=row_split,
        check_vma=False,
    )
```

```python
import jax
import jax.numpy as jnp
from jax import lax
from jax.experimental import pallas as pl
from jax.experimental.pallas import tpu as pltpu
from jax.sharding import PartitionSpec as P

MESH = pl.DeviceIdType.MESH
N_DEV = 8
NODES = 4096
BLK = NODES // N_DEV
HALF = NODES // 2
FAN = 10
HID = 128
TILE = 256
LANES = 256
BF = jnp.bfloat16
F32 = jnp.float32


UNITS = (((2, 0), (1, 0)), ((0, 0), (0, 1)), ((0, 2), (0, 3)), ((2, 1), (1, 1)), ((2, 2), (1, 2)), ((2, 3), (1, 3)))
OWN = 6
RING = 6
Q = 128


def spread_ids(ids_s32, idb, wb, inv, u):
    words, weights = [], []
    degree = jnp.zeros((8, LANES), F32)
    for k in range(FAN):
        raw = jnp.broadcast_to(ids_s32[u, k : k + 1, :], (8, LANES))
        valid = raw >= 0
        degree += jnp.where(valid, 1.0, 0.0)
        upper = raw >= HALF
        word = jnp.where(upper, raw - HALF, raw)
        weight = jnp.where(valid, jnp.where(upper, 1.0, 0.0625), 0.0)
        for m in range(k):
            same = word == words[m]
            weights[m] = weights[m] + jnp.where(same, weight, 0.0)
            word = jnp.where(same, -1, word)
        words.append(word)
        weights.append(weight)
    inv[u] = 1.0 / degree
    for k in range(FAN):
        idb[u, k] = words[k].astype(jnp.int16)
        wb[u, k] = weights[k].astype(BF)


def build_tile(tile, row_ids, idb, wb, u, store_low, store_high):
    ids = [idb[u, k] for k in range(FAN)]
    wts = [wb[u, k] for k in range(FAN)]
    for r in range(0, TILE // 8, 8):
        rows = row_ids[tile, r : r + 8]
        acc = jnp.zeros((8, 8, LANES), BF)
        for k in range(FAN):
            acc = jnp.where(ids[k][None] == rows, wts[k][None], acc)
        high = jnp.floor(acc)
        store_high(r, high)
        store_low(r, acc - high)


def kernel(
    x_hbm, ws1_hbm, wn1_hbm, ids_hbm, mask_hbm, ws2_hbm, wn2_hbm, ws3_hbm, wn3_hbm, out_ref,
    x_v, ws1, wn1, ids_in, mask_in, ws2, wn2, ws3t, wn3t,
    w1t, w2st, w2nt, yown, yrecv, ysum, sown, ssend, srecv,
    ids_pkt, ids_rcv, ids_s32, row_ids, idb, wb, inv,
    ring, a_own, acc, zbase, rs_send, rs_recv, h1, h2,
    in_sem, x_sem, ids_ss, ids_rs, y_ss, y_rs, s_ss, s_rs, r_ss, r_rs, g1_ss, g1_rs, g2_ss, g2_rs, go_sem,
):
    me = lax.axis_index("g")
    core = lax.rem(me, 2)
    cx = lax.rem(me // 2, 2)
    cy = me // 4
    partner = me + 1 - 2 * core
    steps = (6 - 4 * cx - 8 * cy, 4 - 8 * cy, 2 - 4 * cx)
    peers = (me + steps[0], partner + steps[1], partner + steps[2])
    mates = (partner + steps[0], me + steps[1], me + steps[2])
    mine, theirs = (me, *peers), (partner, *mates)

    barrier = pltpu.get_barrier_semaphore()
    for peer in (peers[1], peers[2], partner):
        pl.semaphore_signal(barrier, inc=1, device_id=(peer,), device_id_type=MESH)

    def fetch(src, dst, i):
        cp = pltpu.make_async_copy(src, dst, in_sem.at[i])
        cp.start()
        return cp

    ids_cp = fetch(ids_hbm, ids_in, 0)
    mask_cp = fetch(mask_hbm, mask_in, 1)
    w1_cps = [fetch(ws1_hbm, ws1, 2), fetch(wn1_hbm, wn1, 3)]
    for b in range(N_DEV):
        cp = pltpu.make_async_copy(x_hbm.at[:, pl.ds(b * BLK, BLK)], x_v.at[b], x_sem)
        cp.start()
    late_cps = [fetch(ws2_hbm, ws2, 4), fetch(wn2_hbm, wn2, 5), fetch(ws3_hbm, ws3t, 6), fetch(wn3_hbm, wn3t, 7)]

    def remote(src, dst, ss, rs, dev):
        return pltpu.make_async_remote_copy(
            src_ref=src, dst_ref=dst, send_sem=ss, recv_sem=rs, device_id=(dev,), device_id_type=MESH
        )

    def drain(ref, sem):
        pltpu.make_async_copy(ref, ref, sem).wait()

    row_shape = (TILE // 8, 8, LANES)
    row_base = lax.broadcasted_iota(jnp.int32, row_shape, 0) * 8 + lax.broadcasted_iota(jnp.int32, row_shape, 1)
    for tile in range(HALF // TILE):
        row_ids[tile] = (row_base + tile * TILE).astype(jnp.int16)
    ids_pkt[...] = jnp.full(ids_pkt.shape, -1, jnp.int16)
    ids_cp.wait()
    mask_cp.wait()
    masked = jnp.where(mask_in[...] > 0, ids_in[...], -1)
    ids_pkt[0:FAN, :] = masked.astype(jnp.int16)
    pl.semaphore_wait(barrier, 3)
    pl.semaphore_signal(go_sem, inc=1, device_id=(peers[2],), device_id_type=MESH)
    id_copies = [remote(ids_pkt, ids_rcv.at[s], ids_ss, ids_rs.at[s], peers[s]) for s in range(3)]
    for s in (2, 1):
        id_copies[s].start()
    for g in range(2):
        ids_s32[OWN + g, 0:FAN, :] = masked[:, g * LANES : (g + 1) * LANES]
        spread_ids(ids_s32, idb, wb, inv, OWN + g)
    for cp in w1_cps:
        cp.wait()
    w1t[0:HID, :] = ws1[...].T
    w1t[HID:, :] = wn1[...].T

    def build_own(tile, g):
        def put(half):
            def store(r, v):
                v = v if half else v * jnp.array(16.0, BF)
                row = tile % 2 * (TILE // 8) + r
                a_own[half * 4 + tile // 2, row : row + 8, :, g * LANES : (g + 1) * LANES] = v

            return store

        build_tile(tile, row_ids, idb, wb, OWN + g, put(0), put(1))

    drain(x_v, x_sem)
    for i in range(4):
        part = jnp.dot(w1t[...], x_v[theirs[i]], preferred_element_type=F32)
        yown[theirs[i]] = part[HID:].astype(BF)
        ssend[i] = part[:HID].astype(BF)
        part2 = jnp.dot(w1t[...], x_v[mine[i]], preferred_element_type=F32)
        yown[mine[i]] = part2[HID:].astype(BF)
        sown[i] = part2[:HID]
        for b in (theirs[i], mine[i]):
            remote(yown.at[b], yrecv.at[b], y_ss, y_rs, partner).start()
        build_own(2 * i, 0)
        if i == 1:
            pl.semaphore_wait(go_sem, 1)
            id_copies[0].start()
    for i in range(4):
        remote(ssend.at[i], srecv.at[i], s_ss, s_rs, partner).start()
    for tile in range(1, 8, 2):
        build_own(tile, 0)
    for cp in late_cps:
        cp.wait()
    w2st[...] = ws2[...].T
    w2nt[...] = wn2[...].T

    def build_into(flat):
        def put(half):
            def store(r, v):
                ring[flat % RING, half, r : r + 8] = v

            return store

        build_tile(flat % 8, row_ids, idb, wb, flat // 8, put(0), put(1))

    def dot_from(flat):
        tile = flat % 8
        cols = slice(tile % 2 * TILE, (tile % 2 + 1) * TILE)
        low = ring[flat % RING, 0].reshape(TILE, LANES)
        high = ring[flat % RING, 1].reshape(TILE, LANES)
        return (
            jnp.dot(ysum[tile // 2, :, cols], low, preferred_element_type=F32),
            jnp.dot(ysum[4 + tile // 2, :, cols], high, preferred_element_type=F32),
        )

    def lanes(g):
        return slice(g * LANES, (g + 1) * LANES)

    def quarter(q):
        return slice(q * Q, (q + 1) * Q)

    def take_ids(s):
        id_copies[s].wait_recv()
        for u, pair in enumerate(UNITS):
            for half, (slot, q) in enumerate(pair):
                if slot == s:
                    ids_s32[u, :, quarter(half)] = ids_rcv[s, :, quarter(q)].astype(jnp.int32)

    rs_copies = {}

    def finish_unit(u, low, high):
        total = (low * 16.0 + high) * jnp.broadcast_to(inv[u, 0:1, :], (HID, LANES))
        for half, (s, q) in enumerate(UNITS[u]):
            part = total[:, quarter(half)] + sown[1 + s, :, quarter(q)] + srecv[1 + s, :, quarter(q)].astype(F32)
            rs_send[s, q] = part.astype(BF)
            rs_copies[s, q] = remote(rs_send.at[s, q], rs_recv.at[s, q], r_ss, r_rs.at[4 * s + q], peers[s])
            rs_copies[s, q].start()

    def own_piece(b, g):
        return jnp.dot(ysum[b], a_own[b, :, :, lanes(g)].reshape(BLK, LANES), preferred_element_type=F32)

    def own_base(g, own):
        base = own * jnp.broadcast_to(inv[OWN + g, 0:1, :], (HID, LANES))
        zbase[g] = base + sown[0, :, lanes(g)] + srecv[0, :, lanes(g)].astype(F32)

    def own_dot(h, b, p):
        rows = a_own[b, p * Q // 8 : (p + 1) * Q // 8].reshape(Q, BLK)
        return jnp.dot(h[b, p], rows, preferred_element_type=F32)

    class Gather:
        def __init__(self, h, ss, rs, direct):
            self.h, self.ss, self.rs, self.direct = h, ss, rs, direct
            self.copies, self.forwards, self.ready = {}, [], []

        def copy(self, block, p, slot, dev):
            return remote(self.h.at[block, p], self.h.at[block, p], self.ss, self.rs.at[7 * p + slot], dev)

        def send(self, slot, p):
            dev = partner if slot == 3 else peers[slot]
            self.copies[slot, p] = self.copy(me, p, slot, dev)
            self.copies[slot, p].start()

        def take(self, slot, p):
            self.copies[slot, p].wait_recv()
            block = partner if slot == 3 else peers[slot]
            if p not in self.direct and slot == (1 if p % 2 else 2):
                self.copies[0, p] = self.copy(block, p, 0, peers[3 - slot])
                self.copies[0, p].start()
            if slot < 3:
                fwd = self.copy(block, p, 4 + slot, partner)
                fwd.start()
                self.forwards.append((slot, p, fwd))
            self.ready.append((block, p))

        def take_forwards(self, n):
            for slot, p, fwd in self.forwards[:n]:
                fwd.wait_recv()
                self.ready.append((mates[slot], p))
            self.forwards = self.forwards[n:]

        def own(self, pieces):
            acc[...] = sum(own_dot(self.h, me, p) for p in range(pieces))

        def add(self):
            acc[...] += sum(own_dot(self.h, b, p) for b, p in self.ready)
            self.ready = []

    g1 = Gather(h1, g1_ss, g1_rs, direct=(3,))
    g2 = Gather(h2, g2_ss, g2_rs, direct=())

    def finish_quarter(q):
        z = zbase[q // 2, :, quarter(q % 2)]
        for t in (1, 2, 0):
            rs_copies[t, q].wait_recv()
            z = z + rs_recv[t, q].astype(F32)
        h1[me, q] = jnp.maximum(z, 0.0).astype(BF)
        for slot in (0, 2, 1, 3) if q in g1.direct else (2, 1, 3):
            g1.send(slot, q)

    take_ids(2)
    take_ids(1)
    spread_ids(ids_s32, idb, wb, inv, 0)
    lead = 3
    for flat in range(lead):
        build_into(flat)
    drain(yrecv, y_rs)
    for b in range(N_DEV):
        ysum[b] = yown[b] + yrecv[b]
    built = lead
    low = high = own = None
    for flat in range(48):
        u, tile = flat // 8, flat % 8
        while built < 48 and built - flat < 2 or (built < 48 and tile % 2 == 0 and built - flat < lead):
            if built == 8:
                take_ids(0)
            if built % 8 == 0:
                spread_ids(ids_s32, idb, wb, inv, built // 8)
            build_into(built)
            built += 1
        part = dot_from(flat)
        low = part[0] if low is None else low + part[0]
        high = part[1] if high is None else high + part[1]
        if u == 1:
            own = own_piece(tile, 0) if own is None else own + own_piece(tile, 0)
        if tile == 7:
            if u == 0:
                drain(srecv, s_rs)
            finish_unit(u, low, high)
            low = high = None
            if u == 1:
                own_base(0, own)
    for tile in range(8):
        build_own(tile, 1)
    finish_quarter(0)
    finish_quarter(1)
    own_base(1, sum(own_piece(b, 1) for b in range(N_DEV)))
    finish_quarter(2)
    finish_quarter(3)
    g1.own(4)
    for g in range(2):
        block = jnp.concatenate([h1[me, 2 * g], h1[me, 2 * g + 1]], axis=1)
        zbase[g] = jnp.dot(w2st[...], block, preferred_element_type=F32)
    for slot, p in ((2, 0), (1, 0), (1, 1), (2, 1), (2, 2), (1, 2)):
        g1.take(slot, p)
    for p in range(4):
        g1.take(3, p)
    g1.add()
    g1.take(0, 0)
    g1.take(0, 1)
    g1.take_forwards(6)
    g1.add()
    for slot, p in ((2, 3), (1, 3), (0, 3), (0, 2)):
        g1.take(slot, p)
    g1.add()
    g1.take_forwards(4)
    g1.add()
    g1.take_forwards(2)
    g1.add()

    inv_own = jnp.concatenate(
        [jnp.broadcast_to(inv[OWN + g, 0:1, :], (HID, LANES)) for g in range(2)], axis=1
    )
    for g in range(2):
        mean1 = (acc[:, lanes(g)] * inv_own[:, lanes(g)]).astype(BF)
        pre2 = zbase[g] + jnp.dot(w2nt[...], mean1, preferred_element_type=F32)
        for half in range(2):
            h2[me, 2 * g + half] = jnp.maximum(pre2[:, quarter(half)], 0.0).astype(BF)
        g2.send(2, 2 * g)
        g2.send(1, 2 * g + 1)
    for slot, p in ((2, 1), (1, 0), (2, 3), (1, 2)):
        g2.send(slot, p)
    for p in range(4):
        g2.send(3, p)
    g2.own(4)
    for g in range(2):
        block = jnp.concatenate([h2[me, 2 * g], h2[me, 2 * g + 1]], axis=1)
        out_ref[:, lanes(g)] = jnp.dot(ws3t[...], block, preferred_element_type=F32)
    drain(ids_rcv, ids_ss)
    drain(yown, y_ss)
    drain(ssend, s_ss)
    drain(rs_send, r_ss)
    drain(h1.at[0:7], g1_ss)
    for p in range(4):
        g2.take(3, p)
    g2.add()
    for slot, p in ((2, 0), (1, 1), (2, 2), (1, 3)):
        g2.take(slot, p)
    g2.add()
    for slot, p in ((2, 1), (1, 0), (2, 3), (1, 2)):
        g2.take(slot, p)
    g2.take_forwards(4)
    g2.add()
    g2.take(0, 0)
    g2.take(0, 1)
    g2.take_forwards(4)
    g2.add()
    g2.take(0, 2)
    g2.take(0, 3)
    g2.take_forwards(2)
    g2.add()
    g2.take_forwards(2)
    g2.add()
    for g in range(2):
        mean2 = (acc[:, lanes(g)] * inv_own[:, lanes(g)]).astype(BF)
        out_ref[:, lanes(g)] += jnp.dot(wn3t[...], mean2, preferred_element_type=F32)
    drain(h2.at[0:7], g2_ss)


def solution(mesh):
    def device_step(feat, ws1, wn1, ids, mask, ws2, wn2, ws3, wn3):
        operands = (feat.T, ws1, wn1, ids.T, mask.T, ws2, wn2, ws3.T, wn3.T)
        vm = pl.BlockSpec(memory_space=pltpu.VMEM)
        dma = pltpu.SemaphoreType.DMA
        out_t = pl.pallas_call(
            kernel,
            out_shape=jax.ShapeDtypeStruct((7, BLK), F32),
            in_specs=[pl.BlockSpec(memory_space=pltpu.HBM)] * 9,
            out_specs=vm,
            scratch_shapes=[
                pltpu.VMEM((N_DEV, 192, BLK), BF),
                pltpu.VMEM((192, HID), BF),
                pltpu.VMEM((192, HID), BF),
                pltpu.VMEM((FAN, BLK), jnp.int32),
                pltpu.VMEM((FAN, BLK), jnp.int32),
                pltpu.VMEM((HID, HID), BF),
                pltpu.VMEM((HID, HID), BF),
                pltpu.VMEM((7, HID), BF),
                pltpu.VMEM((7, HID), BF),
                pltpu.VMEM((2 * HID, 192), BF),
                pltpu.VMEM((HID, HID), BF),
                pltpu.VMEM((HID, HID), BF),
                pltpu.VMEM((N_DEV, HID, BLK), BF),
                pltpu.VMEM((N_DEV, HID, BLK), BF),
                pltpu.VMEM((N_DEV, HID, BLK), BF),
                pltpu.VMEM((4, HID, BLK), F32),
                pltpu.VMEM((4, HID, BLK), BF),
                pltpu.VMEM((4, HID, BLK), BF),
                pltpu.VMEM((16, BLK), jnp.int16),
                pltpu.VMEM((3, 16, BLK), jnp.int16),
                pltpu.VMEM((8, 16, LANES), jnp.int32),
                pltpu.VMEM((HALF // TILE, TILE // 8, 8, LANES), jnp.int16),
                pltpu.VMEM((8, FAN, 8, LANES), jnp.int16),
                pltpu.VMEM((8, FAN, 8, LANES), BF),
                pltpu.VMEM((8, 8, LANES), F32),
                pltpu.VMEM((RING, 2, TILE // 8, 8, LANES), BF),
                pltpu.VMEM((N_DEV, BLK // 8, 8, BLK), BF),
                pltpu.VMEM((HID, BLK), F32),
                pltpu.VMEM((2, HID, LANES), F32),
                pltpu.VMEM((3, 4, HID, Q), BF),
                pltpu.VMEM((3, 4, HID, Q), BF),
                pltpu.VMEM((N_DEV, 4, HID, Q), BF),
                pltpu.VMEM((N_DEV, 4, HID, Q), BF),
                dma((8,)),
                dma,
                dma, dma((3,)),
                dma, dma,
                dma, dma,
                dma, dma((12,)),
                dma, dma((28,)),
                dma, dma((28,)),
                pltpu.SemaphoreType.REGULAR,
            ],
            compiler_params=pltpu.CompilerParams(
                collective_id=0, has_side_effects=True, vmem_limit_bytes=32 * 1024 * 1024
            ),
            name="graphsage",
        )(*(pltpu.with_memory_space_constraint(a, pltpu.HBM) for a in operands))
        return out_t.T

    col_split = P(None, "g")
    row_split = P("g", None)
    replicated = P()
    return jax.shard_map(
        device_step,
        mesh=mesh,
        in_specs=(col_split, row_split, row_split, row_split, row_split, replicated, replicated, replicated, replicated),
        out_specs=row_split,
        check_vma=False,
    )
```

```python
import jax
import jax.numpy as jnp
from jax import lax
from jax.experimental import pallas as pl
from jax.experimental.pallas import tpu as pltpu
from jax.sharding import PartitionSpec as P

MESH = pl.DeviceIdType.MESH
N_DEV = 8
NODES = 4096
BLK = NODES // N_DEV
HALF = NODES // 2
FAN = 10
HID = 128
TILE = 256
LANES = 256
BF = jnp.bfloat16
F32 = jnp.float32


UNITS = (((2, 0), (1, 0)), ((0, 0), (0, 1)), ((2, 1), (1, 1)), ((0, 2), (0, 3)), ((2, 2), (1, 2)), ((2, 3), (1, 3)))
OWN = 6
RING = 6
Q = 128


def spread_ids(ids_s32, idb, wb, inv, u):
    words, weights = [], []
    degree = jnp.zeros((8, LANES), F32)
    for k in range(FAN):
        raw = jnp.broadcast_to(ids_s32[u, k : k + 1, :], (8, LANES))
        valid = raw >= 0
        degree += jnp.where(valid, 1.0, 0.0)
        upper = raw >= HALF
        word = jnp.where(upper, raw - HALF, raw)
        weight = jnp.where(valid, jnp.where(upper, 1.0, 0.0625), 0.0)
        for m in range(k):
            same = word == words[m]
            weights[m] = weights[m] + jnp.where(same, weight, 0.0)
            word = jnp.where(same, -1, word)
        words.append(word)
        weights.append(weight)
    inv[u] = 1.0 / degree
    for k in range(FAN):
        idb[u, k] = words[k].astype(jnp.int16)
        wb[u, k] = weights[k].astype(BF)


def build_tile(tile, row_ids, idb, wb, u, store_low, store_high):
    ids = [idb[u, k] for k in range(FAN)]
    wts = [wb[u, k] for k in range(FAN)]
    for r in range(0, TILE // 8, 8):
        rows = row_ids[tile, r : r + 8]
        acc = jnp.zeros((8, 8, LANES), BF)
        for k in range(FAN):
            acc = jnp.where(ids[k][None] == rows, wts[k][None], acc)
        high = jnp.floor(acc)
        store_high(r, high)
        store_low(r, acc - high)


def kernel(
    x_hbm, ws1_hbm, wn1_hbm, ids_hbm, mask_hbm, ws2_hbm, wn2_hbm, ws3_hbm, wn3_hbm, out_ref,
    x_v, ws1, wn1, ids_in, mask_in, ws2, wn2, ws3t, wn3t,
    w1t, w2st, w2nt, yown, yrecv, ysum, sown, ssend, srecv,
    ids_pkt, ids_rcv, ids_s32, row_ids, idb, wb, inv,
    ring, a_own, acc, zbase, rs_send, rs_recv, h1, h2,
    in_sem, x_sem, ids_ss, ids_rs, y_ss, y_rs, s_ss, s_rs, r_ss, r_rs, g1_ss, g1_rs, g2_ss, g2_rs,
):
    me = lax.axis_index("g")
    core = lax.rem(me, 2)
    cx = lax.rem(me // 2, 2)
    cy = me // 4
    partner = me + 1 - 2 * core
    steps = (6 - 4 * cx - 8 * cy, 4 - 8 * cy, 2 - 4 * cx)
    peers = tuple(partner + step for step in steps)
    mates = tuple(me + step for step in steps)
    mine, theirs = (me, *peers), (partner, *mates)

    barrier = pltpu.get_barrier_semaphore()
    for peer in (*peers, partner):
        pl.semaphore_signal(barrier, inc=1, device_id=(peer,), device_id_type=MESH)

    def fetch(src, dst, i):
        cp = pltpu.make_async_copy(src, dst, in_sem.at[i])
        cp.start()
        return cp

    ids_cp = fetch(ids_hbm, ids_in, 0)
    mask_cp = fetch(mask_hbm, mask_in, 1)
    w1_cps = [fetch(ws1_hbm, ws1, 2), fetch(wn1_hbm, wn1, 3)]
    for b in range(N_DEV):
        cp = pltpu.make_async_copy(x_hbm.at[:, pl.ds(b * BLK, BLK)], x_v.at[b], x_sem)
        cp.start()
    late_cps = [fetch(ws2_hbm, ws2, 4), fetch(wn2_hbm, wn2, 5), fetch(ws3_hbm, ws3t, 6), fetch(wn3_hbm, wn3t, 7)]

    def remote(src, dst, ss, rs, dev):
        return pltpu.make_async_remote_copy(
            src_ref=src, dst_ref=dst, send_sem=ss, recv_sem=rs, device_id=(dev,), device_id_type=MESH
        )

    def drain(ref, sem):
        pltpu.make_async_copy(ref, ref, sem).wait()

    row_shape = (TILE // 8, 8, LANES)
    row_base = lax.broadcasted_iota(jnp.int32, row_shape, 0) * 8 + lax.broadcasted_iota(jnp.int32, row_shape, 1)
    for tile in range(HALF // TILE):
        row_ids[tile] = (row_base + tile * TILE).astype(jnp.int16)
    ids_pkt[...] = jnp.full(ids_pkt.shape, -1, jnp.int16)
    ids_cp.wait()
    mask_cp.wait()
    masked = jnp.where(mask_in[...] > 0, ids_in[...], -1)
    ids_pkt[0:FAN, :] = masked.astype(jnp.int16)
    pl.semaphore_wait(barrier, 4)
    id_copies = [remote(ids_pkt, ids_rcv.at[s], ids_ss, ids_rs.at[s], peers[s]) for s in range(3)]
    for s in (2, 1, 0):
        id_copies[s].start()
    for g in range(2):
        ids_s32[OWN + g, 0:FAN, :] = masked[:, g * LANES : (g + 1) * LANES]
        spread_ids(ids_s32, idb, wb, inv, OWN + g)
    for cp in w1_cps:
        cp.wait()
    w1t[0:HID, :] = ws1[...].T
    w1t[HID:, :] = wn1[...].T

    def build_own(tile, g):
        def put(half):
            def store(r, v):
                v = v if half else v * jnp.array(16.0, BF)
                row = tile % 2 * (TILE // 8) + r
                a_own[half * 4 + tile // 2, row : row + 8, :, g * LANES : (g + 1) * LANES] = v

            return store

        build_tile(tile, row_ids, idb, wb, OWN + g, put(0), put(1))

    drain(x_v, x_sem)
    for i in range(4):
        part = jnp.dot(w1t[...], x_v[theirs[i]], preferred_element_type=F32)
        yown[theirs[i]] = part[HID:].astype(BF)
        ssend[i] = part[:HID].astype(BF)
        part2 = jnp.dot(w1t[...], x_v[mine[i]], preferred_element_type=F32)
        yown[mine[i]] = part2[HID:].astype(BF)
        sown[i] = part2[:HID]
        for b in (theirs[i], mine[i]):
            remote(yown.at[b], yrecv.at[b], y_ss, y_rs, partner).start()
        build_own(2 * i, 0)
    for i in range(4):
        remote(ssend.at[i], srecv.at[i], s_ss, s_rs, partner).start()
    for tile in range(1, 8, 2):
        build_own(tile, 0)
    for tile in range(8):
        build_own(tile, 1)
    for cp in late_cps:
        cp.wait()
    w2st[...] = ws2[...].T
    w2nt[...] = wn2[...].T

    def build_into(flat):
        def put(half):
            def store(r, v):
                ring[flat % RING, half, r : r + 8] = v

            return store

        build_tile(flat % 8, row_ids, idb, wb, flat // 8, put(0), put(1))

    def dot_from(flat):
        tile = flat % 8
        cols = slice(tile % 2 * TILE, (tile % 2 + 1) * TILE)
        low = ring[flat % RING, 0].reshape(TILE, LANES)
        high = ring[flat % RING, 1].reshape(TILE, LANES)
        return (
            jnp.dot(ysum[tile // 2, :, cols], low, preferred_element_type=F32),
            jnp.dot(ysum[4 + tile // 2, :, cols], high, preferred_element_type=F32),
        )

    def lanes(g):
        return slice(g * LANES, (g + 1) * LANES)

    def quarter(q):
        return slice(q * Q, (q + 1) * Q)

    def take_ids(s):
        id_copies[s].wait_recv()
        for u, pair in enumerate(UNITS):
            for half, (slot, q) in enumerate(pair):
                if slot == s:
                    ids_s32[u, :, quarter(half)] = ids_rcv[s, :, quarter(q)].astype(jnp.int32)

    rs_copies = {}

    def finish_unit(u, low, high):
        total = (low * 16.0 + high) * jnp.broadcast_to(inv[u, 0:1, :], (HID, LANES))
        for half, (s, q) in enumerate(UNITS[u]):
            part = total[:, quarter(half)] + sown[1 + s, :, quarter(q)] + srecv[1 + s, :, quarter(q)].astype(F32)
            rs_send[s, q] = part.astype(BF)
            rs_copies[s, q] = remote(rs_send.at[s, q], rs_recv.at[s, q], r_ss, r_rs.at[4 * s + q], peers[s])
            rs_copies[s, q].start()

    def own_piece(b, g):
        return jnp.dot(ysum[b], a_own[b, :, :, lanes(g)].reshape(BLK, LANES), preferred_element_type=F32)

    def own_base(g, own):
        base = own * jnp.broadcast_to(inv[OWN + g, 0:1, :], (HID, LANES))
        zbase[g] = base + sown[0, :, lanes(g)] + srecv[0, :, lanes(g)].astype(F32)

    def own_dot(h, b, p):
        rows = a_own[b, p * Q // 8 : (p + 1) * Q // 8].reshape(Q, BLK)
        return jnp.dot(h[b, p], rows, preferred_element_type=F32)

    class Gather:
        def __init__(self, h, ss, rs, direct):
            self.h, self.ss, self.rs, self.direct = h, ss, rs, direct
            self.copies, self.forwards, self.ready = {}, [], []

        def copy(self, block, p, slot, dev):
            return remote(self.h.at[block, p], self.h.at[block, p], self.ss, self.rs.at[7 * p + slot], dev)

        def send(self, slot, p):
            dev = partner if slot == 3 else peers[slot]
            self.copies[slot, p] = self.copy(me, p, slot, dev)
            self.copies[slot, p].start()

        def take(self, slot, p):
            self.copies[slot, p].wait_recv()
            block = partner if slot == 3 else mates[0] if slot == 0 and p not in self.direct else peers[slot]
            if p not in self.direct and slot == (1 if p % 2 else 2):
                self.copies[0, p] = self.copy(block, p, 0, peers[3 - slot])
                self.copies[0, p].start()
            if slot < 3:
                fwd = self.copy(block, p, 4 + slot, partner)
                fwd.start()
                self.forwards.append((slot, p, fwd))
            self.ready.append((block, p))

        def take_forwards(self, n):
            for slot, p, fwd in self.forwards[:n]:
                fwd.wait_recv()
                relayed = slot == 0 and p not in self.direct
                self.ready.append((peers[0] if relayed else mates[slot], p))
            self.forwards = self.forwards[n:]

        def own(self, pieces):
            acc[...] = sum(own_dot(self.h, me, p) for p in range(pieces))

        def add(self):
            acc[...] += sum(own_dot(self.h, b, p) for b, p in self.ready)
            self.ready = []

    g1 = Gather(h1, g1_ss, g1_rs, direct=(3,))
    g2 = Gather(h2, g2_ss, g2_rs, direct=())

    def finish_quarter(q):
        z = zbase[q // 2, :, quarter(q % 2)]
        for t in (1, 2, 0):
            rs_copies[t, q].wait_recv()
            z = z + rs_recv[t, q].astype(F32)
        h1[me, q] = jnp.maximum(z, 0.0).astype(BF)
        for slot in (0, 2, 1, 3) if q in g1.direct else (2, 1, 3):
            g1.send(slot, q)

    take_ids(2)
    take_ids(1)
    spread_ids(ids_s32, idb, wb, inv, 0)
    lead = 3
    for flat in range(lead):
        build_into(flat)
    drain(yrecv, y_rs)
    for b in range(N_DEV):
        ysum[b] = yown[b] + yrecv[b]
    built = lead
    low = high = own = None
    for flat in range(48):
        u, tile = flat // 8, flat % 8
        while built < 48 and built - flat < 2 or (built < 48 and tile % 2 == 0 and built - flat < lead):
            if built == 8:
                take_ids(0)
            if built % 8 == 0:
                spread_ids(ids_s32, idb, wb, inv, built // 8)
            build_into(built)
            built += 1
        part = dot_from(flat)
        low = part[0] if low is None else low + part[0]
        high = part[1] if high is None else high + part[1]
        if u in (1, 3):
            own = own_piece(tile, u // 2) if own is None else own + own_piece(tile, u // 2)
        if tile == 7:
            if u == 0:
                drain(srecv, s_rs)
            finish_unit(u, low, high)
            low = high = None
            if u in (1, 3):
                own_base(u // 2, own)
                own = None
    finish_quarter(0)
    finish_quarter(1)
    finish_quarter(2)
    finish_quarter(3)
    g1.own(4)
    for g in range(2):
        block = jnp.concatenate([h1[me, 2 * g], h1[me, 2 * g + 1]], axis=1)
        zbase[g] = jnp.dot(w2st[...], block, preferred_element_type=F32)
    for slot, p in ((2, 0), (1, 0), (1, 1), (2, 1), (2, 2), (1, 2)):
        g1.take(slot, p)
    for p in range(4):
        g1.take(3, p)
    g1.add()
    g1.take(0, 0)
    g1.take(0, 1)
    g1.take_forwards(6)
    g1.add()
    for slot, p in ((2, 3), (1, 3), (0, 3), (0, 2)):
        g1.take(slot, p)
    g1.add()
    g1.take_forwards(4)
    g1.add()
    g1.take_forwards(2)
    g1.add()

    inv_own = jnp.concatenate(
        [jnp.broadcast_to(inv[OWN + g, 0:1, :], (HID, LANES)) for g in range(2)], axis=1
    )
    for g in range(2):
        mean1 = (acc[:, lanes(g)] * inv_own[:, lanes(g)]).astype(BF)
        pre2 = zbase[g] + jnp.dot(w2nt[...], mean1, preferred_element_type=F32)
        for half in range(2):
            h2[me, 2 * g + half] = jnp.maximum(pre2[:, quarter(half)], 0.0).astype(BF)
        g2.send(2, 2 * g)
        g2.send(1, 2 * g + 1)
    for slot, p in ((2, 1), (1, 0), (2, 3), (1, 2)):
        g2.send(slot, p)
    for p in range(4):
        g2.send(3, p)
    g2.own(4)
    for g in range(2):
        block = jnp.concatenate([h2[me, 2 * g], h2[me, 2 * g + 1]], axis=1)
        out_ref[:, lanes(g)] = jnp.dot(ws3t[...], block, preferred_element_type=F32)
    drain(ids_rcv, ids_ss)
    drain(yown, y_ss)
    drain(ssend, s_ss)
    drain(rs_send, r_ss)
    drain(h1.at[0:7], g1_ss)
    for p in range(4):
        g2.take(3, p)
    g2.add()
    for slot, p in ((2, 0), (1, 1), (2, 2), (1, 3)):
        g2.take(slot, p)
    g2.add()
    for slot, p in ((2, 1), (1, 0), (2, 3), (1, 2)):
        g2.take(slot, p)
    g2.take_forwards(4)
    g2.add()
    g2.take(0, 0)
    g2.take(0, 1)
    g2.take_forwards(4)
    g2.add()
    g2.take(0, 2)
    g2.take(0, 3)
    g2.take_forwards(2)
    g2.add()
    g2.take_forwards(2)
    g2.add()
    for g in range(2):
        mean2 = (acc[:, lanes(g)] * inv_own[:, lanes(g)]).astype(BF)
        out_ref[:, lanes(g)] += jnp.dot(wn3t[...], mean2, preferred_element_type=F32)
    drain(h2.at[0:7], g2_ss)


def solution(mesh):
    def device_step(feat, ws1, wn1, ids, mask, ws2, wn2, ws3, wn3):
        operands = (feat.T, ws1, wn1, ids.T, mask.T, ws2, wn2, ws3.T, wn3.T)
        vm = pl.BlockSpec(memory_space=pltpu.VMEM)
        dma = pltpu.SemaphoreType.DMA
        out_t = pl.pallas_call(
            kernel,
            out_shape=jax.ShapeDtypeStruct((7, BLK), F32),
            in_specs=[pl.BlockSpec(memory_space=pltpu.HBM)] * 9,
            out_specs=vm,
            scratch_shapes=[
                pltpu.VMEM((N_DEV, 192, BLK), BF),
                pltpu.VMEM((192, HID), BF),
                pltpu.VMEM((192, HID), BF),
                pltpu.VMEM((FAN, BLK), jnp.int32),
                pltpu.VMEM((FAN, BLK), jnp.int32),
                pltpu.VMEM((HID, HID), BF),
                pltpu.VMEM((HID, HID), BF),
                pltpu.VMEM((7, HID), BF),
                pltpu.VMEM((7, HID), BF),
                pltpu.VMEM((2 * HID, 192), BF),
                pltpu.VMEM((HID, HID), BF),
                pltpu.VMEM((HID, HID), BF),
                pltpu.VMEM((N_DEV, HID, BLK), BF),
                pltpu.VMEM((N_DEV, HID, BLK), BF),
                pltpu.VMEM((N_DEV, HID, BLK), BF),
                pltpu.VMEM((4, HID, BLK), F32),
                pltpu.VMEM((4, HID, BLK), BF),
                pltpu.VMEM((4, HID, BLK), BF),
                pltpu.VMEM((16, BLK), jnp.int16),
                pltpu.VMEM((3, 16, BLK), jnp.int16),
                pltpu.VMEM((8, 16, LANES), jnp.int32),
                pltpu.VMEM((HALF // TILE, TILE // 8, 8, LANES), jnp.int16),
                pltpu.VMEM((8, FAN, 8, LANES), jnp.int16),
                pltpu.VMEM((8, FAN, 8, LANES), BF),
                pltpu.VMEM((8, 8, LANES), F32),
                pltpu.VMEM((RING, 2, TILE // 8, 8, LANES), BF),
                pltpu.VMEM((N_DEV, BLK // 8, 8, BLK), BF),
                pltpu.VMEM((HID, BLK), F32),
                pltpu.VMEM((2, HID, LANES), F32),
                pltpu.VMEM((3, 4, HID, Q), BF),
                pltpu.VMEM((3, 4, HID, Q), BF),
                pltpu.VMEM((N_DEV, 4, HID, Q), BF),
                pltpu.VMEM((N_DEV, 4, HID, Q), BF),
                dma((8,)),
                dma,
                dma, dma((3,)),
                dma, dma,
                dma, dma,
                dma, dma((12,)),
                dma, dma((28,)),
                dma, dma((28,)),
            ],
            compiler_params=pltpu.CompilerParams(
                collective_id=0, has_side_effects=True, vmem_limit_bytes=32 * 1024 * 1024
            ),
            name="graphsage",
        )(*(pltpu.with_memory_space_constraint(a, pltpu.HBM) for a in operands))
        return out_t.T

    col_split = P(None, "g")
    row_split = P("g", None)
    replicated = P()
    return jax.shard_map(
        device_step,
        mesh=mesh,
        in_specs=(col_split, row_split, row_split, row_split, row_split, replicated, replicated, replicated, replicated),
        out_specs=row_split,
        check_vma=False,
    )
```

```python
import jax
import jax.numpy as jnp
from jax import lax
from jax.experimental import pallas as pl
from jax.experimental.pallas import tpu as pltpu
from jax.sharding import PartitionSpec as P

MESH = pl.DeviceIdType.MESH
N_DEV = 8
NODES = 4096
BLK = NODES // N_DEV
HALF = NODES // 2
FAN = 10
HID = 128
TILE = 256
LANES = 256
BF = jnp.bfloat16
F32 = jnp.float32


UNITS = (((2, 0), (1, 0)), ((0, 0), (0, 1)), ((2, 1), (1, 1)), ((0, 2), (0, 3)), ((2, 2), (1, 2)), ((2, 3), (1, 3)))
OWN = 6
RING = 6
Q = 128


def spread_ids(ids_s32, idb, wb, inv, u):
    words, weights = [], []
    degree = jnp.zeros((8, LANES), F32)
    for k in range(FAN):
        raw = jnp.broadcast_to(ids_s32[u, k : k + 1, :], (8, LANES))
        valid = raw >= 0
        degree += jnp.where(valid, 1.0, 0.0)
        upper = raw >= HALF
        word = jnp.where(upper, raw - HALF, raw)
        weight = jnp.where(valid, jnp.where(upper, 1.0, 0.0625), 0.0)
        for m in range(k):
            same = word == words[m]
            weights[m] = weights[m] + jnp.where(same, weight, 0.0)
            word = jnp.where(same, -1, word)
        words.append(word)
        weights.append(weight)
    inv[u] = 1.0 / degree
    for k in range(FAN):
        idb[u, k] = words[k].astype(jnp.int16)
        wb[u, k] = weights[k].astype(BF)


def build_tile(tile, row_ids, idb, wb, u, store_low, store_high):
    ids = [idb[u, k] for k in range(FAN)]
    wts = [wb[u, k] for k in range(FAN)]
    for r in range(0, TILE // 8, 8):
        rows = row_ids[tile, r : r + 8]
        acc = jnp.zeros((8, 8, LANES), BF)
        for k in range(FAN):
            acc = jnp.where(ids[k][None] == rows, wts[k][None], acc)
        high = jnp.floor(acc)
        store_high(r, high)
        store_low(r, acc - high)


def kernel(
    x_hbm, ws1_hbm, wn1_hbm, ids_hbm, mask_hbm, ws2_hbm, wn2_hbm, ws3_hbm, wn3_hbm, out_ref,
    x_v, ws1, wn1, ids_in, mask_in, ws2, wn2, ws3t, wn3t,
    w1t, w2st, w2nt, yown, yrecv, ysum, sown, ssend, srecv,
    ids_pkt, ids_rcv, ids_s32, row_ids, idb, wb, inv,
    ring, a_own, acc, zbase, rs_send, rs_recv, h1, h2,
    in_sem, x_sem, ids_ss, ids_rs, y_ss, y_rs, s_ss, s_rs, r_ss, r_rs, g1_ss, g1_rs, g2_ss, g2_rs,
):
    me = lax.axis_index("g")
    core = lax.rem(me, 2)
    cx = lax.rem(me // 2, 2)
    cy = me // 4
    partner = me + 1 - 2 * core
    steps = (6 - 4 * cx - 8 * cy, 4 - 8 * cy, 2 - 4 * cx)
    peers = tuple(partner + step for step in steps)
    mates = tuple(me + step for step in steps)
    mine, theirs = (me, *peers), (partner, *mates)

    barrier = pltpu.get_barrier_semaphore()
    for peer in (*peers, partner):
        pl.semaphore_signal(barrier, inc=1, device_id=(peer,), device_id_type=MESH)

    def fetch(src, dst, i):
        cp = pltpu.make_async_copy(src, dst, in_sem.at[i])
        cp.start()
        return cp

    ids_cp = fetch(ids_hbm, ids_in, 0)
    mask_cp = fetch(mask_hbm, mask_in, 1)
    w1_cps = [fetch(ws1_hbm, ws1, 2), fetch(wn1_hbm, wn1, 3)]
    for b in range(N_DEV):
        cp = pltpu.make_async_copy(x_hbm.at[:, pl.ds(b * BLK, BLK)], x_v.at[b], x_sem)
        cp.start()
    late_cps = [fetch(ws2_hbm, ws2, 4), fetch(wn2_hbm, wn2, 5), fetch(ws3_hbm, ws3t, 6), fetch(wn3_hbm, wn3t, 7)]

    def remote(src, dst, ss, rs, dev):
        return pltpu.make_async_remote_copy(
            src_ref=src, dst_ref=dst, send_sem=ss, recv_sem=rs, device_id=(dev,), device_id_type=MESH
        )

    def drain(ref, sem):
        pltpu.make_async_copy(ref, ref, sem).wait()

    row_shape = (TILE // 8, 8, LANES)
    row_base = lax.broadcasted_iota(jnp.int32, row_shape, 0) * 8 + lax.broadcasted_iota(jnp.int32, row_shape, 1)
    for tile in range(HALF // TILE):
        row_ids[tile] = (row_base + tile * TILE).astype(jnp.int16)
    ids_pkt[...] = jnp.full(ids_pkt.shape, -1, jnp.int16)
    ids_cp.wait()
    mask_cp.wait()
    masked = jnp.where(mask_in[...] > 0, ids_in[...], -1)
    ids_pkt[0:FAN, :] = masked.astype(jnp.int16)
    pl.semaphore_wait(barrier, 4)
    id_copies = [remote(ids_pkt, ids_rcv.at[s], ids_ss, ids_rs.at[s], peers[s]) for s in range(3)]
    for s in (2, 1, 0):
        id_copies[s].start()
    for g in range(2):
        ids_s32[OWN + g, 0:FAN, :] = masked[:, g * LANES : (g + 1) * LANES]
        spread_ids(ids_s32, idb, wb, inv, OWN + g)
    for cp in w1_cps:
        cp.wait()
    w1t[0:HID, :] = ws1[...].T
    w1t[HID:, :] = wn1[...].T

    def build_own(tile, g):
        def put(half):
            def store(r, v):
                v = v if half else v * jnp.array(16.0, BF)
                row = tile % 2 * (TILE // 8) + r
                a_own[half * 4 + tile // 2, row : row + 8, :, g * LANES : (g + 1) * LANES] = v

            return store

        build_tile(tile, row_ids, idb, wb, OWN + g, put(0), put(1))

    drain(x_v, x_sem)
    for i in range(4):
        part = jnp.dot(w1t[...], x_v[theirs[i]], preferred_element_type=F32)
        yown[theirs[i]] = part[HID:].astype(BF)
        ssend[i] = part[:HID].astype(BF)
        part2 = jnp.dot(w1t[...], x_v[mine[i]], preferred_element_type=F32)
        yown[mine[i]] = part2[HID:].astype(BF)
        sown[i] = part2[:HID]
        for b in (theirs[i], mine[i]):
            remote(yown.at[b], yrecv.at[b], y_ss, y_rs, partner).start()
        build_own(2 * i, 0)
    for i in range(4):
        remote(ssend.at[i], srecv.at[i], s_ss, s_rs, partner).start()
    for tile in range(1, 8, 2):
        build_own(tile, 0)
    for tile in range(8):
        build_own(tile, 1)
    for cp in late_cps:
        cp.wait()
    w2st[...] = ws2[...].T
    w2nt[...] = wn2[...].T

    def build_into(flat):
        def put(half):
            def store(r, v):
                ring[flat % RING, half, r : r + 8] = v

            return store

        build_tile(flat % 8, row_ids, idb, wb, flat // 8, put(0), put(1))

    def dot_from(flat):
        tile = flat % 8
        cols = slice(tile % 2 * TILE, (tile % 2 + 1) * TILE)
        low = ring[flat % RING, 0].reshape(TILE, LANES)
        high = ring[flat % RING, 1].reshape(TILE, LANES)
        return (
            jnp.dot(ysum[tile // 2, :, cols], low, preferred_element_type=F32),
            jnp.dot(ysum[4 + tile // 2, :, cols], high, preferred_element_type=F32),
        )

    def lanes(g):
        return slice(g * LANES, (g + 1) * LANES)

    def quarter(q):
        return slice(q * Q, (q + 1) * Q)

    def take_ids(s):
        id_copies[s].wait_recv()
        for u, pair in enumerate(UNITS):
            for half, (slot, q) in enumerate(pair):
                if slot == s:
                    ids_s32[u, :, quarter(half)] = ids_rcv[s, :, quarter(q)].astype(jnp.int32)

    rs_copies = {}

    def finish_unit(u, low, high):
        total = (low * 16.0 + high) * jnp.broadcast_to(inv[u, 0:1, :], (HID, LANES))
        for half, (s, q) in enumerate(UNITS[u]):
            part = total[:, quarter(half)] + sown[1 + s, :, quarter(q)] + srecv[1 + s, :, quarter(q)].astype(F32)
            rs_send[s, q] = part.astype(BF)
            rs_copies[s, q] = remote(rs_send.at[s, q], rs_recv.at[s, q], r_ss, r_rs.at[4 * s + q], peers[s])
            rs_copies[s, q].start()

    def own_piece(b, g):
        return jnp.dot(ysum[b], a_own[b, :, :, lanes(g)].reshape(BLK, LANES), preferred_element_type=F32)

    def own_base(g, own):
        base = own * jnp.broadcast_to(inv[OWN + g, 0:1, :], (HID, LANES))
        zbase[g] = base + sown[0, :, lanes(g)] + srecv[0, :, lanes(g)].astype(F32)

    def own_dot(h, b, p):
        rows = a_own[b, p * Q // 8 : (p + 1) * Q // 8].reshape(Q, BLK)
        return jnp.dot(h[b, p], rows, preferred_element_type=F32)

    class Gather:
        def __init__(self, h, ss, rs, direct):
            self.h, self.ss, self.rs, self.direct = h, ss, rs, direct
            self.copies, self.forwards, self.ready = {}, [], []

        def copy(self, block, p, slot, dev):
            return remote(self.h.at[block, p], self.h.at[block, p], self.ss, self.rs.at[7 * p + slot], dev)

        def send(self, slot, p):
            dev = partner if slot == 3 else peers[slot]
            self.copies[slot, p] = self.copy(me, p, slot, dev)
            self.copies[slot, p].start()

        def take(self, slot, p):
            self.copies[slot, p].wait_recv()
            block = partner if slot == 3 else mates[0] if slot == 0 and p not in self.direct else peers[slot]
            if p not in self.direct and slot == (1 if p % 2 else 2):
                self.copies[0, p] = self.copy(block, p, 0, peers[3 - slot])
                self.copies[0, p].start()
            if slot < 3:
                fwd = self.copy(block, p, 4 + slot, partner)
                fwd.start()
                self.forwards.append((slot, p, fwd))
            self.ready.append((block, p))

        def take_forwards(self, n):
            for slot, p, fwd in self.forwards[:n]:
                fwd.wait_recv()
                relayed = slot == 0 and p not in self.direct
                self.ready.append((peers[0] if relayed else mates[slot], p))
            self.forwards = self.forwards[n:]

        def own(self, pieces):
            acc[...] = sum(own_dot(self.h, me, p) for p in range(pieces))

        def add(self):
            acc[...] += sum(own_dot(self.h, b, p) for b, p in self.ready)
            self.ready = []

    g1 = Gather(h1, g1_ss, g1_rs, direct=(3,))
    g2 = Gather(h2, g2_ss, g2_rs, direct=())

    def finish_quarter(q):
        z = zbase[q // 2, :, quarter(q % 2)]
        for t in (1, 2, 0):
            rs_copies[t, q].wait_recv()
            z = z + rs_recv[t, q].astype(F32)
        h1[me, q] = jnp.maximum(z, 0.0).astype(BF)
        for slot in (0, 2, 1, 3) if q in g1.direct else (2, 1, 3):
            g1.send(slot, q)

    take_ids(2)
    take_ids(1)
    spread_ids(ids_s32, idb, wb, inv, 0)
    lead = 3
    for flat in range(lead):
        build_into(flat)
    drain(yrecv, y_rs)
    for b in range(N_DEV):
        ysum[b] = yown[b] + yrecv[b]
    built = lead
    low = high = own = None
    for flat in range(48):
        u, tile = flat // 8, flat % 8
        while built < 48 and built - flat < 2 or (built < 48 and tile % 2 == 0 and built - flat < lead):
            if built == 8:
                take_ids(0)
            if built % 8 == 0:
                spread_ids(ids_s32, idb, wb, inv, built // 8)
            build_into(built)
            built += 1
        part = dot_from(flat)
        low = part[0] if low is None else low + part[0]
        high = part[1] if high is None else high + part[1]
        if u in (1, 3):
            own = own_piece(tile, u // 2) if own is None else own + own_piece(tile, u // 2)
        if tile == 7:
            if u == 0:
                drain(srecv, s_rs)
            finish_unit(u, low, high)
            low = high = None
            if u in (1, 3):
                own_base(u // 2, own)
                own = None
    finish_quarter(0)
    finish_quarter(1)
    finish_quarter(2)
    finish_quarter(3)
    g1.own(4)
    for g in range(2):
        block = jnp.concatenate([h1[me, 2 * g], h1[me, 2 * g + 1]], axis=1)
        zbase[g] = jnp.dot(w2st[...], block, preferred_element_type=F32)
    for slot, p in ((2, 0), (1, 0), (1, 1), (2, 1), (2, 2), (1, 2)):
        g1.take(slot, p)
    for p in range(4):
        g1.take(3, p)
    g1.add()
    for slot, p in ((2, 3), (1, 3), (0, 0), (0, 1)):
        g1.take(slot, p)
    g1.take_forwards(6)
    g1.add()
    for slot, p in ((0, 3), (0, 2)):
        g1.take(slot, p)
    g1.add()
    g1.take_forwards(4)
    g1.add()
    g1.take_forwards(2)
    g1.add()

    inv_own = jnp.concatenate(
        [jnp.broadcast_to(inv[OWN + g, 0:1, :], (HID, LANES)) for g in range(2)], axis=1
    )
    for g in range(2):
        mean1 = (acc[:, lanes(g)] * inv_own[:, lanes(g)]).astype(BF)
        pre2 = zbase[g] + jnp.dot(w2nt[...], mean1, preferred_element_type=F32)
        for half in range(2):
            h2[me, 2 * g + half] = jnp.maximum(pre2[:, quarter(half)], 0.0).astype(BF)
        g2.send(2, 2 * g)
        g2.send(1, 2 * g + 1)
    for slot, p in ((2, 1), (1, 0), (2, 3), (1, 2)):
        g2.send(slot, p)
    for p in range(4):
        g2.send(3, p)
    g2.own(4)
    for g in range(2):
        block = jnp.concatenate([h2[me, 2 * g], h2[me, 2 * g + 1]], axis=1)
        out_ref[:, lanes(g)] = jnp.dot(ws3t[...], block, preferred_element_type=F32)
    drain(ids_rcv, ids_ss)
    drain(yown, y_ss)
    drain(ssend, s_ss)
    drain(rs_send, r_ss)
    drain(h1.at[0:7], g1_ss)
    for p in range(4):
        g2.take(3, p)
    g2.add()
    for slot, p in ((2, 0), (1, 1), (2, 2), (1, 3)):
        g2.take(slot, p)
    g2.add()
    for slot, p in ((2, 1), (1, 0), (2, 3), (1, 2)):
        g2.take(slot, p)
    g2.take_forwards(4)
    g2.add()
    g2.take(0, 0)
    g2.take(0, 1)
    g2.take_forwards(4)
    g2.add()
    g2.take(0, 2)
    g2.take(0, 3)
    g2.take_forwards(2)
    g2.add()
    g2.take_forwards(2)
    g2.add()
    for g in range(2):
        mean2 = (acc[:, lanes(g)] * inv_own[:, lanes(g)]).astype(BF)
        out_ref[:, lanes(g)] += jnp.dot(wn3t[...], mean2, preferred_element_type=F32)
    drain(h2.at[0:7], g2_ss)


def solution(mesh):
    def device_step(feat, ws1, wn1, ids, mask, ws2, wn2, ws3, wn3):
        operands = (feat.T, ws1, wn1, ids.T, mask.T, ws2, wn2, ws3.T, wn3.T)
        vm = pl.BlockSpec(memory_space=pltpu.VMEM)
        dma = pltpu.SemaphoreType.DMA
        out_t = pl.pallas_call(
            kernel,
            out_shape=jax.ShapeDtypeStruct((7, BLK), F32),
            in_specs=[pl.BlockSpec(memory_space=pltpu.HBM)] * 9,
            out_specs=vm,
            scratch_shapes=[
                pltpu.VMEM((N_DEV, 192, BLK), BF),
                pltpu.VMEM((192, HID), BF),
                pltpu.VMEM((192, HID), BF),
                pltpu.VMEM((FAN, BLK), jnp.int32),
                pltpu.VMEM((FAN, BLK), jnp.int32),
                pltpu.VMEM((HID, HID), BF),
                pltpu.VMEM((HID, HID), BF),
                pltpu.VMEM((7, HID), BF),
                pltpu.VMEM((7, HID), BF),
                pltpu.VMEM((2 * HID, 192), BF),
                pltpu.VMEM((HID, HID), BF),
                pltpu.VMEM((HID, HID), BF),
                pltpu.VMEM((N_DEV, HID, BLK), BF),
                pltpu.VMEM((N_DEV, HID, BLK), BF),
                pltpu.VMEM((N_DEV, HID, BLK), BF),
                pltpu.VMEM((4, HID, BLK), F32),
                pltpu.VMEM((4, HID, BLK), BF),
                pltpu.VMEM((4, HID, BLK), BF),
                pltpu.VMEM((16, BLK), jnp.int16),
                pltpu.VMEM((3, 16, BLK), jnp.int16),
                pltpu.VMEM((8, 16, LANES), jnp.int32),
                pltpu.VMEM((HALF // TILE, TILE // 8, 8, LANES), jnp.int16),
                pltpu.VMEM((8, FAN, 8, LANES), jnp.int16),
                pltpu.VMEM((8, FAN, 8, LANES), BF),
                pltpu.VMEM((8, 8, LANES), F32),
                pltpu.VMEM((RING, 2, TILE // 8, 8, LANES), BF),
                pltpu.VMEM((N_DEV, BLK // 8, 8, BLK), BF),
                pltpu.VMEM((HID, BLK), F32),
                pltpu.VMEM((2, HID, LANES), F32),
                pltpu.VMEM((3, 4, HID, Q), BF),
                pltpu.VMEM((3, 4, HID, Q), BF),
                pltpu.VMEM((N_DEV, 4, HID, Q), BF),
                pltpu.VMEM((N_DEV, 4, HID, Q), BF),
                dma((8,)),
                dma,
                dma, dma((3,)),
                dma, dma,
                dma, dma,
                dma, dma((12,)),
                dma, dma((28,)),
                dma, dma((28,)),
            ],
            compiler_params=pltpu.CompilerParams(
                collective_id=0, has_side_effects=True, vmem_limit_bytes=32 * 1024 * 1024
            ),
            name="graphsage",
        )(*(pltpu.with_memory_space_constraint(a, pltpu.HBM) for a in operands))
        return out_t.T

    col_split = P(None, "g")
    row_split = P("g", None)
    replicated = P()
    return jax.shard_map(
        device_step,
        mesh=mesh,
        in_specs=(col_split, row_split, row_split, row_split, row_split, replicated, replicated, replicated, replicated),
        out_specs=row_split,
        check_vma=False,
    )
```

```python
import jax
import jax.numpy as jnp
from jax import lax
from jax.experimental import pallas as pl
from jax.experimental.pallas import tpu as pltpu
from jax.sharding import PartitionSpec as P

MESH = pl.DeviceIdType.MESH
N_DEV = 8
NODES = 4096
BLK = NODES // N_DEV
HALF = NODES // 2
FAN = 10
HID = 128
TILE = 256
LANES = 256
BF = jnp.bfloat16
F32 = jnp.float32


UNITS = (((2, 0), (1, 0)), ((0, 0), (0, 1)), ((2, 1), (1, 1)), ((0, 2), (0, 3)), ((2, 2), (1, 2)), ((2, 3), (1, 3)))
OWN = 6
RING = 6
Q = 128


def spread_ids(ids_s32, idb, wb, inv, u):
    words, weights = [], []
    degree = jnp.zeros((8, LANES), F32)
    for k in range(FAN):
        raw = jnp.broadcast_to(ids_s32[u, k : k + 1, :], (8, LANES))
        valid = raw >= 0
        degree += jnp.where(valid, 1.0, 0.0)
        upper = raw >= HALF
        word = jnp.where(upper, raw - HALF, raw)
        weight = jnp.where(valid, jnp.where(upper, 1.0, 0.0625), 0.0)
        for m in range(k):
            same = word == words[m]
            weights[m] = weights[m] + jnp.where(same, weight, 0.0)
            word = jnp.where(same, -1, word)
        words.append(word)
        weights.append(weight)
    inv[u] = 1.0 / degree
    for k in range(FAN):
        idb[u, k] = words[k].astype(jnp.int16)
        wb[u, k] = weights[k].astype(BF)


def build_tile(tile, row_ids, idb, wb, u, store_low, store_high):
    ids = [idb[u, k] for k in range(FAN)]
    wts = [wb[u, k] for k in range(FAN)]
    for r in range(0, TILE // 8, 8):
        rows = row_ids[tile, r : r + 8]
        acc = jnp.zeros((8, 8, LANES), BF)
        for k in range(FAN):
            acc = jnp.where(ids[k][None] == rows, wts[k][None], acc)
        high = jnp.floor(acc)
        store_high(r, high)
        store_low(r, acc - high)


def kernel(
    x_hbm, ws1_hbm, wn1_hbm, ids_hbm, mask_hbm, ws2_hbm, wn2_hbm, ws3_hbm, wn3_hbm, out_ref,
    x_v, ws1, wn1, ids_in, mask_in, ws2, wn2, ws3t, wn3t,
    w1t, w2st, w2nt, yown, yrecv, ysum, sown, ssend, srecv,
    ids_pkt, ids_rcv, ids_s32, row_ids, idb, wb, inv,
    ring, a_own, acc, zbase, rs_send, rs_recv, h1, h2,
    in_sem, x_sem, ids_ss, ids_rs, y_ss, y_rs, s_ss, s_rs, r_ss, r_rs, g1_ss, g1_rs, g2_ss, g2_rs,
):
    me = lax.axis_index("g")
    core = lax.rem(me, 2)
    cx = lax.rem(me // 2, 2)
    cy = me // 4
    partner = me + 1 - 2 * core
    steps = (6 - 4 * cx - 8 * cy, 4 - 8 * cy, 2 - 4 * cx)
    peers = tuple(partner + step for step in steps)
    mates = tuple(me + step for step in steps)
    mine, theirs = (me, *peers), (partner, *mates)

    barrier = pltpu.get_barrier_semaphore()
    for peer in (*peers, partner):
        pl.semaphore_signal(barrier, inc=1, device_id=(peer,), device_id_type=MESH)

    def fetch(src, dst, i):
        cp = pltpu.make_async_copy(src, dst, in_sem.at[i])
        cp.start()
        return cp

    ids_cp = fetch(ids_hbm, ids_in, 0)
    mask_cp = fetch(mask_hbm, mask_in, 1)
    w1_cps = [fetch(ws1_hbm, ws1, 2), fetch(wn1_hbm, wn1, 3)]
    for b in range(N_DEV):
        cp = pltpu.make_async_copy(x_hbm.at[:, pl.ds(b * BLK, BLK)], x_v.at[b], x_sem)
        cp.start()
    late_cps = [fetch(ws2_hbm, ws2, 4), fetch(wn2_hbm, wn2, 5), fetch(ws3_hbm, ws3t, 6), fetch(wn3_hbm, wn3t, 7)]

    def remote(src, dst, ss, rs, dev):
        return pltpu.make_async_remote_copy(
            src_ref=src, dst_ref=dst, send_sem=ss, recv_sem=rs, device_id=(dev,), device_id_type=MESH
        )

    def drain(ref, sem):
        pltpu.make_async_copy(ref, ref, sem).wait()

    row_shape = (TILE // 8, 8, LANES)
    row_base = lax.broadcasted_iota(jnp.int32, row_shape, 0) * 8 + lax.broadcasted_iota(jnp.int32, row_shape, 1)
    for tile in range(HALF // TILE):
        row_ids[tile] = (row_base + tile * TILE).astype(jnp.int16)
    ids_pkt[...] = jnp.full(ids_pkt.shape, -1, jnp.int16)
    ids_cp.wait()
    mask_cp.wait()
    masked = jnp.where(mask_in[...] > 0, ids_in[...], -1)
    ids_pkt[0:FAN, :] = masked.astype(jnp.int16)
    pl.semaphore_wait(barrier, 4)
    id_copies = [remote(ids_pkt, ids_rcv.at[s], ids_ss, ids_rs.at[s], peers[s]) for s in range(3)]
    for s in (2, 1, 0):
        id_copies[s].start()
    for g in range(2):
        ids_s32[OWN + g, 0:FAN, :] = masked[:, g * LANES : (g + 1) * LANES]
        spread_ids(ids_s32, idb, wb, inv, OWN + g)
    for cp in w1_cps:
        cp.wait()
    w1t[0:HID, :] = ws1[...].T
    w1t[HID:, :] = wn1[...].T

    def build_own(tile, g):
        def put(half):
            def store(r, v):
                v = v if half else v * jnp.array(16.0, BF)
                row = tile % 2 * (TILE // 8) + r
                a_own[half * 4 + tile // 2, row : row + 8, :, g * LANES : (g + 1) * LANES] = v

            return store

        build_tile(tile, row_ids, idb, wb, OWN + g, put(0), put(1))

    drain(x_v, x_sem)
    for i in range(4):
        part = jnp.dot(w1t[...], x_v[theirs[i]], preferred_element_type=F32)
        yown[theirs[i]] = part[HID:].astype(BF)
        ssend[i] = part[:HID].astype(BF)
        part2 = jnp.dot(w1t[...], x_v[mine[i]], preferred_element_type=F32)
        yown[mine[i]] = part2[HID:].astype(BF)
        sown[i] = part2[:HID]
        for b in (theirs[i], mine[i]):
            remote(yown.at[b], yrecv.at[b], y_ss, y_rs, partner).start()
        build_own(2 * i, 0)
    for i in range(4):
        remote(ssend.at[i], srecv.at[i], s_ss, s_rs, partner).start()
    for tile in range(1, 8, 2):
        build_own(tile, 0)
    for tile in range(8):
        build_own(tile, 1)
    for cp in late_cps:
        cp.wait()
    w2st[...] = ws2[...].T
    w2nt[...] = wn2[...].T

    def build_into(flat):
        def put(half):
            def store(r, v):
                ring[flat % RING, half, r : r + 8] = v

            return store

        build_tile(flat % 8, row_ids, idb, wb, flat // 8, put(0), put(1))

    def dot_from(flat):
        tile = flat % 8
        cols = slice(tile % 2 * TILE, (tile % 2 + 1) * TILE)
        low = ring[flat % RING, 0].reshape(TILE, LANES)
        high = ring[flat % RING, 1].reshape(TILE, LANES)
        return (
            jnp.dot(ysum[tile // 2, :, cols], low, preferred_element_type=F32),
            jnp.dot(ysum[4 + tile // 2, :, cols], high, preferred_element_type=F32),
        )

    def lanes(g):
        return slice(g * LANES, (g + 1) * LANES)

    def quarter(q):
        return slice(q * Q, (q + 1) * Q)

    def take_ids(s):
        id_copies[s].wait_recv()
        for u, pair in enumerate(UNITS):
            for half, (slot, q) in enumerate(pair):
                if slot == s:
                    ids_s32[u, :, quarter(half)] = ids_rcv[s, :, quarter(q)].astype(jnp.int32)

    rs_copies = {}

    def finish_unit(u, low, high):
        total = (low * 16.0 + high) * jnp.broadcast_to(inv[u, 0:1, :], (HID, LANES))
        for half, (s, q) in enumerate(UNITS[u]):
            part = total[:, quarter(half)] + sown[1 + s, :, quarter(q)] + srecv[1 + s, :, quarter(q)].astype(F32)
            rs_send[s, q] = part.astype(BF)
            rs_copies[s, q] = remote(rs_send.at[s, q], rs_recv.at[s, q], r_ss, r_rs.at[4 * s + q], peers[s])
            rs_copies[s, q].start()

    def own_piece(b, g):
        return jnp.dot(ysum[b], a_own[b, :, :, lanes(g)].reshape(BLK, LANES), preferred_element_type=F32)

    def own_base(g, own):
        base = own * jnp.broadcast_to(inv[OWN + g, 0:1, :], (HID, LANES))
        zbase[g] = base + sown[0, :, lanes(g)] + srecv[0, :, lanes(g)].astype(F32)

    def own_dot(h, b, p):
        rows = a_own[b, p * Q // 8 : (p + 1) * Q // 8].reshape(Q, BLK)
        return jnp.dot(h[b, p], rows, preferred_element_type=F32)

    class Gather:
        def __init__(self, h, ss, rs, direct):
            self.h, self.ss, self.rs, self.direct = h, ss, rs, direct
            self.copies, self.forwards, self.ready = {}, [], []

        def copy(self, block, p, slot, dev):
            return remote(self.h.at[block, p], self.h.at[block, p], self.ss, self.rs.at[7 * p + slot], dev)

        def send(self, slot, p):
            dev = partner if slot == 3 else peers[slot]
            self.copies[slot, p] = self.copy(me, p, slot, dev)
            self.copies[slot, p].start()

        def take(self, slot, p):
            self.copies[slot, p].wait_recv()
            block = partner if slot == 3 else mates[0] if slot == 0 and p not in self.direct else peers[slot]
            if p not in self.direct and slot == (1 if p % 2 else 2):
                self.copies[0, p] = self.copy(block, p, 0, peers[3 - slot])
                self.copies[0, p].start()
            if slot < 3:
                fwd = self.copy(block, p, 4 + slot, partner)
                fwd.start()
                self.forwards.append((slot, p, fwd))
            self.ready.append((block, p))

        def take_forwards(self, n):
            for slot, p, fwd in self.forwards[:n]:
                fwd.wait_recv()
                relayed = slot == 0 and p not in self.direct
                self.ready.append((peers[0] if relayed else mates[slot], p))
            self.forwards = self.forwards[n:]

        def own(self, pieces):
            acc[...] = sum(own_dot(self.h, me, p) for p in range(pieces))

        def add(self):
            acc[...] += sum(own_dot(self.h, b, p) for b, p in self.ready)
            self.ready = []

    g1 = Gather(h1, g1_ss, g1_rs, direct=(2, 3))
    g2 = Gather(h2, g2_ss, g2_rs, direct=())

    def finish_quarter(q):
        z = zbase[q // 2, :, quarter(q % 2)]
        for t in (1, 2, 0):
            rs_copies[t, q].wait_recv()
            z = z + rs_recv[t, q].astype(F32)
        h1[me, q] = jnp.maximum(z, 0.0).astype(BF)
        for slot in (0, 2, 1, 3) if q in g1.direct else (2, 1, 3):
            g1.send(slot, q)

    take_ids(2)
    take_ids(1)
    spread_ids(ids_s32, idb, wb, inv, 0)
    lead = 3
    for flat in range(lead):
        build_into(flat)
    drain(yrecv, y_rs)
    for b in range(N_DEV):
        ysum[b] = yown[b] + yrecv[b]
    built = lead
    low = high = own = None
    for flat in range(48):
        u, tile = flat // 8, flat % 8
        while built < 48 and built - flat < 2 or (built < 48 and tile % 2 == 0 and built - flat < lead):
            if built == 8:
                take_ids(0)
            if built % 8 == 0:
                spread_ids(ids_s32, idb, wb, inv, built // 8)
            build_into(built)
            built += 1
        part = dot_from(flat)
        low = part[0] if low is None else low + part[0]
        high = part[1] if high is None else high + part[1]
        if u in (1, 3):
            own = own_piece(tile, u // 2) if own is None else own + own_piece(tile, u // 2)
        if tile == 7:
            if u == 0:
                drain(srecv, s_rs)
            finish_unit(u, low, high)
            low = high = None
            if u in (1, 3):
                own_base(u // 2, own)
                own = None
    finish_quarter(0)
    finish_quarter(1)
    finish_quarter(2)
    finish_quarter(3)
    g1.own(4)
    for g in range(2):
        block = jnp.concatenate([h1[me, 2 * g], h1[me, 2 * g + 1]], axis=1)
        zbase[g] = jnp.dot(w2st[...], block, preferred_element_type=F32)
    for slot, p in ((2, 0), (1, 0), (1, 1), (2, 1), (2, 2), (1, 2)):
        g1.take(slot, p)
    for p in range(4):
        g1.take(3, p)
    g1.add()
    for slot, p in ((2, 3), (1, 3), (0, 0), (0, 1)):
        g1.take(slot, p)
    g1.take_forwards(6)
    g1.add()
    for slot, p in ((0, 3), (0, 2)):
        g1.take(slot, p)
    g1.add()
    g1.take_forwards(4)
    g1.add()
    g1.take_forwards(2)
    g1.add()

    inv_own = jnp.concatenate(
        [jnp.broadcast_to(inv[OWN + g, 0:1, :], (HID, LANES)) for g in range(2)], axis=1
    )
    for g in range(2):
        mean1 = (acc[:, lanes(g)] * inv_own[:, lanes(g)]).astype(BF)
        pre2 = zbase[g] + jnp.dot(w2nt[...], mean1, preferred_element_type=F32)
        for half in range(2):
            h2[me, 2 * g + half] = jnp.maximum(pre2[:, quarter(half)], 0.0).astype(BF)
        g2.send(2, 2 * g)
        g2.send(1, 2 * g + 1)
    for slot, p in ((2, 1), (1, 0), (2, 3), (1, 2)):
        g2.send(slot, p)
    for p in range(4):
        g2.send(3, p)
    g2.own(4)
    for g in range(2):
        block = jnp.concatenate([h2[me, 2 * g], h2[me, 2 * g + 1]], axis=1)
        out_ref[:, lanes(g)] = jnp.dot(ws3t[...], block, preferred_element_type=F32)
    drain(ids_rcv, ids_ss)
    drain(yown, y_ss)
    drain(ssend, s_ss)
    drain(rs_send, r_ss)
    drain(h1.at[0:7], g1_ss)
    for p in range(4):
        g2.take(3, p)
    g2.add()
    for slot, p in ((2, 0), (1, 1), (2, 2), (1, 3)):
        g2.take(slot, p)
    g2.add()
    for slot, p in ((2, 1), (1, 0), (2, 3), (1, 2)):
        g2.take(slot, p)
    g2.take_forwards(4)
    g2.add()
    g2.take(0, 0)
    g2.take(0, 1)
    g2.take_forwards(4)
    g2.add()
    g2.take(0, 2)
    g2.take(0, 3)
    g2.take_forwards(2)
    g2.add()
    g2.take_forwards(2)
    g2.add()
    for g in range(2):
        mean2 = (acc[:, lanes(g)] * inv_own[:, lanes(g)]).astype(BF)
        out_ref[:, lanes(g)] += jnp.dot(wn3t[...], mean2, preferred_element_type=F32)
    drain(h2.at[0:7], g2_ss)


def solution(mesh):
    def device_step(feat, ws1, wn1, ids, mask, ws2, wn2, ws3, wn3):
        operands = (feat.T, ws1, wn1, ids.T, mask.T, ws2, wn2, ws3.T, wn3.T)
        vm = pl.BlockSpec(memory_space=pltpu.VMEM)
        dma = pltpu.SemaphoreType.DMA
        out_t = pl.pallas_call(
            kernel,
            out_shape=jax.ShapeDtypeStruct((7, BLK), F32),
            in_specs=[pl.BlockSpec(memory_space=pltpu.HBM)] * 9,
            out_specs=vm,
            scratch_shapes=[
                pltpu.VMEM((N_DEV, 192, BLK), BF),
                pltpu.VMEM((192, HID), BF),
                pltpu.VMEM((192, HID), BF),
                pltpu.VMEM((FAN, BLK), jnp.int32),
                pltpu.VMEM((FAN, BLK), jnp.int32),
                pltpu.VMEM((HID, HID), BF),
                pltpu.VMEM((HID, HID), BF),
                pltpu.VMEM((7, HID), BF),
                pltpu.VMEM((7, HID), BF),
                pltpu.VMEM((2 * HID, 192), BF),
                pltpu.VMEM((HID, HID), BF),
                pltpu.VMEM((HID, HID), BF),
                pltpu.VMEM((N_DEV, HID, BLK), BF),
                pltpu.VMEM((N_DEV, HID, BLK), BF),
                pltpu.VMEM((N_DEV, HID, BLK), BF),
                pltpu.VMEM((4, HID, BLK), F32),
                pltpu.VMEM((4, HID, BLK), BF),
                pltpu.VMEM((4, HID, BLK), BF),
                pltpu.VMEM((16, BLK), jnp.int16),
                pltpu.VMEM((3, 16, BLK), jnp.int16),
                pltpu.VMEM((8, 16, LANES), jnp.int32),
                pltpu.VMEM((HALF // TILE, TILE // 8, 8, LANES), jnp.int16),
                pltpu.VMEM((8, FAN, 8, LANES), jnp.int16),
                pltpu.VMEM((8, FAN, 8, LANES), BF),
                pltpu.VMEM((8, 8, LANES), F32),
                pltpu.VMEM((RING, 2, TILE // 8, 8, LANES), BF),
                pltpu.VMEM((N_DEV, BLK // 8, 8, BLK), BF),
                pltpu.VMEM((HID, BLK), F32),
                pltpu.VMEM((2, HID, LANES), F32),
                pltpu.VMEM((3, 4, HID, Q), BF),
                pltpu.VMEM((3, 4, HID, Q), BF),
                pltpu.VMEM((N_DEV, 4, HID, Q), BF),
                pltpu.VMEM((N_DEV, 4, HID, Q), BF),
                dma((8,)),
                dma,
                dma, dma((3,)),
                dma, dma,
                dma, dma,
                dma, dma((12,)),
                dma, dma((28,)),
                dma, dma((28,)),
            ],
            compiler_params=pltpu.CompilerParams(
                collective_id=0, has_side_effects=True, vmem_limit_bytes=32 * 1024 * 1024
            ),
            name="graphsage",
        )(*(pltpu.with_memory_space_constraint(a, pltpu.HBM) for a in operands))
        return out_t.T

    col_split = P(None, "g")
    row_split = P("g", None)
    replicated = P()
    return jax.shard_map(
        device_step,
        mesh=mesh,
        in_specs=(col_split, row_split, row_split, row_split, row_split, replicated, replicated, replicated, replicated),
        out_specs=row_split,
        check_vma=False,
    )
```

```python
import jax
import jax.numpy as jnp
from jax import lax
from jax.experimental import pallas as pl
from jax.experimental.pallas import tpu as pltpu
from jax.sharding import PartitionSpec as P

MESH = pl.DeviceIdType.MESH
N_DEV = 8
NODES = 4096
BLK = NODES // N_DEV
HALF = NODES // 2
FAN = 10
HID = 128
TILE = 256
LANES = 256
BF = jnp.bfloat16
F32 = jnp.float32


UNITS = (((2, 0), (1, 0)), ((0, 0), (0, 1)), ((2, 1), (1, 1)), ((0, 2), (0, 3)), ((2, 2), (1, 2)), ((2, 3), (1, 3)))
OWN = 6
RING = 6
Q = 128


def spread_ids(ids_s32, idb, wb, inv, u):
    words, weights = [], []
    degree = jnp.zeros((8, LANES), F32)
    for k in range(FAN):
        raw = jnp.broadcast_to(ids_s32[u, k : k + 1, :], (8, LANES))
        valid = raw >= 0
        degree += jnp.where(valid, 1.0, 0.0)
        upper = raw >= HALF
        word = jnp.where(upper, raw - HALF, raw)
        weight = jnp.where(valid, jnp.where(upper, 1.0, 0.0625), 0.0)
        for m in range(k):
            same = word == words[m]
            weights[m] = weights[m] + jnp.where(same, weight, 0.0)
            word = jnp.where(same, -1, word)
        words.append(word)
        weights.append(weight)
    inv[u] = 1.0 / degree
    for k in range(FAN):
        idb[u, k] = words[k].astype(jnp.int16)
        wb[u, k] = weights[k].astype(BF)


def build_tile(tile, row_ids, idb, wb, u, store_low, store_high):
    ids = [idb[u, k] for k in range(FAN)]
    wts = [wb[u, k] for k in range(FAN)]
    for r in range(0, TILE // 8, 8):
        rows = row_ids[tile, r : r + 8]
        acc = jnp.zeros((8, 8, LANES), BF)
        for k in range(FAN):
            acc = jnp.where(ids[k][None] == rows, wts[k][None], acc)
        high = jnp.floor(acc)
        store_high(r, high)
        store_low(r, acc - high)


def kernel(
    x_hbm, ws1_hbm, wn1_hbm, ids_hbm, mask_hbm, ws2_hbm, wn2_hbm, ws3_hbm, wn3_hbm, out_ref,
    x_v, ws1, wn1, ids_in, mask_in, ws2, wn2, ws3t, wn3t,
    w1t, w2st, w2nt, yown, yrecv, ysum, sown, ssend, srecv,
    ids_pkt, ids_rcv, ids_s32, row_ids, idb, wb, inv,
    ring, a_own, acc, zbase, rs_send, rs_recv, h1, h2,
    in_sem, x_sem, ids_ss, ids_rs, y_ss, y_rs, s_ss, s_rs, r_ss, r_rs, g1_ss, g1_rs, g2_ss, g2_rs,
):
    me = lax.axis_index("g")
    core = lax.rem(me, 2)
    cx = lax.rem(me // 2, 2)
    cy = me // 4
    partner = me + 1 - 2 * core
    steps = (6 - 4 * cx - 8 * cy, 4 - 8 * cy, 2 - 4 * cx)
    peers = tuple(partner + step for step in steps)
    mates = tuple(me + step for step in steps)
    mine, theirs = (me, *peers), (partner, *mates)

    barrier = pltpu.get_barrier_semaphore()
    for peer in (*peers, partner):
        pl.semaphore_signal(barrier, inc=1, device_id=(peer,), device_id_type=MESH)

    def fetch(src, dst, i):
        cp = pltpu.make_async_copy(src, dst, in_sem.at[i])
        cp.start()
        return cp

    ids_cp = fetch(ids_hbm, ids_in, 0)
    mask_cp = fetch(mask_hbm, mask_in, 1)
    w1_cps = [fetch(ws1_hbm, ws1, 2), fetch(wn1_hbm, wn1, 3)]
    for b in range(N_DEV):
        cp = pltpu.make_async_copy(x_hbm.at[:, pl.ds(b * BLK, BLK)], x_v.at[b], x_sem)
        cp.start()
    late_cps = [fetch(ws2_hbm, ws2, 4), fetch(wn2_hbm, wn2, 5), fetch(ws3_hbm, ws3t, 6), fetch(wn3_hbm, wn3t, 7)]

    def remote(src, dst, ss, rs, dev):
        return pltpu.make_async_remote_copy(
            src_ref=src, dst_ref=dst, send_sem=ss, recv_sem=rs, device_id=(dev,), device_id_type=MESH
        )

    def drain(ref, sem):
        pltpu.make_async_copy(ref, ref, sem).wait()

    row_shape = (TILE // 8, 8, LANES)
    row_base = lax.broadcasted_iota(jnp.int32, row_shape, 0) * 8 + lax.broadcasted_iota(jnp.int32, row_shape, 1)
    for tile in range(HALF // TILE):
        row_ids[tile] = (row_base + tile * TILE).astype(jnp.int16)
    ids_pkt[...] = jnp.full(ids_pkt.shape, -1, jnp.int16)
    ids_cp.wait()
    mask_cp.wait()
    masked = jnp.where(mask_in[...] > 0, ids_in[...], -1)
    ids_pkt[0:FAN, :] = masked.astype(jnp.int16)
    pl.semaphore_wait(barrier, 4)
    id_copies = [remote(ids_pkt, ids_rcv.at[s], ids_ss, ids_rs.at[s], peers[s]) for s in range(3)]
    for s in (2, 1, 0):
        id_copies[s].start()
    for g in range(2):
        ids_s32[OWN + g, 0:FAN, :] = masked[:, g * LANES : (g + 1) * LANES]
        spread_ids(ids_s32, idb, wb, inv, OWN + g)
    for cp in w1_cps:
        cp.wait()
    w1t[0:HID, :] = ws1[...].T
    w1t[HID:, :] = wn1[...].T

    def build_own(tile, g):
        def put(half):
            def store(r, v):
                v = v if half else v * jnp.array(16.0, BF)
                row = tile % 2 * (TILE // 8) + r
                a_own[half * 4 + tile // 2, row : row + 8, :, g * LANES : (g + 1) * LANES] = v

            return store

        build_tile(tile, row_ids, idb, wb, OWN + g, put(0), put(1))

    drain(x_v, x_sem)
    for i in range(4):
        part = jnp.dot(w1t[...], x_v[theirs[i]], preferred_element_type=F32)
        yown[theirs[i]] = part[HID:].astype(BF)
        ssend[i] = part[:HID].astype(BF)
        part2 = jnp.dot(w1t[...], x_v[mine[i]], preferred_element_type=F32)
        yown[mine[i]] = part2[HID:].astype(BF)
        sown[i] = part2[:HID]
        for b in (theirs[i], mine[i]):
            remote(yown.at[b], yrecv.at[b], y_ss, y_rs, partner).start()
        build_own(2 * i, 0)
    for i in range(4):
        remote(ssend.at[i], srecv.at[i], s_ss, s_rs, partner).start()
    for tile in range(1, 8, 2):
        build_own(tile, 0)
    for tile in range(8):
        build_own(tile, 1)
    for cp in late_cps:
        cp.wait()
    w2st[...] = ws2[...].T
    w2nt[...] = wn2[...].T

    def build_into(flat):
        def put(half):
            def store(r, v):
                ring[flat % RING, half, r : r + 8] = v

            return store

        build_tile(flat % 8, row_ids, idb, wb, flat // 8, put(0), put(1))

    def dot_from(flat):
        tile = flat % 8
        cols = slice(tile % 2 * TILE, (tile % 2 + 1) * TILE)
        low = ring[flat % RING, 0].reshape(TILE, LANES)
        high = ring[flat % RING, 1].reshape(TILE, LANES)
        return (
            jnp.dot(ysum[tile // 2, :, cols], low, preferred_element_type=F32),
            jnp.dot(ysum[4 + tile // 2, :, cols], high, preferred_element_type=F32),
        )

    def lanes(g):
        return slice(g * LANES, (g + 1) * LANES)

    def quarter(q):
        return slice(q * Q, (q + 1) * Q)

    def take_ids(s):
        id_copies[s].wait_recv()
        for u, pair in enumerate(UNITS):
            for half, (slot, q) in enumerate(pair):
                if slot == s:
                    ids_s32[u, :, quarter(half)] = ids_rcv[s, :, quarter(q)].astype(jnp.int32)

    rs_copies = {}

    def finish_unit(u, low, high):
        total = (low * 16.0 + high) * jnp.broadcast_to(inv[u, 0:1, :], (HID, LANES))
        for half, (s, q) in enumerate(UNITS[u]):
            part = total[:, quarter(half)] + sown[1 + s, :, quarter(q)] + srecv[1 + s, :, quarter(q)].astype(F32)
            rs_send[s, q] = part.astype(BF)
            rs_copies[s, q] = remote(rs_send.at[s, q], rs_recv.at[s, q], r_ss, r_rs.at[4 * s + q], peers[s])
            rs_copies[s, q].start()

    def own_piece(b, g):
        return jnp.dot(ysum[b], a_own[b, :, :, lanes(g)].reshape(BLK, LANES), preferred_element_type=F32)

    def own_base(g, own):
        base = own * jnp.broadcast_to(inv[OWN + g, 0:1, :], (HID, LANES))
        zbase[g] = base + sown[0, :, lanes(g)] + srecv[0, :, lanes(g)].astype(F32)

    def own_dot(h, b, p):
        rows = a_own[b, p * Q // 8 : (p + 1) * Q // 8].reshape(Q, BLK)
        return jnp.dot(h[b, p], rows, preferred_element_type=F32)

    class Gather:
        def __init__(self, h, ss, rs, direct):
            self.h, self.ss, self.rs, self.direct = h, ss, rs, direct
            self.copies, self.forwards, self.ready = {}, [], []

        def copy(self, block, p, slot, dev):
            return remote(self.h.at[block, p], self.h.at[block, p], self.ss, self.rs.at[7 * p + slot], dev)

        def send(self, slot, p):
            dev = partner if slot == 3 else peers[slot]
            self.copies[slot, p] = self.copy(me, p, slot, dev)
            self.copies[slot, p].start()

        def take(self, slot, p):
            self.copies[slot, p].wait_recv()
            block = partner if slot == 3 else mates[0] if slot == 0 and p not in self.direct else peers[slot]
            if p not in self.direct and slot == (1 if p % 2 else 2):
                self.copies[0, p] = self.copy(block, p, 0, peers[3 - slot])
                self.copies[0, p].start()
            if slot < 3:
                fwd = self.copy(block, p, 4 + slot, partner)
                fwd.start()
                self.forwards.append((slot, p, fwd))
            self.ready.append((block, p))

        def take_forwards(self, n):
            for slot, p, fwd in self.forwards[:n]:
                fwd.wait_recv()
                relayed = slot == 0 and p not in self.direct
                self.ready.append((peers[0] if relayed else mates[slot], p))
            self.forwards = self.forwards[n:]

        def own(self, pieces):
            acc[...] = sum(own_dot(self.h, me, p) for p in range(pieces))

        def add(self):
            acc[...] += sum(own_dot(self.h, b, p) for b, p in self.ready)
            self.ready = []

    g1 = Gather(h1, g1_ss, g1_rs, direct=())
    g2 = Gather(h2, g2_ss, g2_rs, direct=())

    def finish_quarter(q):
        z = zbase[q // 2, :, quarter(q % 2)]
        for t in (1, 2, 0):
            rs_copies[t, q].wait_recv()
            z = z + rs_recv[t, q].astype(F32)
        h1[me, q] = jnp.maximum(z, 0.0).astype(BF)
        for slot in (0, 2, 1, 3) if q in g1.direct else (2, 1, 3):
            g1.send(slot, q)

    take_ids(2)
    take_ids(1)
    spread_ids(ids_s32, idb, wb, inv, 0)
    lead = 3
    for flat in range(lead):
        build_into(flat)
    drain(yrecv, y_rs)
    for b in range(N_DEV):
        ysum[b] = yown[b] + yrecv[b]
    built = lead
    low = high = own = None
    for flat in range(48):
        u, tile = flat // 8, flat % 8
        while built < 48 and built - flat < 2 or (built < 48 and tile % 2 == 0 and built - flat < lead):
            if built == 8:
                take_ids(0)
            if built % 8 == 0:
                spread_ids(ids_s32, idb, wb, inv, built // 8)
            build_into(built)
            built += 1
        part = dot_from(flat)
        low = part[0] if low is None else low + part[0]
        high = part[1] if high is None else high + part[1]
        if u in (1, 3):
            own = own_piece(tile, u // 2) if own is None else own + own_piece(tile, u // 2)
        if tile == 7:
            if u == 0:
                drain(srecv, s_rs)
            finish_unit(u, low, high)
            low = high = None
            if u in (1, 3):
                own_base(u // 2, own)
                own = None
    finish_quarter(0)
    finish_quarter(1)
    finish_quarter(2)
    finish_quarter(3)
    g1.own(4)
    for g in range(2):
        block = jnp.concatenate([h1[me, 2 * g], h1[me, 2 * g + 1]], axis=1)
        zbase[g] = jnp.dot(w2st[...], block, preferred_element_type=F32)
    for slot, p in ((2, 0), (1, 0), (1, 1), (2, 1), (2, 2), (1, 2)):
        g1.take(slot, p)
    for p in range(4):
        g1.take(3, p)
    g1.add()
    for slot, p in ((2, 3), (1, 3), (0, 0), (0, 1)):
        g1.take(slot, p)
    g1.take_forwards(6)
    g1.add()
    for slot, p in ((0, 2), (0, 3)):
        g1.take(slot, p)
    g1.add()
    g1.take_forwards(4)
    g1.add()
    g1.take_forwards(2)
    g1.add()

    inv_own = jnp.concatenate(
        [jnp.broadcast_to(inv[OWN + g, 0:1, :], (HID, LANES)) for g in range(2)], axis=1
    )
    for g in range(2):
        mean1 = (acc[:, lanes(g)] * inv_own[:, lanes(g)]).astype(BF)
        pre2 = zbase[g] + jnp.dot(w2nt[...], mean1, preferred_element_type=F32)
        for half in range(2):
            h2[me, 2 * g + half] = jnp.maximum(pre2[:, quarter(half)], 0.0).astype(BF)
        g2.send(2, 2 * g)
        g2.send(1, 2 * g + 1)
    for slot, p in ((2, 1), (1, 0), (2, 3), (1, 2)):
        g2.send(slot, p)
    for p in range(4):
        g2.send(3, p)
    g2.own(4)
    for g in range(2):
        block = jnp.concatenate([h2[me, 2 * g], h2[me, 2 * g + 1]], axis=1)
        out_ref[:, lanes(g)] = jnp.dot(ws3t[...], block, preferred_element_type=F32)
    drain(ids_rcv, ids_ss)
    drain(yown, y_ss)
    drain(ssend, s_ss)
    drain(rs_send, r_ss)
    drain(h1.at[0:7], g1_ss)
    for p in range(4):
        g2.take(3, p)
    g2.add()
    for slot, p in ((2, 0), (1, 1), (2, 2), (1, 3)):
        g2.take(slot, p)
    g2.add()
    for slot, p in ((2, 1), (1, 0), (2, 3), (1, 2)):
        g2.take(slot, p)
    g2.take_forwards(4)
    g2.add()
    g2.take(0, 0)
    g2.take(0, 1)
    g2.take_forwards(4)
    g2.add()
    g2.take(0, 2)
    g2.take(0, 3)
    g2.take_forwards(2)
    g2.add()
    g2.take_forwards(2)
    g2.add()
    for g in range(2):
        mean2 = (acc[:, lanes(g)] * inv_own[:, lanes(g)]).astype(BF)
        out_ref[:, lanes(g)] += jnp.dot(wn3t[...], mean2, preferred_element_type=F32)
    drain(h2.at[0:7], g2_ss)


def solution(mesh):
    def device_step(feat, ws1, wn1, ids, mask, ws2, wn2, ws3, wn3):
        operands = (feat.T, ws1, wn1, ids.T, mask.T, ws2, wn2, ws3.T, wn3.T)
        vm = pl.BlockSpec(memory_space=pltpu.VMEM)
        dma = pltpu.SemaphoreType.DMA
        out_t = pl.pallas_call(
            kernel,
            out_shape=jax.ShapeDtypeStruct((7, BLK), F32),
            in_specs=[pl.BlockSpec(memory_space=pltpu.HBM)] * 9,
            out_specs=vm,
            scratch_shapes=[
                pltpu.VMEM((N_DEV, 192, BLK), BF),
                pltpu.VMEM((192, HID), BF),
                pltpu.VMEM((192, HID), BF),
                pltpu.VMEM((FAN, BLK), jnp.int32),
                pltpu.VMEM((FAN, BLK), jnp.int32),
                pltpu.VMEM((HID, HID), BF),
                pltpu.VMEM((HID, HID), BF),
                pltpu.VMEM((7, HID), BF),
                pltpu.VMEM((7, HID), BF),
                pltpu.VMEM((2 * HID, 192), BF),
                pltpu.VMEM((HID, HID), BF),
                pltpu.VMEM((HID, HID), BF),
                pltpu.VMEM((N_DEV, HID, BLK), BF),
                pltpu.VMEM((N_DEV, HID, BLK), BF),
                pltpu.VMEM((N_DEV, HID, BLK), BF),
                pltpu.VMEM((4, HID, BLK), F32),
                pltpu.VMEM((4, HID, BLK), BF),
                pltpu.VMEM((4, HID, BLK), BF),
                pltpu.VMEM((16, BLK), jnp.int16),
                pltpu.VMEM((3, 16, BLK), jnp.int16),
                pltpu.VMEM((8, 16, LANES), jnp.int32),
                pltpu.VMEM((HALF // TILE, TILE // 8, 8, LANES), jnp.int16),
                pltpu.VMEM((8, FAN, 8, LANES), jnp.int16),
                pltpu.VMEM((8, FAN, 8, LANES), BF),
                pltpu.VMEM((8, 8, LANES), F32),
                pltpu.VMEM((RING, 2, TILE // 8, 8, LANES), BF),
                pltpu.VMEM((N_DEV, BLK // 8, 8, BLK), BF),
                pltpu.VMEM((HID, BLK), F32),
                pltpu.VMEM((2, HID, LANES), F32),
                pltpu.VMEM((3, 4, HID, Q), BF),
                pltpu.VMEM((3, 4, HID, Q), BF),
                pltpu.VMEM((N_DEV, 4, HID, Q), BF),
                pltpu.VMEM((N_DEV, 4, HID, Q), BF),
                dma((8,)),
                dma,
                dma, dma((3,)),
                dma, dma,
                dma, dma,
                dma, dma((12,)),
                dma, dma((28,)),
                dma, dma((28,)),
            ],
            compiler_params=pltpu.CompilerParams(
                collective_id=0, has_side_effects=True, vmem_limit_bytes=32 * 1024 * 1024
            ),
            name="graphsage",
        )(*(pltpu.with_memory_space_constraint(a, pltpu.HBM) for a in operands))
        return out_t.T

    col_split = P(None, "g")
    row_split = P("g", None)
    replicated = P()
    return jax.shard_map(
        device_step,
        mesh=mesh,
        in_specs=(col_split, row_split, row_split, row_split, row_split, replicated, replicated, replicated, replicated),
        out_specs=row_split,
        check_vma=False,
    )
```

```python
import jax
import jax.numpy as jnp
from jax import lax
from jax.experimental import pallas as pl
from jax.experimental.pallas import tpu as pltpu
from jax.sharding import PartitionSpec as P

MESH = pl.DeviceIdType.MESH
N_DEV = 8
NODES = 4096
BLK = NODES // N_DEV
HALF = NODES // 2
FAN = 10
HID = 128
TILE = 256
LANES = 256
BF = jnp.bfloat16
F32 = jnp.float32


UNITS = (((2, 0), (1, 0)), ((0, 0), (0, 1)), ((2, 1), (1, 1)), ((0, 2), (0, 3)), ((2, 2), (1, 2)), ((2, 3), (1, 3)))
OWN = 6
RING = 6
Q = 128


def spread_ids(ids_s32, idb, wb, inv, u):
    words, weights = [], []
    degree = jnp.zeros((8, LANES), F32)
    for k in range(FAN):
        raw = jnp.broadcast_to(ids_s32[u, k : k + 1, :], (8, LANES))
        valid = raw >= 0
        degree += jnp.where(valid, 1.0, 0.0)
        upper = raw >= HALF
        word = jnp.where(upper, raw - HALF, raw)
        weight = jnp.where(valid, jnp.where(upper, 1.0, 0.0625), 0.0)
        for m in range(k):
            same = word == words[m]
            weights[m] = weights[m] + jnp.where(same, weight, 0.0)
            word = jnp.where(same, -1, word)
        words.append(word)
        weights.append(weight)
    inv[u] = 1.0 / degree
    for k in range(FAN):
        idb[u, k] = words[k].astype(jnp.int16)
        wb[u, k] = weights[k].astype(BF)


def build_tile(tile, row_ids, idb, wb, u, store_low, store_high):
    ids = [idb[u, k] for k in range(FAN)]
    wts = [wb[u, k] for k in range(FAN)]
    for r in range(0, TILE // 8, 8):
        rows = row_ids[tile, r : r + 8]
        acc = jnp.zeros((8, 8, LANES), BF)
        for k in range(FAN):
            acc = jnp.where(ids[k][None] == rows, wts[k][None], acc)
        high = jnp.floor(acc)
        store_high(r, high)
        store_low(r, acc - high)


def kernel(
    x_hbm, ws1_hbm, wn1_hbm, ids_hbm, mask_hbm, ws2_hbm, wn2_hbm, ws3_hbm, wn3_hbm, out_ref,
    x_v, ws1, wn1, ids_in, mask_in, ws2, wn2, ws3t, wn3t,
    w1t, w2st, w2nt, yown, yrecv, ysum, sown, ssend, srecv,
    ids_pkt, ids_rcv, ids_s32, row_ids, idb, wb, inv,
    ring, a_own, acc, zbase, rs_send, rs_recv, h1, h2,
    in_sem, x_sem, ids_ss, ids_rs, y_ss, y_rs, s_ss, s_rs, r_ss, r_rs, g1_ss, g1_rs, g2_ss, g2_rs,
):
    me = lax.axis_index("g")
    core = lax.rem(me, 2)
    cx = lax.rem(me // 2, 2)
    cy = me // 4
    partner = me + 1 - 2 * core
    steps = (6 - 4 * cx - 8 * cy, 4 - 8 * cy, 2 - 4 * cx)
    peers = tuple(partner + step for step in steps)
    mates = tuple(me + step for step in steps)
    mine, theirs = (me, *peers), (partner, *mates)

    barrier = pltpu.get_barrier_semaphore()
    for peer in (*peers, partner):
        pl.semaphore_signal(barrier, inc=1, device_id=(peer,), device_id_type=MESH)

    def fetch(src, dst, i):
        cp = pltpu.make_async_copy(src, dst, in_sem.at[i])
        cp.start()
        return cp

    ids_cp = fetch(ids_hbm, ids_in, 0)
    mask_cp = fetch(mask_hbm, mask_in, 1)
    w1_cps = [fetch(ws1_hbm, ws1, 2), fetch(wn1_hbm, wn1, 3)]
    for b in range(N_DEV):
        cp = pltpu.make_async_copy(x_hbm.at[:, pl.ds(b * BLK, BLK)], x_v.at[b], x_sem)
        cp.start()
    late_cps = [fetch(ws2_hbm, ws2, 4), fetch(wn2_hbm, wn2, 5), fetch(ws3_hbm, ws3t, 6), fetch(wn3_hbm, wn3t, 7)]

    def remote(src, dst, ss, rs, dev):
        return pltpu.make_async_remote_copy(
            src_ref=src, dst_ref=dst, send_sem=ss, recv_sem=rs, device_id=(dev,), device_id_type=MESH
        )

    def drain(ref, sem):
        pltpu.make_async_copy(ref, ref, sem).wait()

    row_shape = (TILE // 8, 8, LANES)
    row_base = lax.broadcasted_iota(jnp.int32, row_shape, 0) * 8 + lax.broadcasted_iota(jnp.int32, row_shape, 1)
    for tile in range(HALF // TILE):
        row_ids[tile] = (row_base + tile * TILE).astype(jnp.int16)
    ids_pkt[...] = jnp.full(ids_pkt.shape, -1, jnp.int16)
    ids_cp.wait()
    mask_cp.wait()
    masked = jnp.where(mask_in[...] > 0, ids_in[...], -1)
    ids_pkt[0:FAN, :] = masked.astype(jnp.int16)
    pl.semaphore_wait(barrier, 4)
    id_copies = [remote(ids_pkt, ids_rcv.at[s], ids_ss, ids_rs.at[s], peers[s]) for s in range(3)]
    for s in (2, 1, 0):
        id_copies[s].start()
    for g in range(2):
        ids_s32[OWN + g, 0:FAN, :] = masked[:, g * LANES : (g + 1) * LANES]
        spread_ids(ids_s32, idb, wb, inv, OWN + g)
    for cp in w1_cps:
        cp.wait()
    w1t[0:HID, :] = ws1[...].T
    w1t[HID:, :] = wn1[...].T

    def build_own(tile, g):
        def put(half):
            def store(r, v):
                v = v if half else v * jnp.array(16.0, BF)
                row = tile % 2 * (TILE // 8) + r
                a_own[half * 4 + tile // 2, row : row + 8, :, g * LANES : (g + 1) * LANES] = v

            return store

        build_tile(tile, row_ids, idb, wb, OWN + g, put(0), put(1))

    drain(x_v, x_sem)
    for i in range(4):
        part = jnp.dot(w1t[...], x_v[theirs[i]], preferred_element_type=F32)
        yown[theirs[i]] = part[HID:].astype(BF)
        ssend[i] = part[:HID].astype(BF)
        part2 = jnp.dot(w1t[...], x_v[mine[i]], preferred_element_type=F32)
        yown[mine[i]] = part2[HID:].astype(BF)
        sown[i] = part2[:HID]
        for b in (theirs[i], mine[i]):
            remote(yown.at[b], yrecv.at[b], y_ss, y_rs, partner).start()
        build_own(2 * i, 0)
    for i in range(4):
        remote(ssend.at[i], srecv.at[i], s_ss, s_rs, partner).start()
    for tile in range(1, 8, 2):
        build_own(tile, 0)
    for tile in range(8):
        build_own(tile, 1)
    for cp in late_cps:
        cp.wait()
    w2st[...] = ws2[...].T
    w2nt[...] = wn2[...].T

    def build_into(flat):
        def put(half):
            def store(r, v):
                ring[flat % RING, half, r : r + 8] = v

            return store

        build_tile(flat % 8, row_ids, idb, wb, flat // 8, put(0), put(1))

    def dot_from(flat):
        tile = flat % 8
        cols = slice(tile % 2 * TILE, (tile % 2 + 1) * TILE)
        low = ring[flat % RING, 0].reshape(TILE, LANES)
        high = ring[flat % RING, 1].reshape(TILE, LANES)
        return (
            jnp.dot(ysum[tile // 2, :, cols], low, preferred_element_type=F32),
            jnp.dot(ysum[4 + tile // 2, :, cols], high, preferred_element_type=F32),
        )

    def lanes(g):
        return slice(g * LANES, (g + 1) * LANES)

    def quarter(q):
        return slice(q * Q, (q + 1) * Q)

    def take_ids(s):
        id_copies[s].wait_recv()
        for u, pair in enumerate(UNITS):
            for half, (slot, q) in enumerate(pair):
                if slot == s:
                    ids_s32[u, :, quarter(half)] = ids_rcv[s, :, quarter(q)].astype(jnp.int32)

    rs_copies = {}

    def finish_unit(u, low, high):
        total = (low * 16.0 + high) * jnp.broadcast_to(inv[u, 0:1, :], (HID, LANES))
        for half, (s, q) in enumerate(UNITS[u]):
            part = total[:, quarter(half)] + sown[1 + s, :, quarter(q)] + srecv[1 + s, :, quarter(q)].astype(F32)
            rs_send[s, q] = part.astype(BF)
            rs_copies[s, q] = remote(rs_send.at[s, q], rs_recv.at[s, q], r_ss, r_rs.at[4 * s + q], peers[s])
            rs_copies[s, q].start()

    def own_piece(b, g):
        return jnp.dot(ysum[b], a_own[b, :, :, lanes(g)].reshape(BLK, LANES), preferred_element_type=F32)

    def own_base(g, own):
        base = own * jnp.broadcast_to(inv[OWN + g, 0:1, :], (HID, LANES))
        zbase[g] = base + sown[0, :, lanes(g)] + srecv[0, :, lanes(g)].astype(F32)

    def own_dot(h, b, p):
        rows = a_own[b, p * Q // 8 : (p + 1) * Q // 8].reshape(Q, BLK)
        return jnp.dot(h[b, p], rows, preferred_element_type=F32)

    class Gather:
        def __init__(self, h, ss, rs, direct):
            self.h, self.ss, self.rs, self.direct = h, ss, rs, direct
            self.copies, self.forwards, self.ready = {}, [], []

        def copy(self, block, p, slot, dev):
            return remote(self.h.at[block, p], self.h.at[block, p], self.ss, self.rs.at[7 * p + slot], dev)

        def send(self, slot, p):
            dev = partner if slot == 3 else peers[slot]
            self.copies[slot, p] = self.copy(me, p, slot, dev)
            self.copies[slot, p].start()

        def take(self, slot, p):
            self.copies[slot, p].wait_recv()
            block = partner if slot == 3 else mates[0] if slot == 0 and p not in self.direct else peers[slot]
            if p not in self.direct and slot == (1 if p % 2 else 2):
                self.copies[0, p] = self.copy(block, p, 0, peers[3 - slot])
                self.copies[0, p].start()
            if slot < 3:
                fwd = self.copy(block, p, 4 + slot, partner)
                fwd.start()
                self.forwards.append((slot, p, fwd))
            self.ready.append((block, p))

        def take_forwards(self, n):
            for slot, p, fwd in self.forwards[:n]:
                fwd.wait_recv()
                relayed = slot == 0 and p not in self.direct
                self.ready.append((peers[0] if relayed else mates[slot], p))
            self.forwards = self.forwards[n:]

        def own(self, pieces):
            acc[...] = sum(own_dot(self.h, me, p) for p in range(pieces))

        def add(self):
            acc[...] += sum(own_dot(self.h, b, p) for b, p in self.ready)
            self.ready = []

    g1 = Gather(h1, g1_ss, g1_rs, direct=(3,))
    g2 = Gather(h2, g2_ss, g2_rs, direct=())

    def finish_quarter(q):
        z = zbase[q // 2, :, quarter(q % 2)]
        for t in (1, 2, 0):
            rs_copies[t, q].wait_recv()
            z = z + rs_recv[t, q].astype(F32)
        h1[me, q] = jnp.maximum(z, 0.0).astype(BF)
        for slot in (0, 2, 1, 3) if q in g1.direct else (2, 1, 3):
            g1.send(slot, q)

    take_ids(2)
    take_ids(1)
    spread_ids(ids_s32, idb, wb, inv, 0)
    lead = 3
    for flat in range(lead):
        build_into(flat)
    drain(yrecv, y_rs)
    for b in range(N_DEV):
        ysum[b] = yown[b] + yrecv[b]
    built = lead
    low = high = own = None
    for flat in range(48):
        u, tile = flat // 8, flat % 8
        while built < 48 and built - flat < 2 or (built < 48 and tile % 2 == 0 and built - flat < lead):
            if built == 8:
                take_ids(0)
            if built % 8 == 0:
                spread_ids(ids_s32, idb, wb, inv, built // 8)
            build_into(built)
            built += 1
        part = dot_from(flat)
        low = part[0] if low is None else low + part[0]
        high = part[1] if high is None else high + part[1]
        if u in (1, 3):
            own = own_piece(tile, u // 2) if own is None else own + own_piece(tile, u // 2)
        if tile == 7:
            if u == 0:
                drain(srecv, s_rs)
            finish_unit(u, low, high)
            low = high = None
            if u in (1, 3):
                own_base(u // 2, own)
                own = None
    finish_quarter(0)
    finish_quarter(2)
    finish_quarter(1)
    finish_quarter(3)
    g1.own(4)
    for g in range(2):
        block = jnp.concatenate([h1[me, 2 * g], h1[me, 2 * g + 1]], axis=1)
        zbase[g] = jnp.dot(w2st[...], block, preferred_element_type=F32)
    for slot, p in ((2, 0), (1, 0), (1, 1), (2, 1), (2, 2), (1, 2)):
        g1.take(slot, p)
    for p in range(4):
        g1.take(3, p)
    g1.add()
    g1.take(0, 0)
    g1.take(0, 1)
    g1.take_forwards(6)
    g1.add()
    for slot, p in ((2, 3), (1, 3), (0, 3), (0, 2)):
        g1.take(slot, p)
    g1.add()
    g1.take_forwards(4)
    g1.add()
    g1.take_forwards(2)
    g1.add()

    inv_own = jnp.concatenate(
        [jnp.broadcast_to(inv[OWN + g, 0:1, :], (HID, LANES)) for g in range(2)], axis=1
    )
    for g in range(2):
        mean1 = (acc[:, lanes(g)] * inv_own[:, lanes(g)]).astype(BF)
        pre2 = zbase[g] + jnp.dot(w2nt[...], mean1, preferred_element_type=F32)
        for half in range(2):
            h2[me, 2 * g + half] = jnp.maximum(pre2[:, quarter(half)], 0.0).astype(BF)
        g2.send(2, 2 * g)
        g2.send(1, 2 * g + 1)
    for slot, p in ((2, 1), (1, 0), (2, 3), (1, 2)):
        g2.send(slot, p)
    for p in range(4):
        g2.send(3, p)
    g2.own(4)
    for g in range(2):
        block = jnp.concatenate([h2[me, 2 * g], h2[me, 2 * g + 1]], axis=1)
        out_ref[:, lanes(g)] = jnp.dot(ws3t[...], block, preferred_element_type=F32)
    drain(ids_rcv, ids_ss)
    drain(yown, y_ss)
    drain(ssend, s_ss)
    drain(rs_send, r_ss)
    drain(h1.at[0:7], g1_ss)
    for p in range(4):
        g2.take(3, p)
    g2.add()
    for slot, p in ((2, 0), (1, 1), (2, 2), (1, 3)):
        g2.take(slot, p)
    g2.add()
    for slot, p in ((2, 1), (1, 0), (2, 3), (1, 2)):
        g2.take(slot, p)
    g2.take_forwards(4)
    g2.add()
    g2.take(0, 0)
    g2.take(0, 1)
    g2.take_forwards(4)
    g2.add()
    g2.take(0, 2)
    g2.take(0, 3)
    g2.take_forwards(2)
    g2.add()
    g2.take_forwards(2)
    g2.add()
    for g in range(2):
        mean2 = (acc[:, lanes(g)] * inv_own[:, lanes(g)]).astype(BF)
        out_ref[:, lanes(g)] += jnp.dot(wn3t[...], mean2, preferred_element_type=F32)
    drain(h2.at[0:7], g2_ss)


def solution(mesh):
    def device_step(feat, ws1, wn1, ids, mask, ws2, wn2, ws3, wn3):
        operands = (feat.T, ws1, wn1, ids.T, mask.T, ws2, wn2, ws3.T, wn3.T)
        vm = pl.BlockSpec(memory_space=pltpu.VMEM)
        dma = pltpu.SemaphoreType.DMA
        out_t = pl.pallas_call(
            kernel,
            out_shape=jax.ShapeDtypeStruct((7, BLK), F32),
            in_specs=[pl.BlockSpec(memory_space=pltpu.HBM)] * 9,
            out_specs=vm,
            scratch_shapes=[
                pltpu.VMEM((N_DEV, 192, BLK), BF),
                pltpu.VMEM((192, HID), BF),
                pltpu.VMEM((192, HID), BF),
                pltpu.VMEM((FAN, BLK), jnp.int32),
                pltpu.VMEM((FAN, BLK), jnp.int32),
                pltpu.VMEM((HID, HID), BF),
                pltpu.VMEM((HID, HID), BF),
                pltpu.VMEM((7, HID), BF),
                pltpu.VMEM((7, HID), BF),
                pltpu.VMEM((2 * HID, 192), BF),
                pltpu.VMEM((HID, HID), BF),
                pltpu.VMEM((HID, HID), BF),
                pltpu.VMEM((N_DEV, HID, BLK), BF),
                pltpu.VMEM((N_DEV, HID, BLK), BF),
                pltpu.VMEM((N_DEV, HID, BLK), BF),
                pltpu.VMEM((4, HID, BLK), F32),
                pltpu.VMEM((4, HID, BLK), BF),
                pltpu.VMEM((4, HID, BLK), BF),
                pltpu.VMEM((16, BLK), jnp.int16),
                pltpu.VMEM((3, 16, BLK), jnp.int16),
                pltpu.VMEM((8, 16, LANES), jnp.int32),
                pltpu.VMEM((HALF // TILE, TILE // 8, 8, LANES), jnp.int16),
                pltpu.VMEM((8, FAN, 8, LANES), jnp.int16),
                pltpu.VMEM((8, FAN, 8, LANES), BF),
                pltpu.VMEM((8, 8, LANES), F32),
                pltpu.VMEM((RING, 2, TILE // 8, 8, LANES), BF),
                pltpu.VMEM((N_DEV, BLK // 8, 8, BLK), BF),
                pltpu.VMEM((HID, BLK), F32),
                pltpu.VMEM((2, HID, LANES), F32),
                pltpu.VMEM((3, 4, HID, Q), BF),
                pltpu.VMEM((3, 4, HID, Q), BF),
                pltpu.VMEM((N_DEV, 4, HID, Q), BF),
                pltpu.VMEM((N_DEV, 4, HID, Q), BF),
                dma((8,)),
                dma,
                dma, dma((3,)),
                dma, dma,
                dma, dma,
                dma, dma((12,)),
                dma, dma((28,)),
                dma, dma((28,)),
            ],
            compiler_params=pltpu.CompilerParams(
                collective_id=0, has_side_effects=True, vmem_limit_bytes=32 * 1024 * 1024
            ),
            name="graphsage",
        )(*(pltpu.with_memory_space_constraint(a, pltpu.HBM) for a in operands))
        return out_t.T

    col_split = P(None, "g")
    row_split = P("g", None)
    replicated = P()
    return jax.shard_map(
        device_step,
        mesh=mesh,
        in_specs=(col_split, row_split, row_split, row_split, row_split, replicated, replicated, replicated, replicated),
        out_specs=row_split,
        check_vma=False,
    )
```
